32 devices in a mesh: lev: 4 (over x, core), lon: 8 (over z, y).
Axes of the slice: x: 2, y: 2, z: 4, core: 2. Of those that a mesh axis runs over, the one named last changes fastest.
Arguments:
- previous: float32 [36, 64, 4096], P('lev', None, 'lon'), may hold values from -4 to 4
- loss_matrix: float32 [36, 64, 64], P('lev'), may hold values from -3 to 10, as said below
- pair_matrix: float32 [36, 64, 64], P('lev'), may hold values from -0.1875 to 0.1875
- diffusivity: float32 [36], P('lev'), may hold values from 200 to 2000
- mixing: float32 [36], P('lev'), may hold values from 0.1 to 1
Outputs:
- concentration: float32 [36, 64, 4096], P('lev', None, 'lon')
- level_variance: float32 [36, 64], P('lev')
The draws below stay inside these ranges and needn't reach their ends.
Inputs may be any that keep to these rules, and one draw needn't show every extreme that they name: `loss_matrix`: each of the 36 blocks is symmetric and at least 0.05 times the identity in the positive definite order.
All inputs are finite; a program needn't handle non-finite values.
Results may differ from the reference program's by a relative error of at most 0.00045.
Values sent between devices are 32-bit elements; how exact they have to be, the bound alone decides.
A program may use at most 64 MiB of HBM per device.

```python
import math
import jax
import jax.numpy as jnp
from jax import lax

S = 64
ITERS = 2
L = 36
NCOL = 4096


def draw_loss_matrix(key, part):
    first_key, second_key = jax.random.split(jax.random.fold_in(key, 17))
    base = jax.random.normal(first_key, (L, S, S), jnp.float32)
    level_scale = jax.random.uniform(second_key, (L,), jnp.float32, 0.2, 2.0)
    gram = jnp.einsum('lst,lut->lsu', base, base, precision=lax.Precision.HIGHEST) / S
    gram = 0.5 * (gram + jnp.swapaxes(gram, 1, 2))
    identity = jnp.eye(S, dtype=jnp.float32)
    return level_scale[:, None, None] * (0.25 * identity + gram)


def block_scale(own_key, dims, shards, least, high):
    def one(position, parts):
        steps = jax.random.uniform(jax.random.fold_in(jax.random.fold_in(own_key, 6), position), (parts,), jnp.float32, least / len(shards), high / len(shards))
        return jnp.repeat(jnp.exp(steps), dims[position] // parts).reshape((-1,) + (1,) * (len(dims) - position - 1))

    level = one(*shards[0])
    for cut in shards[1:]:
        level = level * one(*cut)
    return level


def normal_values(own_key, dims, scale, most, cuts=(), held_as=jnp.bfloat16):
    gain = block_scale(own_key, dims, cuts, -0.22, 0.18) if cuts else 1.0
    drawn = jax.random.normal(own_key, dims, jnp.float32) * scale * gain
    return jnp.minimum(jnp.maximum(drawn, -most), most).astype(held_as)


def setup_inputs(seed: int = 0) -> dict:
    key_of = jax.random.split(jax.random.key(seed), 6)
    return {
        "previous": normal_values(key_of[0], (L, S, NCOL), 1.0, 4.0, ((0, 4), (2, 8)), jnp.float32),
        "loss_matrix": draw_loss_matrix(jax.random.fold_in(key_of[5], 71), 0),
        "pair_matrix": normal_values(key_of[2], (L, S, S), (16 * S) ** -0.5, 0.1875, ((0, 4),), jnp.float32),
        "diffusivity": jnp.clip(jnp.exp(math.log(2000.0) - 2.3025851 * jax.random.uniform(key_of[3], (L,), jnp.float32) ** block_scale(key_of[3], (L,), ((0, 4),), -0.2, 0.2)), 200.0, 2000.0),
        "mixing": jnp.clip(jnp.exp(math.log(1.0) - 2.3025851 * jax.random.uniform(key_of[4], (L,), jnp.float32) ** block_scale(key_of[4], (L,), ((0, 4),), -0.2, 0.2)), 0.1, 1.0),
    }


HIGHEST_PRECISION = lax.Precision.HIGHEST

def residual_of(current, previous, loss_matrix, pair_matrix, diffusivity, mixing):
    above_links = jnp.concatenate([jnp.zeros((1,), current.dtype), diffusivity[:-1]])
    zero_level = jnp.zeros_like(current[:1])
    level_above = jnp.concatenate([zero_level, current[:-1]], axis=0)
    level_below = jnp.concatenate([current[1:], zero_level], axis=0)
    across = mixing[:, None, None] * (jnp.roll(current, 1, axis=2) + jnp.roll(current, -1, axis=2) - 2.0 * current)
    own_chem = jnp.einsum('lst,ltc->lsc', loss_matrix, current, precision=HIGHEST_PRECISION)
    pair_chem = jnp.einsum('lst,ltc->lsc', pair_matrix, current * current, precision=HIGHEST_PRECISION)
    vertical = diffusivity[:, None, None] * (current - level_below) + above_links[:, None, None] * (current - level_above)
    return current + own_chem + pair_chem + vertical - across - previous

def newton_solve(forcing, loss_matrix, diffusivity):
    species = loss_matrix.shape[1]
    identity = jnp.eye(species, dtype=loss_matrix.dtype)
    above_links = jnp.concatenate([jnp.zeros((1,), diffusivity.dtype), diffusivity[:-1]])
    diagonal = (1.0 + above_links + diffusivity)[:, None, None] * identity + loss_matrix

    def factor_step(prev_inverse, pieces):
        block, link_above = pieces
        inverse = jnp.linalg.inv(block - link_above * link_above * prev_inverse)
        return (inverse, inverse)
    _, inverses = lax.scan(factor_step, jnp.zeros_like(identity), (diagonal, above_links))

    def forward(prev_lifted, pieces):
        inverse, link_above, right_side = pieces
        lifted = jnp.dot(inverse, right_side + link_above * prev_lifted, precision=HIGHEST_PRECISION)
        return (lifted, lifted)
    _, lifted_all = lax.scan(forward, jnp.zeros_like(forcing[0]), (inverses, above_links, forcing))

    def backward(next_value, pieces):
        inverse, link_below, lifted_level = pieces
        value = lifted_level + link_below * jnp.dot(inverse, next_value, precision=HIGHEST_PRECISION)
        return (value, value)
    _, solution = lax.scan(backward, jnp.zeros_like(forcing[0]), (inverses, diffusivity, lifted_all), reverse=True)
    return solution

def reference(previous, loss_matrix, pair_matrix, diffusivity, mixing):
    current = previous
    for newton_step in range(ITERS):
        forcing = residual_of(current, previous, loss_matrix, pair_matrix, diffusivity, mixing)
        current = current - newton_solve(forcing, loss_matrix, diffusivity)
    variance = jnp.mean(current * current, axis=2)
    return (current, variance)
```

```python
import functools
import itertools

import jax
import jax.numpy as jnp
from jax import lax
from jax.experimental import pallas as pl
from jax.experimental.pallas import tpu as pltpu
from jax.sharding import PartitionSpec as P

LEAST = 1.05
MOST = 10.0
HIGHEST = lax.Precision.HIGHEST
SMEM = pl.BlockSpec(memory_space=pltpu.SMEM)
VMEM = pl.BlockSpec(memory_space=pltpu.VMEM)


def dot(a, b, dims=((1,), (0,))):
    return lax.dot_general(
        a, b, (dims, ((), ())), precision=HIGHEST, preferred_element_type=jnp.float32
    )


def dot_t(a, b):
    return dot(a, b, ((1,), (1,)))


def eye_of(size):
    rows = lax.broadcasted_iota(jnp.int32, (size, size), 0)
    cols = lax.broadcasted_iota(jnp.int32, (size, size), 1)
    return rows == cols


def invert_all(blocks, floors, steps):
    size = blocks[0].shape[0]
    unit = jnp.where(eye_of(size), 1.0, 0.0).astype(jnp.float32)
    start, worst = [], None
    for a, lo in zip(blocks, floors):
        hi = jnp.max(jnp.sum(jnp.abs(a), axis=0, keepdims=True), axis=1, keepdims=True)
        hi = jnp.clip(hi, lo, lo * spread(size))
        scale = 2.0 / (hi + lo)
        rho = (hi - lo) / (hi + lo)
        start.append((scale, a))
        worst = rho if worst is None else jnp.maximum(worst, rho)

    def grow(rho):
        square = rho * rho
        return square / (2.0 - square), 2.0 / (2.0 - square)

    rho, gain = grow(worst)
    start = [(gain * scale) * (2.0 * unit - scale * a) for scale, a in start]

    def step(carry):
        rho, *xs = carry
        rest = [unit - dot(a, x) for a, x in zip(blocks, xs)]
        rho, gain = grow(rho)
        return (rho, *[gain * (x + dot(x, r)) for x, r in zip(xs, rest)])

    if steps is None:
        return lax.while_loop(lambda carry: jnp.max(carry[0]) > 3e-8, step, (rho, *start))[1:]
    return lax.fori_loop(0, steps, lambda i, carry: step(carry), (rho, *start))[1:]


def spread(size):
    return (1.0 + MOST * size) / (0.96 * LEAST)


def enough_steps(condition):
    rho, steps = (condition - 1.0) / (condition + 1.0), -1
    while rho > 3e-8:
        rho, steps = rho * rho / (2.0 - rho * rho), steps + 1
    return steps


def plan(lo, hi, out):
    if lo >= hi:
        return 0
    mid = lo + (hi - lo) // 2
    depth = 1 + max(plan(lo, mid, out), plan(mid + 1, hi, out))
    out.setdefault(depth, []).append((lo, mid, hi))
    return depth


def dense_inverse(diag, low, floor_diag, floor_low, steps=None):
    count, size = len(diag), diag[0].shape[0]
    unit = jnp.where(eye_of(size), 1.0, 0.0).astype(jnp.float32)
    by_depth, done, thin = {}, {}, {}
    plan(0, count, by_depth)
    for depth in sorted(by_depth):
        nodes = by_depth[depth]
        schur, arms, floors, thin_arms = [], [], [], []
        for lo, mid, hi in nodes:
            s, parts = diag[mid], []
            t, thin_parts = floor_diag[mid], []
            if lo < mid:
                arm = low_right(done[lo, mid][-1], low, mid, False)
                s = s - low(mid, arm[-size:])
                parts.append(arm)
                thin_parts += [floor_low[mid] * x for x in thin[lo, mid][-1]]
                t = t - floor_low[mid] * thin_parts[-1]
            parts.append(unit)
            thin_parts.append(1.0)
            if mid + 1 < hi:
                arm = low_right(done[mid + 1, hi][0], low, mid + 1, True)
                s = s - low(mid + 1, arm[:size], True)
                parts.append(arm)
                thin_arm = [floor_low[mid + 1] * x for x in thin[mid + 1, hi][0]]
                t = t - floor_low[mid + 1] * thin_arm[0]
                thin_parts += thin_arm
            schur.append(s)
            floors.append(t)
            arms.append(jnp.concatenate(parts, axis=0) if len(parts) > 1 else parts[0])
            thin_arms.append(thin_parts)
        inverses = invert_all(schur, [0.97 * t for t in floors], steps)
        for (lo, mid, hi), v, z, thin_v, t in zip(nodes, arms, inverses, thin_arms, floors):
            thin[lo, hi] = [[a * b / t for b in thin_v] for a in thin_v]
            for a, b in ((lo, mid), (mid + 1, hi)):
                for i in range(a, b):
                    for j in range(a, b):
                        thin[lo, hi][i - lo][j - lo] += thin[a, b][i - a][j - a]
            if hi - lo == 1:
                done[lo, hi] = [z]
                continue
            w = dot(v, z)
            panels = []
            for k in range(lo, hi):
                vk = v[(k - lo) * size : (k - lo + 1) * size]
                new = w if k == mid else dot_t(w, vk)
                pieces = []
                for a, b in ((lo, mid), (mid, mid + 1), (mid + 1, hi)):
                    if a >= b:
                        continue
                    piece = new[(a - lo) * size : (b - lo) * size]
                    if a <= k < b and k != mid:
                        piece = piece + done[a, b][k - a]
                    pieces.append(piece)
                panels.append(jnp.concatenate(pieces, axis=0) if len(pieces) > 1 else pieces[0])
            done[lo, hi] = panels
    return done[0, count], thin[0, count]


def low_right(panel, low, k, plain):
    return low(k, panel, not plain, True)


def split(x):
    high = x.astype(jnp.bfloat16)
    return high, (x - high.astype(jnp.float32)).astype(jnp.bfloat16)


def dot3(a_high, a_low, b):
    b_high, b_low = split(b)
    mul = functools.partial(jnp.dot, preferred_element_type=jnp.float32)
    return mul(a_high, b_high) + (mul(a_low, b_high) + mul(a_high, b_low))


def factor_kernel(links_ref, top_ref, loss_ref, high_ref, low_ref, ends_ref, send_ref):
    levels, size = loss_ref.shape[0], loss_ref.shape[1]
    inner = levels - 1
    on_diag = eye_of(size)
    top_link, inner_link = top_ref[0:1, 0:1], jnp.full((1, 1), links_ref[inner - 1])
    links = [jnp.full((1, 1), links_ref[k]) for k in range(levels)]

    def diag_of(k):
        above = top_link if k == 0 else links[k - 1]
        return loss_ref[k] + jnp.where(on_diag, 1.0 + above + links[k], 0.0)

    def low(k, x, transposed=False, right=False):
        return links_ref[k - 1] * x

    floor_diag = [
        LEAST + links[k] + (top_link if k == 0 else links[k - 1]) for k in range(levels)
    ]
    panels, thin = dense_inverse(
        [diag_of(k) for k in range(inner)], low, floor_diag[:inner], [top_link] + links[: inner - 1]
    )
    for k, panel in enumerate(panels):
        high, rest = split(panel)
        high_ref[:, k * size : (k + 1) * size] = high
        low_ref[:, k * size : (k + 1) * size] = rest
    ends_ref[0] = top_link * panels[0]
    ends_ref[1] = inner_link * panels[-1]
    blocks = [
        (
            diag_of(inner) - inner_link * inner_link * panels[-1][-size:],
            floor_diag[inner] - inner_link * inner_link * thin[-1][-1],
        ),
        (top_link * top_link * panels[0][:size], top_link * top_link * thin[0][0]),
        (inner_link * top_link * panels[0][-size:], inner_link * top_link * thin[0][-1]),
    ]
    for k, (block, floor) in enumerate(blocks):
        send_ref[k, :size] = block
        send_ref[k, size:] = jnp.broadcast_to(floor, (8, size))


def interface(all_ref, ends_ref, high_ref, low_ref, rows_ref):
    count, size = all_ref.shape[0], all_ref.shape[3]

    def diag_of(rows, cols):
        own = [all_ref[k, 0, rows, cols] for k in range(count)]
        return [
            own[k] - all_ref[k + 1, 1, rows, cols] if k + 1 < count else own[k]
            for k in range(count)
        ]

    def low(k, x, transposed=False, right=False):
        block = all_ref[k, 2, :size]
        if right:
            return dot_t(x, block) if transposed else dot(x, block)
        return dot(block, x, ((0,), (0,))) if transposed else dot(block, x)

    thin = slice(size, size + 1), slice(0, 1)
    panels, _ = dense_inverse(
        diag_of(slice(0, size), slice(0, size)),
        low,
        diag_of(*thin),
        [all_ref[k, 2, thin[0], thin[1]] for k in range(count)],
        enough_steps(spread(size)),
    )
    for k, panel in enumerate(panels):
        rows_ref[k] = panel
    me = lax.axis_index("lev")
    own = rows_ref[me]
    above = rows_ref[jnp.maximum(me - 1, 0)]
    inner = dot_t(ends_ref[0], above) + dot_t(ends_ref[1], own)
    length = inner.shape[0]
    high_ref[:length], low_ref[:length] = split(inner)
    high_ref[length:], low_ref[length:] = split(own.T)


def send(src, dst, sems, slot, device):
    return pltpu.make_async_remote_copy(
        src_ref=src,
        dst_ref=dst,
        send_sem=sems.at[0, slot],
        recv_sem=sems.at[1, slot],
        device_id=device,
        device_id_type=pl.DeviceIdType.MESH,
    )


def greet(lev_all, lon_all):
    barrier = pltpu.get_barrier_semaphore()
    partners = []
    for axis, everyone in (("lev", lev_all), ("lon", lon_all)):
        count, me = lax.axis_size(axis), lax.axis_index(axis)
        if everyone is None:
            continue
        steps = range(1, count) if everyone else sorted({1, count - 1})
        partners += [{axis: lax.rem(me + d, count)} for d in steps if d % count]
    for device in partners:
        pl.semaphore_signal(
            barrier, inc=1, device_id=device, device_id_type=pl.DeviceIdType.MESH
        )
    pl.semaphore_wait(barrier, len(partners))


def pack_edges(cur_ref, edges_ref):
    levels, size, columns = cur_ref.shape
    lane = lax.broadcasted_iota(jnp.int32, (size, 128), 1)
    last = jnp.zeros((size, 128), jnp.float32)
    first = last
    for k in range(levels):
        tail = pltpu.roll(cur_ref[k, :, columns - 128 :], k + 1, 1)
        head = cur_ref[k, :, :128]
        head = pltpu.roll(head, k, 1) if k else head
        last = jnp.where(lane == k, tail, last)
        first = jnp.where(lane == k, head, first)
    edges_ref[0] = last
    edges_ref[1] = first


def halo_copies(edges_ref, halo_ref, sems):
    around, me = lax.axis_size("lon"), lax.axis_index("lon")
    return [
        send(edges_ref.at[0], halo_ref.at[0], sems, 0, {"lon": lax.rem(me + 1, around)}),
        send(edges_ref.at[1], halo_ref.at[1], sems, 1, {"lon": lax.rem(me + around - 1, around)}),
    ]


def local_forcing(mix_ref, cur_ref, prev_ref, pair_ref, force_ref):
    levels, size, columns = cur_ref.shape
    lane = lax.broadcasted_iota(jnp.int32, (size, columns), 1)
    for k in range(levels):
        c = cur_ref[k]
        back = jnp.where(lane == 0, 0.0, pltpu.roll(c, 1, 1))
        ahead = jnp.where(lane == columns - 1, 0.0, pltpu.roll(c, columns - 1, 1))
        p_high, p_low = split(pair_ref[k])
        chem = dot3(p_high, p_low, c * c)
        force_ref[k * size : (k + 1) * size] = (
            prev_ref[k] - chem + mix_ref[k] * (back + ahead - 2.0 * c)
        )


def add_halo(mix_ref, halo_ref, force_ref):
    levels = mix_ref.shape[0]
    size, columns = halo_ref.shape[1], force_ref.shape[1]
    lane = lax.broadcasted_iota(jnp.int32, (size, 128), 1)
    before, after = halo_ref[0], halo_ref[1]
    for k in range(levels):
        rows = slice(k * size, (k + 1) * size)
        at_head = pltpu.roll(before, 128 - k, 1) if k else before
        at_tail = pltpu.roll(after, 127 - k, 1)
        force_ref[rows, :128] += jnp.where(lane == 0, mix_ref[k] * at_head, 0.0)
        force_ref[rows, columns - 128 :] += jnp.where(lane == 127, mix_ref[k] * at_tail, 0.0)


def couple(
    links_ref, top_link, g_high, g_low, force_ref, part_ref, f_high, f_low, top_out, top_in, sides_ref,
    sems, direct,
):
    count, me = lax.axis_size("lev"), lax.axis_index("lev")
    inner, size = part_ref.shape[0], top_out.shape[0]
    f_high[...], f_low[...] = split(force_ref[:inner])
    mul = functools.partial(jnp.dot, preferred_element_type=jnp.float32)

    def rows_of(start, stop):
        a, b = g_high[start:stop], g_low[start:stop]
        part = mul(a, f_high[...]) + (mul(b, f_high[...]) + mul(a, f_low[...]))
        part_ref[start:stop] = part
        return part

    top_out[...] = top_link * rows_of(0, size)
    sides_ref[me] = force_ref[inner:] + links_ref[inner // size - 1] * rows_of(inner - size, inner)
    up = send(top_out, top_in, sems, 0, {"lev": lax.rem(me + count - 1, count)})
    half = size * ((inner // size) // 2)

    @pl.when(me > 0)
    def _():
        up.start()

    rows_of(size, half)

    @pl.when(me < count - 1)
    def _():
        up.wait_recv()
        sides_ref[me] += top_in[...]

    partner = me + 1 - 2 * lax.rem(me, 2)
    copies = [
        send(sides_ref.at[me], sides_ref.at[me], sems, d, {"lev": lax.rem(me + d, count)})
        for d in range(1 if direct else 2, count, 1 if direct else 2)
    ]
    onward = [] if direct else [send(sides_ref.at[me], sides_ref.at[me], sems, 1, {"lev": partner})]
    for d in range(count if direct else 2, count, 2):
        origin = lax.rem(me - d + count, count)
        onward.append(
            send(sides_ref.at[origin], sides_ref.at[origin], sems, d + 1, {"lev": partner})
        )
    for copy in copies + onward[:1]:
        copy.start()
    rows_of(half, inner - size)

    @pl.when(me > 0)
    def _():
        up.wait_send()

    return copies, onward


def relay(copies, onward):
    for copy, later in zip(copies, onward[1:]):
        copy.wait_recv()
        later.start()
    for copy in copies:
        copy.wait_send()
    for copy in onward:
        copy.wait()


def finish(part_ref, sides_ref, high_ref, low_ref, out_ref):
    levels, size, columns = out_ref.shape
    count = sides_ref.shape[0]
    b_high, b_low = split(sides_ref[...].reshape(count * size, columns))
    mul = functools.partial(jnp.dot, preferred_element_type=jnp.float32)
    for k in range(levels):
        rows = slice(k * size, (k + 1) * size)
        a, b = high_ref[rows], low_ref[rows]
        row = mul(a, b_high) + (mul(b, b_high) + mul(a, b_low))
        out_ref[k] = row + part_ref[rows] if k < levels - 1 else row


def open_kernel(
    links_ref, mix_ref, prev_ref, pair_ref, force_ref, top_ref, edges, halo, link_out, sems
):
    levels = prev_ref.shape[0]
    count, me = lax.axis_size("lev"), lax.axis_index("lev")
    pack_edges(prev_ref, edges)
    link_out[...] = jnp.full(link_out.shape, links_ref[levels - 1], jnp.float32)
    greet(False, False)
    copies = halo_copies(edges, halo, sems)
    down = send(link_out, top_ref, sems, 2, {"lev": lax.rem(me + 1, count)})
    for copy in copies:
        copy.start()

    @pl.when(me < count - 1)
    def _():
        down.start()

    @pl.when(me == 0)
    def _():
        top_ref[...] = jnp.zeros(top_ref.shape, jnp.float32)

    local_forcing(mix_ref, prev_ref, prev_ref, pair_ref, force_ref)
    for copy in copies:
        copy.wait()
    add_halo(mix_ref, halo, force_ref)

    @pl.when(me < count - 1)
    def _():
        down.wait_send()

    @pl.when(me > 0)
    def _():
        down.wait_recv()


def newton_kernel(
    links_ref, mix_ref, top_ref, sent_ref, ends_ref, first_force, g_high, g_low, prev_ref, pair_ref,
    out_ref, var_ref, all_ref, rows_ref, h_high, h_low, cur_ref, edges, halo, force_ref, part_ref,
    first_sides, sides_ref, f_high, f_low, first_out, first_in, top_out, top_in, sums_ref,
    block_sems, first_sems, halo_sems, sems, sum_sems,
):
    levels, size, columns = prev_ref.shape
    count, me = lax.axis_size("lev"), lax.axis_index("lev")
    around, place = lax.axis_size("lon"), lax.axis_index("lon")
    greet(True, True)
    blocks = [
        send(sent_ref, all_ref.at[me], block_sems, d, {"lev": lax.rem(me + d, count)})
        for d in range(1, count)
    ]
    for copy in blocks:
        copy.start()
    all_ref[me] = sent_ref[...]
    copies = couple(
        links_ref, top_ref[0:1, 0:1], g_high, g_low, first_force, part_ref, f_high, f_low,
        first_out, first_in, first_sides, first_sems, True,
    )
    for copy in blocks:
        copy.wait()
    interface(all_ref, ends_ref, h_high, h_low, rows_ref)
    for copy in copies[0]:
        copy.wait()
    finish(part_ref, first_sides, h_high, h_low, cur_ref)
    pack_edges(cur_ref, edges)
    copies = halo_copies(edges, halo, halo_sems)
    for copy in copies:
        copy.start()
    local_forcing(mix_ref, cur_ref, prev_ref, pair_ref, force_ref)
    for copy in copies:
        copy.wait()
    add_halo(mix_ref, halo, force_ref)
    copies = couple(
        links_ref, top_ref[0:1, 0:1], g_high, g_low, force_ref, part_ref, f_high, f_low,
        top_out, top_in, sides_ref, sems, False,
    )
    relay(*copies)
    finish(part_ref, sides_ref, h_high, h_low, out_ref)
    lane = lax.broadcasted_iota(jnp.int32, (size, 128), 1)
    total = jnp.zeros((size, 128), jnp.float32)
    for k in range(levels):
        row = out_ref[k]
        total = jnp.where(lane == k, jnp.sum(row * row, axis=1, keepdims=True), total)
    sums_ref[0] = total.T[: sums_ref.shape[1]]
    copies = [
        send(sums_ref.at[0], sums_ref.at[d], sum_sems, d, {"lon": lax.rem(place + d, around)})
        for d in range(1, around)
    ]
    for copy in copies:
        copy.start()
    for copy in copies:
        copy.wait()
    total = sums_ref[place]
    for j in range(1, around):
        total = total + sums_ref[lax.rem(place - j + around, around)]
    var_ref[...] = (total / (columns * around))[:levels]


def call(kernel, outs, places, scratch=(), group=None):
    extra = {} if group is None else {"collective_id": group, "has_side_effects": True}
    return pl.pallas_call(
        kernel,
        out_shape=[jax.ShapeDtypeStruct(shape, dtype) for shape, dtype in outs],
        in_specs=places,
        out_specs=[VMEM] * len(outs),
        scratch_shapes=list(scratch),
        compiler_params=pltpu.CompilerParams(vmem_limit_bytes=60 * 2**20, **extra),
    )


def local(previous, loss_matrix, pair_matrix, diffusivity, mixing):
    levels, size, columns = previous.shape
    count = lax.axis_size("lev")
    around = lax.axis_size("lon")
    inner = (levels - 1) * size
    f32, bf16 = jnp.float32, jnp.bfloat16
    buf, sem = pltpu.VMEM, lambda n: pltpu.SemaphoreType.DMA((2, n))
    force, top = call(
        open_kernel,
        [((levels * size, columns), f32), ((8, 128), f32)],
        [SMEM, SMEM, VMEM, VMEM],
        [buf((2, size, 128), f32), buf((2, size, 128), f32), buf((8, 128), f32), sem(3)],
        0,
    )(diffusivity, mixing, previous, pair_matrix)
    g_high, g_low, ends, sent = call(
        factor_kernel,
        [((inner, inner), bf16), ((inner, inner), bf16), ((2, inner, size), f32), ((3, size + 8, size), f32)],
        [SMEM, VMEM, VMEM],
    )(diffusivity, top, loss_matrix)
    return call(
        newton_kernel,
        [((levels, size, columns), f32), ((levels, size), f32)],
        [SMEM, SMEM] + [VMEM] * 8,
        [
            buf((count, 3, size + 8, size), f32),
            buf((count, count * size, size), f32),
            buf((levels * size, count * size), bf16),
            buf((levels * size, count * size), bf16),
            buf((levels, size, columns), f32),
            buf((2, size, 128), f32),
            buf((2, size, 128), f32),
            buf((levels * size, columns), f32),
            buf((inner, columns), f32),
            buf((count, size, columns), f32),
            buf((count, size, columns), f32),
            buf((inner, columns), bf16),
            buf((inner, columns), bf16),
            buf((size, columns), f32),
            buf((size, columns), f32),
            buf((size, columns), f32),
            buf((size, columns), f32),
            buf((around, -(-levels // 8) * 8, size), f32),
            sem(count),
            sem(count),
            sem(2),
            sem(count),
            sem(around),
        ],
        1,
    )(diffusivity, mixing, top, sent, ends, force, g_high, g_low, previous, pair_matrix)


def cat3(a_high, a_low, b_high, b_low):
    return jnp.dot(
        jnp.concatenate([a_high, a_low, a_high], axis=1),
        jnp.concatenate([b_high, b_high, b_low], axis=0),
        preferred_element_type=jnp.float32,
    )


def wide(a):
    high, low = split(a)
    return jnp.concatenate([high, low, high, jnp.zeros_like(high)], axis=1)


def tall(b):
    high, low = split(b)
    return jnp.concatenate([high, high, low, jnp.zeros_like(high)], axis=0)


def wide_dot(a, b):
    return jnp.dot(a, b, preferred_element_type=jnp.float32)


def pull(links, loss):
    stiff = links[0]
    for a in links[1:]:
        own = 1.0 + loss + stiff
        stiff = a * own / (a + own)
    return stiff


def worst_ratio(above, below):
    sides = []
    for count in (above, below):
        draws = itertools.product((200.0, 2000.0), repeat=min(count, 8) + 1)
        sides.append([(pull(d, 640.0), pull(d, 0.05)) for d in draws])
    return 1.15 * max((641.0 + a + c) / (1.05 + b + d) for a, b in sides[0] for c, d in sides[1])


def gains_for(ratio):
    rho, gains = (ratio - 1.0) / (ratio + 1.0), []
    while rho > 1.5e-4:
        gains.append(2.0 / (2.0 - rho * rho))
        rho = rho * rho / (2.0 - rho * rho)
    return gains


def invert_fixed(blocks, floors, ratio):
    size = blocks[0].shape[0]
    unit = jnp.where(eye_of(size), 1.0, 0.0).astype(jnp.float32)
    gains = gains_for(ratio)
    xs, rests = [], []
    for a, low in zip(blocks, floors):
        scale = (2.0 / (1.0 + ratio)) / low
        rest = unit - scale * a
        xs.append((gains[0] * scale) * (unit + rest))
        rests.append(rest)
    rests = [gains[0] * dot(r, r) - (gains[0] - 1.0) * unit for r in rests]
    for step, g in enumerate(gains[1:]):
        if step + 2 == len(gains):
            xs = [g * (x + dot(x, r)) for x, r in zip(xs, rests)]
            break
        both = [dot(jnp.concatenate([x, r], axis=0), r) for x, r in zip(xs, rests)]
        xs = [g * (x + b[:size]) for x, b in zip(xs, both)]
        rests = [g * b[size:] - (g - 1.0) * unit for b in both]
    rests = [unit - dot(a, x) for a, x in zip(blocks, xs)]
    return [x + dot(x, r) for x, r in zip(xs, rests)]


def chain_factor(diag, links, floors, panel_ref, hook):
    count, size = len(diag), diag[0].shape[0]
    unit = jnp.where(eye_of(size), 1.0, 0.0).astype(jnp.float32)
    by_depth, thin = {}, {}
    plan(0, count, by_depth)

    def rows(lo, hi):
        return slice(lo * size, hi * size)

    for depth in sorted(by_depth):
        nodes = by_depth[depth]
        ratio = max(worst_ratio(mid - lo, hi - 1 - mid) for lo, mid, hi in nodes)
        schur, arms, lows, thin_arms = [], [], [], []
        for lo, mid, hi in nodes:
            s, parts = diag[mid], []
            t, thin_parts = floors[mid], []
            if lo < mid:
                arm = links[mid] * panel_ref[mid - 1, rows(lo, mid)]
                s = s - links[mid] * arm[-size:]
                parts.append(arm)
                thin_parts += [links[mid] * x for x in thin[lo, mid][-1]]
                t = t - links[mid] * thin_parts[-1]
            parts.append(unit)
            thin_parts.append(1.0)
            if mid + 1 < hi:
                arm = links[mid + 1] * panel_ref[mid + 1, rows(mid + 1, hi)]
                s = s - links[mid + 1] * arm[:size]
                parts.append(arm)
                thin_arm = [links[mid + 1] * x for x in thin[mid + 1, hi][0]]
                t = t - links[mid + 1] * thin_arm[0]
                thin_parts += thin_arm
            schur.append(s)
            lows.append(t)
            arms.append(jnp.concatenate(parts, axis=0) if len(parts) > 1 else parts[0])
            thin_arms.append(thin_parts)
        inverses = invert_fixed(schur, [0.97 * t for t in lows], ratio)
        for (lo, mid, hi), v, z, thin_v, t in zip(nodes, arms, inverses, thin_arms, lows):
            thin[lo, hi] = [[a * b / t for b in thin_v] for a in thin_v]
            for a, b in ((lo, mid), (mid + 1, hi)):
                for i in range(a, b):
                    for j in range(a, b):
                        thin[lo, hi][i - lo][j - lo] += thin[a, b][i - a][j - a]
            if hi - lo == 1:
                panel_ref[mid, rows(mid, hi)] = z
                continue
            w = dot(v, z)
            if hi - lo == count:
                continue
            new = dot_t(w, v)
            for k in range(lo, hi):
                own = new[:, (k - lo) * size : (k - lo + 1) * size]
                panel_ref[k, rows(mid, mid + 1)] = own[rows(mid - lo, mid - lo + 1)]
                for a, b in ((lo, mid), (mid + 1, hi)):
                    if a >= b:
                        continue
                    piece = own[rows(a - lo, b - lo)]
                    if a <= k < b:
                        piece = piece + panel_ref[k, rows(a, b)]
                    panel_ref[k, rows(a, b)] = piece
        if depth < max(by_depth):
            hook(depth)
    return v, w, by_depth[max(by_depth)][0][1], thin[0, count]


def fold(x):
    half = x.shape[0] // 2
    return jnp.concatenate([x[:half], x[half:]], axis=1)


def unfold(x):
    half = x.shape[1] // 2
    return jnp.concatenate([x[:, :half], x[:, half:]], axis=0)


def pack_pairs(field_ref, columns, edges_ref):
    levels, size = field_ref.shape[:2]
    lane = lax.broadcasted_iota(jnp.int32, (size, 128), 1)
    last = jnp.zeros((size, 128), jnp.float32)
    first = last
    for k in range(levels):
        tail = pltpu.roll(field_ref[k, :, columns - 128 : columns], (2 * k + 2) % 128, 1)
        head = field_ref[k, :, :128]
        head = pltpu.roll(head, 2 * k, 1) if k else head
        mine = (lane == 2 * k) | (lane == 2 * k + 1)
        last = jnp.where(mine, tail, last)
        first = jnp.where(mine, head, first)
    edges_ref[0] = last
    edges_ref[1] = first


def unpack_pairs(halo_ref, columns, field_ref):
    levels, size = field_ref.shape[:2]
    lane = lax.broadcasted_iota(jnp.int32, (size, 128), 1)
    before, after = halo_ref[0], halo_ref[1]
    for k in range(levels):
        at_head = pltpu.roll(after, (128 - 2 * k) % 128, 1) if k else after
        at_tail = pltpu.roll(before, (126 - 2 * k) % 128, 1)
        field_ref[k, :, columns:] = jnp.where(lane < 2, at_head, jnp.where(lane >= 126, at_tail, 0.0))


def forcing(mix_ref, cur_ref, prev_ref, pairs_ref, width, sep_ref, f_high, f_low):
    levels, size, full = cur_ref.shape
    for k in range(levels):
        c = cur_ref[k]
        ring = pltpu.roll(c, 1, 1) + pltpu.roll(c, full - 1, 1)
        own = c[:, :width]
        chem = wide_dot(pairs_ref[k], tall(own * own))
        force = prev_ref[k, :, :width] - chem + mix_ref[k] * (ring[:, :width] - 2.0 * own)
        if k == 0:
            sep_ref[:, :width] = force
        else:
            rows = slice((k - 1) * size, k * size)
            f_high[rows, :width], f_low[rows, :width] = split(force)


def start_all(copies):
    @pl.when(lax.axis_index("lev") < lax.axis_size("lev"))
    def _():
        for copy in copies:
            copy.start()


def step_kernel(
    links_ref, mix_ref, loss_hbm, prev_hbm, pair_hbm, out_ref, var_ref,
    loss_ref, prev_ref, pair_ref, pairs_ref, edges, halo, z_high, z_low, send_ref, all_ref,
    ends_high, ends_low, table_ref, sep_ref, f_high, f_low, part_ref, own_ref, near_ref, mine_ref, far_ref,
    side_high, side_low, hq_high, hq_low, u_ref, top_ref, cur_ref, sums_ref, panel_ref,
    load_sems, halo_sems, block_sems, near_sems, far_sems, sum_sems,
):
    levels, size, columns = prev_hbm.shape
    inner = levels - 1
    full = cur_ref.shape[2]
    count, me = lax.axis_size("lev"), lax.axis_index("lev")
    around, place = lax.axis_size("lon"), lax.axis_index("lon")
    core, chip = lax.rem(me, 2), me // 2
    partner = me + 1 - 2 * core
    across = lax.rem(me + 2, count)

    loads = [
        pltpu.make_async_copy(loss_hbm, loss_ref, load_sems.at[0]),
        pltpu.make_async_copy(prev_hbm, prev_ref.at[:, :, pl.ds(0, columns)], load_sems.at[1]),
        pltpu.make_async_copy(pair_hbm, pair_ref, load_sems.at[2]),
    ]
    for load in loads:
        load.start()
    barrier = pltpu.get_barrier_semaphore()
    partners = [{"lev": lax.rem(me + d, count)} for d in range(1, count)]
    partners += [{"lon": lax.rem(place + d, around)} for d in range(1, around)]
    for device in partners:
        pl.semaphore_signal(barrier, inc=1, device_id=device, device_id_type=pl.DeviceIdType.MESH)

    links = [jnp.full((1, 1), links_ref[k]) for k in range(levels)]
    on_diag = eye_of(size)
    halo_moves = halo_copies(edges, halo, halo_sems)

    def hook(depth):
        if depth != 2:
            return
        loads[1].wait()
        pack_pairs(prev_ref, columns, edges)
        pl.semaphore_wait(barrier, len(partners))
        start_all(halo_moves)

    loads[0].wait()
    diag = [
        loss_ref[k] + jnp.where(on_diag, 1.0 + links[k] + (links[k - 1] if k else 0.0), 0.0)
        for k in range(levels)
    ]
    floors = [LEAST + links[k] + (links[k - 1] if k else 0.0) for k in range(levels)]
    v, w, mid, thin = chain_factor(diag[1:], links[:inner], floors[1:], panel_ref, hook)
    a, b = links[0], links[inner]
    old = [
        panel_ref[0, : mid * size],
        jnp.zeros((size, size), jnp.float32),
        panel_ref[inner - 1, (mid + 1) * size :],
    ]
    tips = dot_t(w, jnp.concatenate([v[:size], v[-size:]], axis=0))
    first = tips[:, :size] + jnp.concatenate([old[0], old[1], jnp.zeros_like(old[2])], axis=0)
    last = tips[:, size:] + jnp.concatenate([jnp.zeros_like(old[0]), old[1], old[2]], axis=0)
    sub = lax.broadcasted_iota(jnp.int32, (8, 128), 0)
    send_ref[: size // 2] = fold(diag[0] - a * a * first[:size])
    send_ref[size // 2 : size] = fold(jnp.where(on_diag, b, 0.0) - b * b * last[-size:])
    send_ref[size : 3 * size // 2] = fold(a * b * first[-size:])
    send_ref[3 * size // 2 :] = jnp.where(
        sub == 0, floors[0] - a * a * thin[0][0], jnp.where(sub == 1, b - b * b * thin[-1][-1], a * b * thin[0][-1])
    )
    blocks = [
        send(send_ref, all_ref.at[me], block_sems, d, {"lev": lax.rem(me + d, count)})
        for d in range(1, count)
    ]
    start_all(blocks)
    all_ref[me] = send_ref[...]

    ends_high[...], ends_low[...] = split(jnp.concatenate([a * first, b * last], axis=1))
    w_wide, (v_high, v_low) = wide(w), split(v)
    v_wide = jnp.concatenate([v_high, v_high, v_low, jnp.zeros_like(v_high)], axis=1)
    for k in range(0, inner, 2):
        new = lax.dot_general(
            w_wide, v_wide[k * size : (k + 2) * size], (((1,), (1,)), ((), ())), preferred_element_type=jnp.float32
        )
        for lo, hi in ((0, mid), (mid, mid + 1), (mid + 1, inner)):
            piece = new[lo * size : hi * size]
            if lo != mid and (lo <= k < hi or lo <= k + 1 < hi):
                old = [
                    panel_ref[j, lo * size : hi * size] if lo <= j < hi else jnp.zeros((piece.shape[0], size), jnp.float32)
                    for j in (k, k + 1)
                ]
                piece = piece + jnp.concatenate(old, axis=1)
            spot = slice(lo * size, hi * size), slice(k * size, (k + 2) * size)
            z_high[spot], z_low[spot] = split(piece)
    loads[2].wait()
    for k in range(levels):
        pairs_ref[k] = wide(pair_ref[k])
    for move in halo_moves:
        move.wait()
    unpack_pairs(halo, columns, prev_ref)

    def z_rows(start, stop, width):
        return cat3(z_high[start:stop], z_low[start:stop], f_high[:, :width], f_low[:, :width])

    def ends(turn, width):
        rows = cat3(
            jnp.concatenate([z_high[:size], z_high[-size:]], axis=0),
            jnp.concatenate([z_low[:size], z_low[-size:]], axis=0),
            f_high[:, :width],
            f_low[:, :width],
        )
        part_ref[:size, :width] = rows[:size]
        part_ref[-size:, :width] = rows[size:]
        own_ref[turn, 0, :, :width] = sep_ref[:, :width] + a * rows[:size]
        own_ref[turn, 1, :, :width] = b * rows[size:]
        copy = send(
            own_ref.at[turn, :, :, pl.ds(0, width)], near_ref.at[turn, :, :, pl.ds(0, width)], near_sems, turn,
            {"lev": partner},
        )
        start_all([copy])
        return copy

    def middle(width):
        for k in range(1, inner - 1):
            part_ref[k * size : (k + 1) * size, :width] = z_rows(k * size, (k + 1) * size, width)

    def merge(turn, width):
        upper = core == 0
        s_own, t_own = own_ref[turn, 0, :, :width], own_ref[turn, 1, :, :width]
        s_in, t_in = near_ref[turn, 0, :, :width], near_ref[turn, 1, :, :width]
        low_side = jnp.where(upper, s_own, s_in)
        high_side = jnp.where(upper, s_in + t_own, s_own + t_in)
        side_high[:size, :width], side_low[:size, :width] = split(low_side)
        side_high[size:, :width], side_low[size:, :width] = split(high_side)
        return jnp.where(chip == 0, jnp.where(upper, t_in, t_own), 0.0)

    def condense(turn, width, tail, k_high, k_low):
        mine_ref[turn, :, :width] = tail + cat3(k_high, k_low, side_high[:, :width], side_low[:, :width])
        copy = send(
            mine_ref.at[turn, :, pl.ds(0, width)], far_ref.at[turn, :, pl.ds(0, width)], far_sems, turn,
            {"lev": across},
        )
        start_all([copy])
        return copy

    def gather_sides(width):
        for k in range(levels):
            spot = slice(k * size, (k + 1) * size)
            rows = cat3(hq_high[spot], hq_low[spot], side_high[:, :width], side_low[:, :width])
            cur_ref[k, :, :width] = rows if k == 0 else rows + part_ref[(k - 1) * size : k * size, :width]

    def finish(turn, width, to_ref):
        total = mine_ref[turn, :, :width] + far_ref[turn, :, :width]
        top = tall(wide_dot(top_ref[...], tall(total)))
        for k in range(levels):
            to_ref[k, :, :width] = cur_ref[k, :, :width] + wide_dot(u_ref[k * size : (k + 1) * size], top)

    forcing(mix_ref, prev_ref, prev_ref, pairs_ref, full, sep_ref, f_high, f_low)
    near = ends(0, full)
    middle(full)
    for copy in blocks:
        copy.wait()

    def block(k, which):
        return unfold(all_ref[k, which * size // 2 : (which + 1) * size // 2])

    def floor(k, which):
        row = 3 * size // 2 + which
        return all_ref[k, row : row + 1, 0:1]

    ratio = spread(size)
    s = [block(k, 0) + (block(k - 1, 1) if k else 0.0) for k in range(count)]
    t = [floor(k, 0) + (floor(k - 1, 1) if k else 0.0) for k in range(count)]
    c = [None] + [block(k, 2) for k in range(count - 1)]
    e = [None] + [floor(k, 2) for k in range(count - 1)]
    z0, z3 = invert_fixed([s[0], s[3]], [0.97 * t[0], 0.97 * t[3]], ratio)
    a1, a3 = dot(c[1], z0), dot(z3, c[3])
    s1 = s[1] - dot_t(a1, c[1])
    t1 = t[1] - e[1] * e[1] / t[0]
    (z1,) = invert_fixed([s1], [0.97 * t1], ratio)
    a2 = dot(c[2], z1)
    s2 = s[2] - dot_t(a2, c[2]) - dot(c[3], a3, ((0,), (0,)))
    t2 = t[2] - e[2] * e[2] / t1 - e[3] * e[3] / t[3]
    b1 = dot(z1, a1)
    p0 = dot(a2, a1)
    zero = jnp.zeros((size, size), jnp.float32)
    unit = jnp.where(on_diag, 1.0, 0.0).astype(jnp.float32)
    sides = [
        (z0 + dot(a1, b1, ((0,), (0,))), b1.T, p0.T),
        (b1, z1, a2.T),
        (zero, zero, unit),
        (zero, z3, a3),
        (zero, zero, zero),
    ]
    for k, (left, right, top) in enumerate(sides):
        table_ref[k, :size] = jnp.concatenate([left, right], axis=1)
        table_ref[k, size:, :size] = top
    for k, (left, right) in enumerate(((p0, a2), (unit, a3.T))):
        table_ref[len(sides) + k, :size] = jnp.concatenate([left, right], axis=1)
    near.wait()
    tail = merge(0, full)
    k_high, k_low = split(table_ref[len(sides) + chip, :size])
    far = condense(0, full, tail, k_high, k_low)
    (z2,) = invert_fixed([s2], [0.97 * t2], ratio)
    top_ref[...] = wide(z2)
    own_q, next_q = table_ref[me, :size], table_ref[me + 1, :size]
    own_p, next_p = table_ref[me, size:, :size], table_ref[me + 1, size:, :size]
    q_high, q_low = split(jnp.concatenate([own_q, next_q], axis=0))
    p_high, p_low = split(jnp.concatenate([own_p, next_p], axis=0))
    hq_high[size:], hq_low[size:] = split(cat3(ends_high[...], ends_low[...], q_high, q_low))
    hq_high[:size], hq_low[:size] = split(own_q)
    u_ref[size:] = wide(cat3(ends_high[...], ends_low[...], p_high, p_low))
    u_ref[:size] = wide(own_p)
    gather_sides(full)
    far.wait()
    finish(0, full, cur_ref)

    forcing(mix_ref, cur_ref, prev_ref, pairs_ref, columns, sep_ref, f_high, f_low)
    near = ends(1, columns)
    middle(columns)
    near.wait()
    tail = merge(1, columns)
    far = condense(1, columns, tail, k_high, k_low)
    gather_sides(columns)
    far.wait()
    finish(1, columns, out_ref)
    lane = lax.broadcasted_iota(jnp.int32, (size, 128), 1)
    total = jnp.zeros((size, 128), jnp.float32)
    for k in range(levels):
        row = out_ref[k]
        total = jnp.where(lane == k, jnp.sum(row * row, axis=1, keepdims=True), total)
    sums_ref[0] = total.T[: sums_ref.shape[1]]
    copies = [
        send(sums_ref.at[0], sums_ref.at[d], sum_sems, d, {"lon": lax.rem(place + d, around)})
        for d in range(1, around)
    ]
    start_all(copies)
    for copy in copies:
        copy.wait()
    total = sums_ref[place]
    for j in range(1, around):
        total = total + sums_ref[lax.rem(place - j + around, around)]
    var_ref[...] = (total / (columns * around))[:levels]


def local_pairs(previous, loss_matrix, pair_matrix, diffusivity, mixing):
    levels, size, columns = previous.shape
    count, around = lax.axis_size("lev"), lax.axis_size("lon")
    inner, full = (levels - 1) * size, columns + 128
    f32, bf16 = jnp.float32, jnp.bfloat16
    buf, sem = pltpu.VMEM, lambda n: pltpu.SemaphoreType.DMA((2, n))
    hbm = pl.BlockSpec(memory_space=pltpu.MemorySpace.HBM)
    packed = 3 * size // 2 + 8
    return pl.pallas_call(
        step_kernel,
        out_shape=[
            jax.ShapeDtypeStruct((levels, size, columns), f32),
            jax.ShapeDtypeStruct((levels, size), f32),
        ],
        in_specs=[SMEM, SMEM, hbm, hbm, hbm],
        out_specs=[VMEM, VMEM],
        scratch_shapes=[
            buf((levels, size, size), f32),
            buf((levels, size, full), f32),
            buf((levels, size, size), f32),
            buf((levels, size, 4 * size), bf16),
            buf((2, size, 128), f32),
            buf((2, size, 128), f32),
            buf((inner, inner), bf16),
            buf((inner, inner), bf16),
            buf((packed, 2 * size), f32),
            buf((count, packed, 2 * size), f32),
            buf((inner, 2 * size), bf16),
            buf((inner, 2 * size), bf16),
            buf((count + 3, 2 * size, 2 * size), f32),
            buf((size, full), f32),
            buf((inner, full), bf16),
            buf((inner, full), bf16),
            buf((inner, full), f32),
            buf((2, 2, size, full), f32),
            buf((2, 2, size, full), f32),
            buf((2, size, full), f32),
            buf((2, size, full), f32),
            buf((2 * size, full), bf16),
            buf((2 * size, full), bf16),
            buf((levels * size, 2 * size), bf16),
            buf((levels * size, 2 * size), bf16),
            buf((levels * size, 4 * size), bf16),
            buf((size, 4 * size), bf16),
            buf((levels, size, full), f32),
            buf((around, -(-levels // 8) * 8, size), f32),
            buf((levels - 1, inner, size), f32),
            pltpu.SemaphoreType.DMA((3,)),
            sem(2),
            sem(count),
            sem(2),
            sem(2),
            sem(around),
        ],
        compiler_params=pltpu.CompilerParams(
            vmem_limit_bytes=40 * 2**20, collective_id=2, has_side_effects=True
        ),
    )(diffusivity, mixing, loss_matrix, previous, pair_matrix)


def solution(mesh):
    placed = (P("lev", None, "lon"), P("lev", None, None), P("lev", None, None), P("lev"), P("lev"))
    return jax.shard_map(
        local_pairs if mesh.shape["lev"] == 4 else local,
        mesh=mesh,
        in_specs=placed,
        out_specs=(P("lev", None, "lon"), P("lev", None)),
        check_vma=False,
    )
```

```python
import functools
import itertools

import jax
import jax.numpy as jnp
from jax import lax
from jax.experimental import pallas as pl
from jax.experimental.pallas import tpu as pltpu
from jax.sharding import PartitionSpec as P

LEAST = 1.05
MOST = 10.0
HIGHEST = lax.Precision.HIGHEST
SMEM = pl.BlockSpec(memory_space=pltpu.SMEM)
VMEM = pl.BlockSpec(memory_space=pltpu.VMEM)


def dot(a, b, dims=((1,), (0,))):
    return lax.dot_general(
        a, b, (dims, ((), ())), precision=HIGHEST, preferred_element_type=jnp.float32
    )


def dot_t(a, b):
    return dot(a, b, ((1,), (1,)))


def eye_of(size):
    rows = lax.broadcasted_iota(jnp.int32, (size, size), 0)
    cols = lax.broadcasted_iota(jnp.int32, (size, size), 1)
    return rows == cols


def invert_all(blocks, floors, steps):
    size = blocks[0].shape[0]
    unit = jnp.where(eye_of(size), 1.0, 0.0).astype(jnp.float32)
    start, worst = [], None
    for a, lo in zip(blocks, floors):
        hi = jnp.max(jnp.sum(jnp.abs(a), axis=0, keepdims=True), axis=1, keepdims=True)
        hi = jnp.clip(hi, lo, lo * spread(size))
        scale = 2.0 / (hi + lo)
        rho = (hi - lo) / (hi + lo)
        start.append((scale, a))
        worst = rho if worst is None else jnp.maximum(worst, rho)

    def grow(rho):
        square = rho * rho
        return square / (2.0 - square), 2.0 / (2.0 - square)

    rho, gain = grow(worst)
    start = [(gain * scale) * (2.0 * unit - scale * a) for scale, a in start]

    def step(carry):
        rho, *xs = carry
        rest = [unit - dot(a, x) for a, x in zip(blocks, xs)]
        rho, gain = grow(rho)
        return (rho, *[gain * (x + dot(x, r)) for x, r in zip(xs, rest)])

    if steps is None:
        return lax.while_loop(lambda carry: jnp.max(carry[0]) > 3e-8, step, (rho, *start))[1:]
    return lax.fori_loop(0, steps, lambda i, carry: step(carry), (rho, *start))[1:]


def spread(size):
    return (1.0 + MOST * size) / (0.96 * LEAST)


def enough_steps(condition):
    rho, steps = (condition - 1.0) / (condition + 1.0), -1
    while rho > 3e-8:
        rho, steps = rho * rho / (2.0 - rho * rho), steps + 1
    return steps


def plan(lo, hi, out):
    if lo >= hi:
        return 0
    mid = lo + (hi - lo) // 2
    depth = 1 + max(plan(lo, mid, out), plan(mid + 1, hi, out))
    out.setdefault(depth, []).append((lo, mid, hi))
    return depth


def dense_inverse(diag, low, floor_diag, floor_low, steps=None):
    count, size = len(diag), diag[0].shape[0]
    unit = jnp.where(eye_of(size), 1.0, 0.0).astype(jnp.float32)
    by_depth, done, thin = {}, {}, {}
    plan(0, count, by_depth)
    for depth in sorted(by_depth):
        nodes = by_depth[depth]
        schur, arms, floors, thin_arms = [], [], [], []
        for lo, mid, hi in nodes:
            s, parts = diag[mid], []
            t, thin_parts = floor_diag[mid], []
            if lo < mid:
                arm = low_right(done[lo, mid][-1], low, mid, False)
                s = s - low(mid, arm[-size:])
                parts.append(arm)
                thin_parts += [floor_low[mid] * x for x in thin[lo, mid][-1]]
                t = t - floor_low[mid] * thin_parts[-1]
            parts.append(unit)
            thin_parts.append(1.0)
            if mid + 1 < hi:
                arm = low_right(done[mid + 1, hi][0], low, mid + 1, True)
                s = s - low(mid + 1, arm[:size], True)
                parts.append(arm)
                thin_arm = [floor_low[mid + 1] * x for x in thin[mid + 1, hi][0]]
                t = t - floor_low[mid + 1] * thin_arm[0]
                thin_parts += thin_arm
            schur.append(s)
            floors.append(t)
            arms.append(jnp.concatenate(parts, axis=0) if len(parts) > 1 else parts[0])
            thin_arms.append(thin_parts)
        inverses = invert_all(schur, [0.97 * t for t in floors], steps)
        for (lo, mid, hi), v, z, thin_v, t in zip(nodes, arms, inverses, thin_arms, floors):
            thin[lo, hi] = [[a * b / t for b in thin_v] for a in thin_v]
            for a, b in ((lo, mid), (mid + 1, hi)):
                for i in range(a, b):
                    for j in range(a, b):
                        thin[lo, hi][i - lo][j - lo] += thin[a, b][i - a][j - a]
            if hi - lo == 1:
                done[lo, hi] = [z]
                continue
            w = dot(v, z)
            panels = []
            for k in range(lo, hi):
                vk = v[(k - lo) * size : (k - lo + 1) * size]
                new = w if k == mid else dot_t(w, vk)
                pieces = []
                for a, b in ((lo, mid), (mid, mid + 1), (mid + 1, hi)):
                    if a >= b:
                        continue
                    piece = new[(a - lo) * size : (b - lo) * size]
                    if a <= k < b and k != mid:
                        piece = piece + done[a, b][k - a]
                    pieces.append(piece)
                panels.append(jnp.concatenate(pieces, axis=0) if len(pieces) > 1 else pieces[0])
            done[lo, hi] = panels
    return done[0, count], thin[0, count]


def low_right(panel, low, k, plain):
    return low(k, panel, not plain, True)


def split(x):
    high = x.astype(jnp.bfloat16)
    return high, (x - high.astype(jnp.float32)).astype(jnp.bfloat16)


def dot3(a_high, a_low, b):
    b_high, b_low = split(b)
    mul = functools.partial(jnp.dot, preferred_element_type=jnp.float32)
    return mul(a_high, b_high) + (mul(a_low, b_high) + mul(a_high, b_low))


def factor_kernel(links_ref, top_ref, loss_ref, high_ref, low_ref, ends_ref, send_ref):
    levels, size = loss_ref.shape[0], loss_ref.shape[1]
    inner = levels - 1
    on_diag = eye_of(size)
    top_link, inner_link = top_ref[0:1, 0:1], jnp.full((1, 1), links_ref[inner - 1])
    links = [jnp.full((1, 1), links_ref[k]) for k in range(levels)]

    def diag_of(k):
        above = top_link if k == 0 else links[k - 1]
        return loss_ref[k] + jnp.where(on_diag, 1.0 + above + links[k], 0.0)

    def low(k, x, transposed=False, right=False):
        return links_ref[k - 1] * x

    floor_diag = [
        LEAST + links[k] + (top_link if k == 0 else links[k - 1]) for k in range(levels)
    ]
    panels, thin = dense_inverse(
        [diag_of(k) for k in range(inner)], low, floor_diag[:inner], [top_link] + links[: inner - 1]
    )
    for k, panel in enumerate(panels):
        high, rest = split(panel)
        high_ref[:, k * size : (k + 1) * size] = high
        low_ref[:, k * size : (k + 1) * size] = rest
    ends_ref[0] = top_link * panels[0]
    ends_ref[1] = inner_link * panels[-1]
    blocks = [
        (
            diag_of(inner) - inner_link * inner_link * panels[-1][-size:],
            floor_diag[inner] - inner_link * inner_link * thin[-1][-1],
        ),
        (top_link * top_link * panels[0][:size], top_link * top_link * thin[0][0]),
        (inner_link * top_link * panels[0][-size:], inner_link * top_link * thin[0][-1]),
    ]
    for k, (block, floor) in enumerate(blocks):
        send_ref[k, :size] = block
        send_ref[k, size:] = jnp.broadcast_to(floor, (8, size))


def interface(all_ref, ends_ref, high_ref, low_ref, rows_ref):
    count, size = all_ref.shape[0], all_ref.shape[3]

    def diag_of(rows, cols):
        own = [all_ref[k, 0, rows, cols] for k in range(count)]
        return [
            own[k] - all_ref[k + 1, 1, rows, cols] if k + 1 < count else own[k]
            for k in range(count)
        ]

    def low(k, x, transposed=False, right=False):
        block = all_ref[k, 2, :size]
        if right:
            return dot_t(x, block) if transposed else dot(x, block)
        return dot(block, x, ((0,), (0,))) if transposed else dot(block, x)

    thin = slice(size, size + 1), slice(0, 1)
    panels, _ = dense_inverse(
        diag_of(slice(0, size), slice(0, size)),
        low,
        diag_of(*thin),
        [all_ref[k, 2, thin[0], thin[1]] for k in range(count)],
        enough_steps(spread(size)),
    )
    for k, panel in enumerate(panels):
        rows_ref[k] = panel
    me = lax.axis_index("lev")
    own = rows_ref[me]
    above = rows_ref[jnp.maximum(me - 1, 0)]
    inner = dot_t(ends_ref[0], above) + dot_t(ends_ref[1], own)
    length = inner.shape[0]
    high_ref[:length], low_ref[:length] = split(inner)
    high_ref[length:], low_ref[length:] = split(own.T)


def send(src, dst, sems, slot, device):
    return pltpu.make_async_remote_copy(
        src_ref=src,
        dst_ref=dst,
        send_sem=sems.at[0, slot],
        recv_sem=sems.at[1, slot],
        device_id=device,
        device_id_type=pl.DeviceIdType.MESH,
    )


def greet(lev_all, lon_all):
    barrier = pltpu.get_barrier_semaphore()
    partners = []
    for axis, everyone in (("lev", lev_all), ("lon", lon_all)):
        count, me = lax.axis_size(axis), lax.axis_index(axis)
        if everyone is None:
            continue
        steps = range(1, count) if everyone else sorted({1, count - 1})
        partners += [{axis: lax.rem(me + d, count)} for d in steps if d % count]
    for device in partners:
        pl.semaphore_signal(
            barrier, inc=1, device_id=device, device_id_type=pl.DeviceIdType.MESH
        )
    pl.semaphore_wait(barrier, len(partners))


def pack_edges(cur_ref, edges_ref):
    levels, size, columns = cur_ref.shape
    lane = lax.broadcasted_iota(jnp.int32, (size, 128), 1)
    last = jnp.zeros((size, 128), jnp.float32)
    first = last
    for k in range(levels):
        tail = pltpu.roll(cur_ref[k, :, columns - 128 :], k + 1, 1)
        head = cur_ref[k, :, :128]
        head = pltpu.roll(head, k, 1) if k else head
        last = jnp.where(lane == k, tail, last)
        first = jnp.where(lane == k, head, first)
    edges_ref[0] = last
    edges_ref[1] = first


def halo_copies(edges_ref, halo_ref, sems):
    around, me = lax.axis_size("lon"), lax.axis_index("lon")
    return [
        send(edges_ref.at[0], halo_ref.at[0], sems, 0, {"lon": lax.rem(me + 1, around)}),
        send(edges_ref.at[1], halo_ref.at[1], sems, 1, {"lon": lax.rem(me + around - 1, around)}),
    ]


def local_forcing(mix_ref, cur_ref, prev_ref, pair_ref, force_ref):
    levels, size, columns = cur_ref.shape
    lane = lax.broadcasted_iota(jnp.int32, (size, columns), 1)
    for k in range(levels):
        c = cur_ref[k]
        back = jnp.where(lane == 0, 0.0, pltpu.roll(c, 1, 1))
        ahead = jnp.where(lane == columns - 1, 0.0, pltpu.roll(c, columns - 1, 1))
        p_high, p_low = split(pair_ref[k])
        chem = dot3(p_high, p_low, c * c)
        force_ref[k * size : (k + 1) * size] = (
            prev_ref[k] - chem + mix_ref[k] * (back + ahead - 2.0 * c)
        )


def add_halo(mix_ref, halo_ref, force_ref):
    levels = mix_ref.shape[0]
    size, columns = halo_ref.shape[1], force_ref.shape[1]
    lane = lax.broadcasted_iota(jnp.int32, (size, 128), 1)
    before, after = halo_ref[0], halo_ref[1]
    for k in range(levels):
        rows = slice(k * size, (k + 1) * size)
        at_head = pltpu.roll(before, 128 - k, 1) if k else before
        at_tail = pltpu.roll(after, 127 - k, 1)
        force_ref[rows, :128] += jnp.where(lane == 0, mix_ref[k] * at_head, 0.0)
        force_ref[rows, columns - 128 :] += jnp.where(lane == 127, mix_ref[k] * at_tail, 0.0)


def couple(
    links_ref, top_link, g_high, g_low, force_ref, part_ref, f_high, f_low, top_out, top_in, sides_ref,
    sems, direct,
):
    count, me = lax.axis_size("lev"), lax.axis_index("lev")
    inner, size = part_ref.shape[0], top_out.shape[0]
    f_high[...], f_low[...] = split(force_ref[:inner])
    mul = functools.partial(jnp.dot, preferred_element_type=jnp.float32)

    def rows_of(start, stop):
        a, b = g_high[start:stop], g_low[start:stop]
        part = mul(a, f_high[...]) + (mul(b, f_high[...]) + mul(a, f_low[...]))
        part_ref[start:stop] = part
        return part

    top_out[...] = top_link * rows_of(0, size)
    sides_ref[me] = force_ref[inner:] + links_ref[inner // size - 1] * rows_of(inner - size, inner)
    up = send(top_out, top_in, sems, 0, {"lev": lax.rem(me + count - 1, count)})
    half = size * ((inner // size) // 2)

    @pl.when(me > 0)
    def _():
        up.start()

    rows_of(size, half)

    @pl.when(me < count - 1)
    def _():
        up.wait_recv()
        sides_ref[me] += top_in[...]

    partner = me + 1 - 2 * lax.rem(me, 2)
    copies = [
        send(sides_ref.at[me], sides_ref.at[me], sems, d, {"lev": lax.rem(me + d, count)})
        for d in range(1 if direct else 2, count, 1 if direct else 2)
    ]
    onward = [] if direct else [send(sides_ref.at[me], sides_ref.at[me], sems, 1, {"lev": partner})]
    for d in range(count if direct else 2, count, 2):
        origin = lax.rem(me - d + count, count)
        onward.append(
            send(sides_ref.at[origin], sides_ref.at[origin], sems, d + 1, {"lev": partner})
        )
    for copy in copies + onward[:1]:
        copy.start()
    rows_of(half, inner - size)

    @pl.when(me > 0)
    def _():
        up.wait_send()

    return copies, onward


def relay(copies, onward):
    for copy, later in zip(copies, onward[1:]):
        copy.wait_recv()
        later.start()
    for copy in copies:
        copy.wait_send()
    for copy in onward:
        copy.wait()


def finish(part_ref, sides_ref, high_ref, low_ref, out_ref):
    levels, size, columns = out_ref.shape
    count = sides_ref.shape[0]
    b_high, b_low = split(sides_ref[...].reshape(count * size, columns))
    mul = functools.partial(jnp.dot, preferred_element_type=jnp.float32)
    for k in range(levels):
        rows = slice(k * size, (k + 1) * size)
        a, b = high_ref[rows], low_ref[rows]
        row = mul(a, b_high) + (mul(b, b_high) + mul(a, b_low))
        out_ref[k] = row + part_ref[rows] if k < levels - 1 else row


def open_kernel(
    links_ref, mix_ref, prev_ref, pair_ref, force_ref, top_ref, edges, halo, link_out, sems
):
    levels = prev_ref.shape[0]
    count, me = lax.axis_size("lev"), lax.axis_index("lev")
    pack_edges(prev_ref, edges)
    link_out[...] = jnp.full(link_out.shape, links_ref[levels - 1], jnp.float32)
    greet(False, False)
    copies = halo_copies(edges, halo, sems)
    down = send(link_out, top_ref, sems, 2, {"lev": lax.rem(me + 1, count)})
    for copy in copies:
        copy.start()

    @pl.when(me < count - 1)
    def _():
        down.start()

    @pl.when(me == 0)
    def _():
        top_ref[...] = jnp.zeros(top_ref.shape, jnp.float32)

    local_forcing(mix_ref, prev_ref, prev_ref, pair_ref, force_ref)
    for copy in copies:
        copy.wait()
    add_halo(mix_ref, halo, force_ref)

    @pl.when(me < count - 1)
    def _():
        down.wait_send()

    @pl.when(me > 0)
    def _():
        down.wait_recv()


def newton_kernel(
    links_ref, mix_ref, top_ref, sent_ref, ends_ref, first_force, g_high, g_low, prev_ref, pair_ref,
    out_ref, var_ref, all_ref, rows_ref, h_high, h_low, cur_ref, edges, halo, force_ref, part_ref,
    first_sides, sides_ref, f_high, f_low, first_out, first_in, top_out, top_in, sums_ref,
    block_sems, first_sems, halo_sems, sems, sum_sems,
):
    levels, size, columns = prev_ref.shape
    count, me = lax.axis_size("lev"), lax.axis_index("lev")
    around, place = lax.axis_size("lon"), lax.axis_index("lon")
    greet(True, True)
    blocks = [
        send(sent_ref, all_ref.at[me], block_sems, d, {"lev": lax.rem(me + d, count)})
        for d in range(1, count)
    ]
    for copy in blocks:
        copy.start()
    all_ref[me] = sent_ref[...]
    copies = couple(
        links_ref, top_ref[0:1, 0:1], g_high, g_low, first_force, part_ref, f_high, f_low,
        first_out, first_in, first_sides, first_sems, True,
    )
    for copy in blocks:
        copy.wait()
    interface(all_ref, ends_ref, h_high, h_low, rows_ref)
    for copy in copies[0]:
        copy.wait()
    finish(part_ref, first_sides, h_high, h_low, cur_ref)
    pack_edges(cur_ref, edges)
    copies = halo_copies(edges, halo, halo_sems)
    for copy in copies:
        copy.start()
    local_forcing(mix_ref, cur_ref, prev_ref, pair_ref, force_ref)
    for copy in copies:
        copy.wait()
    add_halo(mix_ref, halo, force_ref)
    copies = couple(
        links_ref, top_ref[0:1, 0:1], g_high, g_low, force_ref, part_ref, f_high, f_low,
        top_out, top_in, sides_ref, sems, False,
    )
    relay(*copies)
    finish(part_ref, sides_ref, h_high, h_low, out_ref)
    lane = lax.broadcasted_iota(jnp.int32, (size, 128), 1)
    total = jnp.zeros((size, 128), jnp.float32)
    for k in range(levels):
        row = out_ref[k]
        total = jnp.where(lane == k, jnp.sum(row * row, axis=1, keepdims=True), total)
    sums_ref[0] = total.T[: sums_ref.shape[1]]
    copies = [
        send(sums_ref.at[0], sums_ref.at[d], sum_sems, d, {"lon": lax.rem(place + d, around)})
        for d in range(1, around)
    ]
    for copy in copies:
        copy.start()
    for copy in copies:
        copy.wait()
    total = sums_ref[place]
    for j in range(1, around):
        total = total + sums_ref[lax.rem(place - j + around, around)]
    var_ref[...] = (total / (columns * around))[:levels]


def call(kernel, outs, places, scratch=(), group=None):
    extra = {} if group is None else {"collective_id": group, "has_side_effects": True}
    return pl.pallas_call(
        kernel,
        out_shape=[jax.ShapeDtypeStruct(shape, dtype) for shape, dtype in outs],
        in_specs=places,
        out_specs=[VMEM] * len(outs),
        scratch_shapes=list(scratch),
        compiler_params=pltpu.CompilerParams(vmem_limit_bytes=60 * 2**20, **extra),
    )


def local(previous, loss_matrix, pair_matrix, diffusivity, mixing):
    levels, size, columns = previous.shape
    count = lax.axis_size("lev")
    around = lax.axis_size("lon")
    inner = (levels - 1) * size
    f32, bf16 = jnp.float32, jnp.bfloat16
    buf, sem = pltpu.VMEM, lambda n: pltpu.SemaphoreType.DMA((2, n))
    force, top = call(
        open_kernel,
        [((levels * size, columns), f32), ((8, 128), f32)],
        [SMEM, SMEM, VMEM, VMEM],
        [buf((2, size, 128), f32), buf((2, size, 128), f32), buf((8, 128), f32), sem(3)],
        0,
    )(diffusivity, mixing, previous, pair_matrix)
    g_high, g_low, ends, sent = call(
        factor_kernel,
        [((inner, inner), bf16), ((inner, inner), bf16), ((2, inner, size), f32), ((3, size + 8, size), f32)],
        [SMEM, VMEM, VMEM],
    )(diffusivity, top, loss_matrix)
    return call(
        newton_kernel,
        [((levels, size, columns), f32), ((levels, size), f32)],
        [SMEM, SMEM] + [VMEM] * 8,
        [
            buf((count, 3, size + 8, size), f32),
            buf((count, count * size, size), f32),
            buf((levels * size, count * size), bf16),
            buf((levels * size, count * size), bf16),
            buf((levels, size, columns), f32),
            buf((2, size, 128), f32),
            buf((2, size, 128), f32),
            buf((levels * size, columns), f32),
            buf((inner, columns), f32),
            buf((count, size, columns), f32),
            buf((count, size, columns), f32),
            buf((inner, columns), bf16),
            buf((inner, columns), bf16),
            buf((size, columns), f32),
            buf((size, columns), f32),
            buf((size, columns), f32),
            buf((size, columns), f32),
            buf((around, -(-levels // 8) * 8, size), f32),
            sem(count),
            sem(count),
            sem(2),
            sem(count),
            sem(around),
        ],
        1,
    )(diffusivity, mixing, top, sent, ends, force, g_high, g_low, previous, pair_matrix)


def cat3(a_high, a_low, b_high, b_low):
    return jnp.dot(
        jnp.concatenate([a_high, a_low, a_high], axis=1),
        jnp.concatenate([b_high, b_high, b_low], axis=0),
        preferred_element_type=jnp.float32,
    )


def wide(a):
    high, low = split(a)
    return jnp.concatenate([high, low, high, jnp.zeros_like(high)], axis=1)


def tall(b):
    high, low = split(b)
    return jnp.concatenate([high, high, low, jnp.zeros_like(high)], axis=0)


def wide_dot(a, b):
    return jnp.dot(a, b, preferred_element_type=jnp.float32)


def near_dot(a, b):
    return lax.dot_general(
        a, b, (((1,), (0,)), ((), ())), precision=lax.Precision.HIGH, preferred_element_type=jnp.float32
    )


def pull(links, loss):
    stiff = links[0]
    for a in links[1:]:
        own = 1.0 + loss + stiff
        stiff = a * own / (a + own)
    return stiff


def worst_ratio(above, below):
    sides = []
    for count in (above, below):
        draws = itertools.product((200.0, 2000.0), repeat=min(count, 8) + 1)
        sides.append([(pull(d, 640.0), pull(d, 0.05)) for d in draws])
    return 1.15 * max((641.0 + a + c) / (1.05 + b + d) for a, b in sides[0] for c, d in sides[1])


def gains_for(ratio):
    rho, gains = (ratio - 1.0) / (ratio + 1.0), []
    while rho > 1.2e-3:
        gains.append(2.0 / (2.0 - rho * rho))
        rho = rho * rho / (2.0 - rho * rho)
    return gains


def invert_fixed(blocks, floors, ratio):
    size = blocks[0].shape[0]
    unit = jnp.where(eye_of(size), 1.0, 0.0).astype(jnp.float32)
    gains = gains_for(ratio)
    xs, rests = [], []
    for a, low in zip(blocks, floors):
        scale = (2.0 / (1.0 + ratio)) / low
        rest = unit - scale * a
        xs.append((gains[0] * scale) * (unit + rest))
        rests.append(rest)
    rests = [gains[0] * dot(r, r) - (gains[0] - 1.0) * unit for r in rests]
    for step, g in enumerate(gains[1:]):
        left = len(gains) - step - 2
        mul = dot if left > 2 else near_dot
        if left == 0:
            xs = [g * (x + mul(x, r)) for x, r in zip(xs, rests)]
            break
        both = [mul(jnp.concatenate([x, r], axis=0), r) for x, r in zip(xs, rests)]
        xs = [g * (x + b[:size]) for x, b in zip(xs, both)]
        rests = [g * b[size:] - (g - 1.0) * unit for b in both]
    rests = [unit - dot(a, x) for a, x in zip(blocks, xs)]
    return [x + near_dot(x, r) for x, r in zip(xs, rests)]


def chain_factor(diag, links, floors, panel_ref, hook):
    count, size = len(diag), diag[0].shape[0]
    unit = jnp.where(eye_of(size), 1.0, 0.0).astype(jnp.float32)
    by_depth, thin = {}, {}
    plan(0, count, by_depth)

    def rows(lo, hi):
        return slice(lo * size, hi * size)

    for depth in sorted(by_depth):
        nodes = by_depth[depth]
        ratio = max(worst_ratio(mid - lo, hi - 1 - mid) for lo, mid, hi in nodes)
        schur, arms, lows, thin_arms = [], [], [], []
        for lo, mid, hi in nodes:
            s, parts = diag[mid], []
            t, thin_parts = floors[mid], []
            if lo < mid:
                arm = links[mid] * panel_ref[mid - 1, rows(lo, mid)]
                s = s - links[mid] * arm[-size:]
                parts.append(arm)
                thin_parts += [links[mid] * x for x in thin[lo, mid][-1]]
                t = t - links[mid] * thin_parts[-1]
            parts.append(unit)
            thin_parts.append(1.0)
            if mid + 1 < hi:
                arm = links[mid + 1] * panel_ref[mid + 1, rows(mid + 1, hi)]
                s = s - links[mid + 1] * arm[:size]
                parts.append(arm)
                thin_arm = [links[mid + 1] * x for x in thin[mid + 1, hi][0]]
                t = t - links[mid + 1] * thin_arm[0]
                thin_parts += thin_arm
            schur.append(s)
            lows.append(t)
            arms.append(jnp.concatenate(parts, axis=0) if len(parts) > 1 else parts[0])
            thin_arms.append(thin_parts)
        inverses = invert_fixed(schur, [0.97 * t for t in lows], ratio)
        for (lo, mid, hi), v, z, thin_v, t in zip(nodes, arms, inverses, thin_arms, lows):
            thin[lo, hi] = [[a * b / t for b in thin_v] for a in thin_v]
            for a, b in ((lo, mid), (mid + 1, hi)):
                for i in range(a, b):
                    for j in range(a, b):
                        thin[lo, hi][i - lo][j - lo] += thin[a, b][i - a][j - a]
            if hi - lo == 1:
                panel_ref[mid, rows(mid, hi)] = z
                continue
            w = dot(v, z)
            if hi - lo == count:
                continue
            new = dot_t(w, v)
            for k in range(lo, hi):
                own = new[:, (k - lo) * size : (k - lo + 1) * size]
                panel_ref[k, rows(mid, mid + 1)] = own[rows(mid - lo, mid - lo + 1)]
                for a, b in ((lo, mid), (mid + 1, hi)):
                    if a >= b:
                        continue
                    piece = own[rows(a - lo, b - lo)]
                    if a <= k < b:
                        piece = piece + panel_ref[k, rows(a, b)]
                    panel_ref[k, rows(a, b)] = piece
        if depth < max(by_depth):
            hook(depth)
    return v, w, by_depth[max(by_depth)][0][1], thin[0, count]


def fold(x):
    half = x.shape[0] // 2
    return jnp.concatenate([x[:half], x[half:]], axis=1)


def unfold(x):
    half = x.shape[1] // 2
    return jnp.concatenate([x[:, :half], x[:, half:]], axis=0)


def pack_pairs(field_ref, columns, edges_ref):
    levels, size = field_ref.shape[:2]
    lane = lax.broadcasted_iota(jnp.int32, (size, 128), 1)
    last = jnp.zeros((size, 128), jnp.float32)
    first = last
    for k in range(levels):
        tail = pltpu.roll(field_ref[k, :, columns - 128 : columns], (2 * k + 2) % 128, 1)
        head = field_ref[k, :, :128]
        head = pltpu.roll(head, 2 * k, 1) if k else head
        mine = (lane == 2 * k) | (lane == 2 * k + 1)
        last = jnp.where(mine, tail, last)
        first = jnp.where(mine, head, first)
    edges_ref[0] = last
    edges_ref[1] = first


def unpack_pairs(halo_ref, columns, field_ref):
    levels, size = field_ref.shape[:2]
    lane = lax.broadcasted_iota(jnp.int32, (size, 128), 1)
    before, after = halo_ref[0], halo_ref[1]
    for k in range(levels):
        at_head = pltpu.roll(after, (128 - 2 * k) % 128, 1) if k else after
        at_tail = pltpu.roll(before, (126 - 2 * k) % 128, 1)
        field_ref[k, :, columns:] = jnp.where(lane < 2, at_head, jnp.where(lane >= 126, at_tail, 0.0))


def forcing(mix_ref, cur_ref, prev_ref, pairs_ref, width, sep_ref, f_high, f_low):
    levels, size, full = cur_ref.shape
    for k in range(levels):
        c = cur_ref[k]
        ring = pltpu.roll(c, 1, 1) + pltpu.roll(c, full - 1, 1)
        own = c[:, :width]
        chem = wide_dot(pairs_ref[k], tall(own * own))
        force = prev_ref[k, :, :width] - chem + mix_ref[k] * (ring[:, :width] - 2.0 * own)
        if k == 0:
            sep_ref[:, :width] = force
        else:
            rows = slice((k - 1) * size, k * size)
            f_high[rows, :width], f_low[rows, :width] = split(force)


def start_all(copies):
    @pl.when(lax.axis_index("lev") < lax.axis_size("lev"))
    def _():
        for copy in copies:
            copy.start()


def step_kernel(
    links_hbm, mix_hbm, loss_hbm, prev_hbm, pair_hbm, out_ref, var_ref, links_ref, mix_ref,
    loss_ref, prev_ref, pair_ref, pairs_ref, edges, halo, z_high, z_low, send_ref, all_ref,
    ends_high, ends_low, table_ref, sep_ref, f_high, f_low, part_ref, own_ref, near_ref, mine_ref, far_ref,
    side_high, side_low, hq_high, hq_low, u_ref, top_ref, cur_ref, sums_ref, panel_ref, w_ref, v_ref,
    load_sems, halo_sems, block_sems, near_sems, far_sems, sum_sems,
):
    levels, size, columns = prev_hbm.shape
    inner = levels - 1
    full = cur_ref.shape[2]
    count, me = lax.axis_size("lev"), lax.axis_index("lev")
    around, place = lax.axis_size("lon"), lax.axis_index("lon")
    core, chip = lax.rem(me, 2), me // 2
    partner = me + 1 - 2 * core
    across = lax.rem(me + 2, count)

    loads = [
        pltpu.make_async_copy(loss_hbm, loss_ref, load_sems.at[0]),
        pltpu.make_async_copy(prev_hbm, prev_ref.at[:, :, pl.ds(0, columns)], load_sems.at[1]),
        pltpu.make_async_copy(pair_hbm, pair_ref, load_sems.at[2]),
        pltpu.make_async_copy(links_hbm, links_ref, load_sems.at[3]),
        pltpu.make_async_copy(mix_hbm, mix_ref, load_sems.at[4]),
    ]
    for k in (3, 0, 1, 2, 4):
        loads[k].start()
    barrier = pltpu.get_barrier_semaphore()
    partners = [{"lev": lax.rem(me + d, count)} for d in range(1, count)]
    partners += [{"lon": lax.rem(place + d, around)} for d in range(1, around)]
    for device in partners:
        pl.semaphore_signal(barrier, inc=1, device_id=device, device_id_type=pl.DeviceIdType.MESH)

    loads[3].wait()
    links = [jnp.full((1, 1), links_ref[k]) for k in range(levels)]
    on_diag = eye_of(size)
    halo_moves = halo_copies(edges, halo, halo_sems)

    def hook(depth):
        if depth != 2:
            return
        loads[1].wait()
        pack_pairs(prev_ref, columns, edges)
        pl.semaphore_wait(barrier, len(partners))
        start_all(halo_moves)

    loads[0].wait()
    diag = [
        loss_ref[k] + jnp.where(on_diag, 1.0 + links[k] + (links[k - 1] if k else 0.0), 0.0)
        for k in range(levels)
    ]
    floors = [LEAST + links[k] + (links[k - 1] if k else 0.0) for k in range(levels)]
    v, w, mid, thin = chain_factor(diag[1:], links[:inner], floors[1:], panel_ref, hook)
    a, b = links[0], links[inner]
    old = [
        panel_ref[0, : mid * size],
        jnp.zeros((size, size), jnp.float32),
        panel_ref[inner - 1, (mid + 1) * size :],
    ]
    tips = dot_t(w, jnp.concatenate([v[:size], v[-size:]], axis=0))
    first = tips[:, :size] + jnp.concatenate([old[0], old[1], jnp.zeros_like(old[2])], axis=0)
    last = tips[:, size:] + jnp.concatenate([jnp.zeros_like(old[0]), old[1], old[2]], axis=0)
    sub = lax.broadcasted_iota(jnp.int32, (8, 128), 0)
    send_ref[: size // 2] = fold(diag[0] - a * a * first[:size])
    send_ref[size // 2 : size] = fold(jnp.where(on_diag, b, 0.0) - b * b * last[-size:])
    send_ref[size : 3 * size // 2] = fold(a * b * first[-size:])
    send_ref[3 * size // 2 :] = jnp.where(
        sub == 0, floors[0] - a * a * thin[0][0], jnp.where(sub == 1, b - b * b * thin[-1][-1], a * b * thin[0][-1])
    )
    blocks = [
        send(send_ref, all_ref.at[me], block_sems, d, {"lev": lax.rem(me + d, count)})
        for d in range(1, count)
    ]
    start_all(blocks)
    all_ref[me] = send_ref[...]

    ends_high[...], ends_low[...] = split(jnp.concatenate([a * first, b * last], axis=1))
    w_ref[...] = wide(w)
    v_high, v_low = split(v)
    v_ref[...] = jnp.concatenate([v_high, v_high, v_low, jnp.zeros_like(v_high)], axis=1)

    def form(lo, hi):
        spot = slice(lo * size, hi * size)
        new = lax.dot_general(
            w_ref[spot], v_ref[...], (((1,), (1,)), ((), ())), preferred_element_type=jnp.float32
        )
        start, stop = (0, mid) if lo < mid else (mid + 1, inner)
        if lo != mid:
            zeros = jnp.zeros((new.shape[0], size), jnp.float32)
            new = new + jnp.concatenate(
                [panel_ref[j, spot] if start <= j < stop else zeros for j in range(inner)], axis=1
            )
        z_high[spot], z_low[spot] = split(new)

    form(0, 1)
    form(inner - 1, inner)
    loads[2].wait()
    loads[4].wait()
    for k in range(levels):
        pairs_ref[k] = wide(pair_ref[k])
    for move in halo_moves:
        move.wait()
    unpack_pairs(halo, columns, prev_ref)

    def z_rows(start, stop, width):
        return cat3(z_high[start:stop], z_low[start:stop], f_high[:, :width], f_low[:, :width])

    def ends(turn, width):
        rows = cat3(
            jnp.concatenate([z_high[:size], z_high[-size:]], axis=0),
            jnp.concatenate([z_low[:size], z_low[-size:]], axis=0),
            f_high[:, :width],
            f_low[:, :width],
        )
        part_ref[:size, :width] = rows[:size]
        part_ref[-size:, :width] = rows[size:]
        own_ref[turn, 0, :, :width] = sep_ref[:, :width] + a * rows[:size]
        own_ref[turn, 1, :, :width] = b * rows[size:]
        copy = send(
            own_ref.at[turn, :, :, pl.ds(0, width)], near_ref.at[turn, :, :, pl.ds(0, width)], near_sems, turn,
            {"lev": partner},
        )
        start_all([copy])
        return copy

    def middle(width):
        part_ref[size:-size, :width] = z_rows(size, (inner - 1) * size, width)

    def merge(turn, width):
        upper = core == 0
        s_own, t_own = own_ref[turn, 0, :, :width], own_ref[turn, 1, :, :width]
        s_in, t_in = near_ref[turn, 0, :, :width], near_ref[turn, 1, :, :width]
        low_side = jnp.where(upper, s_own, s_in)
        high_side = jnp.where(upper, s_in + t_own, s_own + t_in)
        side_high[:size, :width], side_low[:size, :width] = split(low_side)
        side_high[size:, :width], side_low[size:, :width] = split(high_side)
        return jnp.where(chip == 0, jnp.where(upper, t_in, t_own), 0.0)

    def condense(turn, width, tail, k_high, k_low):
        mine_ref[turn, :, :width] = tail + cat3(k_high, k_low, side_high[:, :width], side_low[:, :width])
        half, quarter = columns // 2, columns // 4
        first = pl.ds(pl.multiple_of(core * half, 128), quarter)
        second = pl.ds(pl.multiple_of(core * half + quarter, 128), quarter)
        routes = [(mine_ref, first, across), (mine_ref, second, across), (mine_ref, second, lax.rem(partner + 2, count))]
        routes += [(mine_ref, pl.ds(columns, width - columns), across)] if width > columns else []
        routes += [(far_ref, first, partner)]
        copies = [
            send(src.at[turn, :, spot], far_ref.at[turn, :, spot], far_sems, 5 * turn + k, {"lev": device})
            for k, (src, spot, device) in enumerate(routes)
        ]
        start_all(copies[:-1])
        return copies

    def relay_far(copies):
        copies[0].wait_recv()
        start_all(copies[-1:])

    def wait_far(copies):
        copies[0].wait_send()
        for copy in copies[1:]:
            copy.wait()

    def gather_sides(width):
        rest = cat3(hq_high[...], hq_low[...], side_high[:, :width], side_low[:, :width])
        for k in range(levels):
            rows = rest[k * size : (k + 1) * size]
            cur_ref[k, :, :width] = rows if k == 0 else rows + part_ref[(k - 1) * size : k * size, :width]

    def finish(turn, width, to_ref):
        total = mine_ref[turn, :, :width] + far_ref[turn, :, :width]
        top = tall(wide_dot(top_ref[...], tall(total)))
        for k in range(levels):
            to_ref[k, :, :width] = cur_ref[k, :, :width] + wide_dot(u_ref[k * size : (k + 1) * size], top)

    forcing(mix_ref, prev_ref, prev_ref, pairs_ref, full, sep_ref, f_high, f_low)
    near = ends(0, full)
    for copy in blocks:
        copy.wait()

    def block(k, which):
        return unfold(all_ref[k, which * size // 2 : (which + 1) * size // 2])

    def floor(k, which):
        row = 3 * size // 2 + which
        return all_ref[k, row : row + 1, 0:1]

    ratio = spread(size)
    s = [block(k, 0) + (block(k - 1, 1) if k else 0.0) for k in range(count)]
    t = [floor(k, 0) + (floor(k - 1, 1) if k else 0.0) for k in range(count)]
    c = [None] + [block(k, 2) for k in range(count - 1)]
    e = [None] + [floor(k, 2) for k in range(count - 1)]
    z0, z3 = invert_fixed([s[0], s[3]], [0.97 * t[0], 0.97 * t[3]], ratio)
    a1, a3 = dot(c[1], z0), dot(z3, c[3])
    s1 = s[1] - dot_t(a1, c[1])
    t1 = t[1] - e[1] * e[1] / t[0]
    (z1,) = invert_fixed([s1], [0.97 * t1], ratio)
    a2 = dot(c[2], z1)
    s2 = s[2] - dot_t(a2, c[2]) - dot(c[3], a3, ((0,), (0,)))
    t2 = t[2] - e[2] * e[2] / t1 - e[3] * e[3] / t[3]
    b1 = dot(z1, a1)
    p0 = dot(a2, a1)
    zero = jnp.zeros((size, size), jnp.float32)
    unit = jnp.where(on_diag, 1.0, 0.0).astype(jnp.float32)
    sides = [
        (z0 + dot(a1, b1, ((0,), (0,))), b1.T, p0.T),
        (b1, z1, a2.T),
        (zero, zero, unit),
        (zero, z3, a3),
        (zero, zero, zero),
    ]
    for k, (left, right, top) in enumerate(sides):
        table_ref[k, :size] = jnp.concatenate([left, right], axis=1)
        table_ref[k, size:, :size] = top
    for k, (left, right) in enumerate(((p0, a2), (unit, a3.T))):
        table_ref[len(sides) + k, :size] = jnp.concatenate([left, right], axis=1)
    near.wait()
    tail = merge(0, full)
    k_high, k_low = split(table_ref[len(sides) + chip, :size])
    far = condense(0, full, tail, k_high, k_low)
    (z2,) = invert_fixed([s2], [0.97 * t2], ratio)
    top_ref[...] = wide(z2)
    own_q, next_q = table_ref[me, :size], table_ref[me + 1, :size]
    own_p, next_p = table_ref[me, size:, :size], table_ref[me + 1, size:, :size]
    q_high, q_low = split(jnp.concatenate([own_q, next_q], axis=0))
    p_high, p_low = split(jnp.concatenate([own_p, next_p], axis=0))
    hq_high[size:], hq_low[size:] = split(cat3(ends_high[...], ends_low[...], q_high, q_low))
    hq_high[:size], hq_low[:size] = split(own_q)
    u_ref[size:] = wide(cat3(ends_high[...], ends_low[...], p_high, p_low))
    u_ref[:size] = wide(own_p)
    for lo, hi in ((1, mid), (mid, mid + 1), (mid + 1, inner - 1)):
        form(lo, hi)
    relay_far(far)
    middle(full)
    gather_sides(full)
    wait_far(far)
    finish(0, full, cur_ref)

    forcing(mix_ref, cur_ref, prev_ref, pairs_ref, columns, sep_ref, f_high, f_low)
    near = ends(1, columns)
    near.wait()
    tail = merge(1, columns)
    far = condense(1, columns, tail, k_high, k_low)
    middle(columns)
    gather_sides(columns)
    relay_far(far)
    wait_far(far)
    finish(1, columns, out_ref)
    lane = lax.broadcasted_iota(jnp.int32, (size, 128), 1)
    total = jnp.zeros((size, 128), jnp.float32)
    for k in range(levels):
        row = out_ref[k]
        total = jnp.where(lane == k, jnp.sum(row * row, axis=1, keepdims=True), total)
    sums_ref[0] = total.T[: sums_ref.shape[1]]
    copies = [
        send(sums_ref.at[0], sums_ref.at[d], sum_sems, d, {"lon": lax.rem(place + d, around)})
        for d in range(1, around)
    ]
    start_all(copies)
    for copy in copies:
        copy.wait()
    total = sums_ref[place]
    for j in range(1, around):
        total = total + sums_ref[lax.rem(place - j + around, around)]
    var_ref[...] = (total / (columns * around))[:levels]


def local_pairs(previous, loss_matrix, pair_matrix, diffusivity, mixing):
    levels, size, columns = previous.shape
    count, around = lax.axis_size("lev"), lax.axis_size("lon")
    inner, full = (levels - 1) * size, columns + 128
    f32, bf16 = jnp.float32, jnp.bfloat16
    buf, sem = pltpu.VMEM, lambda n: pltpu.SemaphoreType.DMA((2, n))
    hbm = pl.BlockSpec(memory_space=pltpu.MemorySpace.HBM)
    packed = 3 * size // 2 + 8
    return pl.pallas_call(
        step_kernel,
        out_shape=[
            jax.ShapeDtypeStruct((levels, size, columns), f32),
            jax.ShapeDtypeStruct((levels, size), f32),
        ],
        in_specs=[hbm] * 5,
        out_specs=[VMEM, VMEM],
        scratch_shapes=[
            pltpu.SMEM((levels,), f32),
            pltpu.SMEM((levels,), f32),
            buf((levels, size, size), f32),
            buf((levels, size, full), f32),
            buf((levels, size, size), f32),
            buf((levels, size, 4 * size), bf16),
            buf((2, size, 128), f32),
            buf((2, size, 128), f32),
            buf((inner, inner), bf16),
            buf((inner, inner), bf16),
            buf((packed, 2 * size), f32),
            buf((count, packed, 2 * size), f32),
            buf((inner, 2 * size), bf16),
            buf((inner, 2 * size), bf16),
            buf((count + 3, 2 * size, 2 * size), f32),
            buf((size, full), f32),
            buf((inner, full), bf16),
            buf((inner, full), bf16),
            buf((inner, full), f32),
            buf((2, 2, size, full), f32),
            buf((2, 2, size, full), f32),
            buf((2, size, full), f32),
            buf((2, size, full), f32),
            buf((2 * size, full), bf16),
            buf((2 * size, full), bf16),
            buf((levels * size, 2 * size), bf16),
            buf((levels * size, 2 * size), bf16),
            buf((levels * size, 4 * size), bf16),
            buf((size, 4 * size), bf16),
            buf((levels, size, full), f32),
            buf((around, -(-levels // 8) * 8, size), f32),
            buf((levels - 1, inner, size), f32),
            buf((inner, 4 * size), bf16),
            buf((inner, 4 * size), bf16),
            pltpu.SemaphoreType.DMA((5,)),
            sem(2),
            sem(count),
            sem(2),
            sem(10),
            sem(around),
        ],
        compiler_params=pltpu.CompilerParams(
            vmem_limit_bytes=40 * 2**20, collective_id=2, has_side_effects=True
        ),
    )(*(pltpu.with_memory_space_constraint(x, pltpu.MemorySpace.HBM) for x in (diffusivity, mixing, loss_matrix, previous, pair_matrix)))


def chosen(previous, *rest):
    paired = lax.axis_size("lev") == 4 and previous.shape[2] % 512 == 0
    return (local_pairs if paired else local)(previous, *rest)


def solution(mesh):
    placed = (P("lev", None, "lon"), P("lev", None, None), P("lev", None, None), P("lev"), P("lev"))
    return jax.shard_map(
        chosen,
        mesh=mesh,
        in_specs=placed,
        out_specs=(P("lev", None, "lon"), P("lev", None)),
        check_vma=False,
    )
```

```python
import functools
import itertools

import jax
import jax.numpy as jnp
from jax import lax
from jax.experimental import pallas as pl
from jax.experimental.pallas import tpu as pltpu
from jax.sharding import PartitionSpec as P

LEAST = 1.05
MOST = 10.0
HIGHEST = lax.Precision.HIGHEST
SMEM = pl.BlockSpec(memory_space=pltpu.SMEM)
VMEM = pl.BlockSpec(memory_space=pltpu.VMEM)


def dot(a, b, dims=((1,), (0,))):
    return lax.dot_general(
        a, b, (dims, ((), ())), precision=HIGHEST, preferred_element_type=jnp.float32
    )


def dot_t(a, b):
    return dot(a, b, ((1,), (1,)))


def eye_of(size):
    rows = lax.broadcasted_iota(jnp.int32, (size, size), 0)
    cols = lax.broadcasted_iota(jnp.int32, (size, size), 1)
    return rows == cols


def invert_all(blocks, floors, steps):
    size = blocks[0].shape[0]
    unit = jnp.where(eye_of(size), 1.0, 0.0).astype(jnp.float32)
    start, worst = [], None
    for a, lo in zip(blocks, floors):
        hi = jnp.max(jnp.sum(jnp.abs(a), axis=0, keepdims=True), axis=1, keepdims=True)
        hi = jnp.clip(hi, lo, lo * spread(size))
        scale = 2.0 / (hi + lo)
        rho = (hi - lo) / (hi + lo)
        start.append((scale, a))
        worst = rho if worst is None else jnp.maximum(worst, rho)

    def grow(rho):
        square = rho * rho
        return square / (2.0 - square), 2.0 / (2.0 - square)

    rho, gain = grow(worst)
    start = [(gain * scale) * (2.0 * unit - scale * a) for scale, a in start]

    def step(carry):
        rho, *xs = carry
        rest = [unit - dot(a, x) for a, x in zip(blocks, xs)]
        rho, gain = grow(rho)
        return (rho, *[gain * (x + dot(x, r)) for x, r in zip(xs, rest)])

    if steps is None:
        return lax.while_loop(lambda carry: jnp.max(carry[0]) > 3e-8, step, (rho, *start))[1:]
    return lax.fori_loop(0, steps, lambda i, carry: step(carry), (rho, *start))[1:]


def spread(size):
    return (1.0 + MOST * size) / (0.96 * LEAST)


def enough_steps(condition):
    rho, steps = (condition - 1.0) / (condition + 1.0), -1
    while rho > 3e-8:
        rho, steps = rho * rho / (2.0 - rho * rho), steps + 1
    return steps


def plan(lo, hi, out):
    if lo >= hi:
        return 0
    mid = lo + (hi - lo) // 2
    depth = 1 + max(plan(lo, mid, out), plan(mid + 1, hi, out))
    out.setdefault(depth, []).append((lo, mid, hi))
    return depth


def dense_inverse(diag, low, floor_diag, floor_low, steps=None):
    count, size = len(diag), diag[0].shape[0]
    unit = jnp.where(eye_of(size), 1.0, 0.0).astype(jnp.float32)
    by_depth, done, thin = {}, {}, {}
    plan(0, count, by_depth)
    for depth in sorted(by_depth):
        nodes = by_depth[depth]
        schur, arms, floors, thin_arms = [], [], [], []
        for lo, mid, hi in nodes:
            s, parts = diag[mid], []
            t, thin_parts = floor_diag[mid], []
            if lo < mid:
                arm = low_right(done[lo, mid][-1], low, mid, False)
                s = s - low(mid, arm[-size:])
                parts.append(arm)
                thin_parts += [floor_low[mid] * x for x in thin[lo, mid][-1]]
                t = t - floor_low[mid] * thin_parts[-1]
            parts.append(unit)
            thin_parts.append(1.0)
            if mid + 1 < hi:
                arm = low_right(done[mid + 1, hi][0], low, mid + 1, True)
                s = s - low(mid + 1, arm[:size], True)
                parts.append(arm)
                thin_arm = [floor_low[mid + 1] * x for x in thin[mid + 1, hi][0]]
                t = t - floor_low[mid + 1] * thin_arm[0]
                thin_parts += thin_arm
            schur.append(s)
            floors.append(t)
            arms.append(jnp.concatenate(parts, axis=0) if len(parts) > 1 else parts[0])
            thin_arms.append(thin_parts)
        inverses = invert_all(schur, [0.97 * t for t in floors], steps)
        for (lo, mid, hi), v, z, thin_v, t in zip(nodes, arms, inverses, thin_arms, floors):
            thin[lo, hi] = [[a * b / t for b in thin_v] for a in thin_v]
            for a, b in ((lo, mid), (mid + 1, hi)):
                for i in range(a, b):
                    for j in range(a, b):
                        thin[lo, hi][i - lo][j - lo] += thin[a, b][i - a][j - a]
            if hi - lo == 1:
                done[lo, hi] = [z]
                continue
            w = dot(v, z)
            panels = []
            for k in range(lo, hi):
                vk = v[(k - lo) * size : (k - lo + 1) * size]
                new = w if k == mid else dot_t(w, vk)
                pieces = []
                for a, b in ((lo, mid), (mid, mid + 1), (mid + 1, hi)):
                    if a >= b:
                        continue
                    piece = new[(a - lo) * size : (b - lo) * size]
                    if a <= k < b and k != mid:
                        piece = piece + done[a, b][k - a]
                    pieces.append(piece)
                panels.append(jnp.concatenate(pieces, axis=0) if len(pieces) > 1 else pieces[0])
            done[lo, hi] = panels
    return done[0, count], thin[0, count]


def low_right(panel, low, k, plain):
    return low(k, panel, not plain, True)


def split(x):
    high = x.astype(jnp.bfloat16)
    return high, (x - high.astype(jnp.float32)).astype(jnp.bfloat16)


def dot3(a_high, a_low, b):
    b_high, b_low = split(b)
    mul = functools.partial(jnp.dot, preferred_element_type=jnp.float32)
    return mul(a_high, b_high) + (mul(a_low, b_high) + mul(a_high, b_low))


def factor_kernel(links_ref, top_ref, loss_ref, high_ref, low_ref, ends_ref, send_ref):
    levels, size = loss_ref.shape[0], loss_ref.shape[1]
    inner = levels - 1
    on_diag = eye_of(size)
    top_link, inner_link = top_ref[0:1, 0:1], jnp.full((1, 1), links_ref[inner - 1])
    links = [jnp.full((1, 1), links_ref[k]) for k in range(levels)]

    def diag_of(k):
        above = top_link if k == 0 else links[k - 1]
        return loss_ref[k] + jnp.where(on_diag, 1.0 + above + links[k], 0.0)

    def low(k, x, transposed=False, right=False):
        return links_ref[k - 1] * x

    floor_diag = [
        LEAST + links[k] + (top_link if k == 0 else links[k - 1]) for k in range(levels)
    ]
    panels, thin = dense_inverse(
        [diag_of(k) for k in range(inner)], low, floor_diag[:inner], [top_link] + links[: inner - 1]
    )
    for k, panel in enumerate(panels):
        high, rest = split(panel)
        high_ref[:, k * size : (k + 1) * size] = high
        low_ref[:, k * size : (k + 1) * size] = rest
    ends_ref[0] = top_link * panels[0]
    ends_ref[1] = inner_link * panels[-1]
    blocks = [
        (
            diag_of(inner) - inner_link * inner_link * panels[-1][-size:],
            floor_diag[inner] - inner_link * inner_link * thin[-1][-1],
        ),
        (top_link * top_link * panels[0][:size], top_link * top_link * thin[0][0]),
        (inner_link * top_link * panels[0][-size:], inner_link * top_link * thin[0][-1]),
    ]
    for k, (block, floor) in enumerate(blocks):
        send_ref[k, :size] = block
        send_ref[k, size:] = jnp.broadcast_to(floor, (8, size))


def interface(all_ref, ends_ref, high_ref, low_ref, rows_ref):
    count, size = all_ref.shape[0], all_ref.shape[3]

    def diag_of(rows, cols):
        own = [all_ref[k, 0, rows, cols] for k in range(count)]
        return [
            own[k] - all_ref[k + 1, 1, rows, cols] if k + 1 < count else own[k]
            for k in range(count)
        ]

    def low(k, x, transposed=False, right=False):
        block = all_ref[k, 2, :size]
        if right:
            return dot_t(x, block) if transposed else dot(x, block)
        return dot(block, x, ((0,), (0,))) if transposed else dot(block, x)

    thin = slice(size, size + 1), slice(0, 1)
    panels, _ = dense_inverse(
        diag_of(slice(0, size), slice(0, size)),
        low,
        diag_of(*thin),
        [all_ref[k, 2, thin[0], thin[1]] for k in range(count)],
        enough_steps(spread(size)),
    )
    for k, panel in enumerate(panels):
        rows_ref[k] = panel
    me = lax.axis_index("lev")
    own = rows_ref[me]
    above = rows_ref[jnp.maximum(me - 1, 0)]
    inner = dot_t(ends_ref[0], above) + dot_t(ends_ref[1], own)
    length = inner.shape[0]
    high_ref[:length], low_ref[:length] = split(inner)
    high_ref[length:], low_ref[length:] = split(own.T)


def send(src, dst, sems, slot, device):
    return pltpu.make_async_remote_copy(
        src_ref=src,
        dst_ref=dst,
        send_sem=sems.at[0, slot],
        recv_sem=sems.at[1, slot],
        device_id=device,
        device_id_type=pl.DeviceIdType.MESH,
    )


def greet(lev_all, lon_all):
    barrier = pltpu.get_barrier_semaphore()
    partners = []
    for axis, everyone in (("lev", lev_all), ("lon", lon_all)):
        count, me = lax.axis_size(axis), lax.axis_index(axis)
        if everyone is None:
            continue
        steps = range(1, count) if everyone else sorted({1, count - 1})
        partners += [{axis: lax.rem(me + d, count)} for d in steps if d % count]
    for device in partners:
        pl.semaphore_signal(
            barrier, inc=1, device_id=device, device_id_type=pl.DeviceIdType.MESH
        )
    pl.semaphore_wait(barrier, len(partners))


def pack_edges(cur_ref, edges_ref):
    levels, size, columns = cur_ref.shape
    lane = lax.broadcasted_iota(jnp.int32, (size, 128), 1)
    last = jnp.zeros((size, 128), jnp.float32)
    first = last
    for k in range(levels):
        tail = pltpu.roll(cur_ref[k, :, columns - 128 :], k + 1, 1)
        head = cur_ref[k, :, :128]
        head = pltpu.roll(head, k, 1) if k else head
        last = jnp.where(lane == k, tail, last)
        first = jnp.where(lane == k, head, first)
    edges_ref[0] = last
    edges_ref[1] = first


def halo_copies(edges_ref, halo_ref, sems):
    around, me = lax.axis_size("lon"), lax.axis_index("lon")
    return [
        send(edges_ref.at[0], halo_ref.at[0], sems, 0, {"lon": lax.rem(me + 1, around)}),
        send(edges_ref.at[1], halo_ref.at[1], sems, 1, {"lon": lax.rem(me + around - 1, around)}),
    ]


def local_forcing(mix_ref, cur_ref, prev_ref, pair_ref, force_ref):
    levels, size, columns = cur_ref.shape
    lane = lax.broadcasted_iota(jnp.int32, (size, columns), 1)
    for k in range(levels):
        c = cur_ref[k]
        back = jnp.where(lane == 0, 0.0, pltpu.roll(c, 1, 1))
        ahead = jnp.where(lane == columns - 1, 0.0, pltpu.roll(c, columns - 1, 1))
        p_high, p_low = split(pair_ref[k])
        chem = dot3(p_high, p_low, c * c)
        force_ref[k * size : (k + 1) * size] = (
            prev_ref[k] - chem + mix_ref[k] * (back + ahead - 2.0 * c)
        )


def add_halo(mix_ref, halo_ref, force_ref):
    levels = mix_ref.shape[0]
    size, columns = halo_ref.shape[1], force_ref.shape[1]
    lane = lax.broadcasted_iota(jnp.int32, (size, 128), 1)
    before, after = halo_ref[0], halo_ref[1]
    for k in range(levels):
        rows = slice(k * size, (k + 1) * size)
        at_head = pltpu.roll(before, 128 - k, 1) if k else before
        at_tail = pltpu.roll(after, 127 - k, 1)
        force_ref[rows, :128] += jnp.where(lane == 0, mix_ref[k] * at_head, 0.0)
        force_ref[rows, columns - 128 :] += jnp.where(lane == 127, mix_ref[k] * at_tail, 0.0)


def couple(
    links_ref, top_link, g_high, g_low, force_ref, part_ref, f_high, f_low, top_out, top_in, sides_ref,
    sems, direct,
):
    count, me = lax.axis_size("lev"), lax.axis_index("lev")
    inner, size = part_ref.shape[0], top_out.shape[0]
    f_high[...], f_low[...] = split(force_ref[:inner])
    mul = functools.partial(jnp.dot, preferred_element_type=jnp.float32)

    def rows_of(start, stop):
        a, b = g_high[start:stop], g_low[start:stop]
        part = mul(a, f_high[...]) + (mul(b, f_high[...]) + mul(a, f_low[...]))
        part_ref[start:stop] = part
        return part

    top_out[...] = top_link * rows_of(0, size)
    sides_ref[me] = force_ref[inner:] + links_ref[inner // size - 1] * rows_of(inner - size, inner)
    up = send(top_out, top_in, sems, 0, {"lev": lax.rem(me + count - 1, count)})
    half = size * ((inner // size) // 2)

    @pl.when(me > 0)
    def _():
        up.start()

    rows_of(size, half)

    @pl.when(me < count - 1)
    def _():
        up.wait_recv()
        sides_ref[me] += top_in[...]

    partner = me + 1 - 2 * lax.rem(me, 2)
    copies = [
        send(sides_ref.at[me], sides_ref.at[me], sems, d, {"lev": lax.rem(me + d, count)})
        for d in range(1 if direct else 2, count, 1 if direct else 2)
    ]
    onward = [] if direct else [send(sides_ref.at[me], sides_ref.at[me], sems, 1, {"lev": partner})]
    for d in range(count if direct else 2, count, 2):
        origin = lax.rem(me - d + count, count)
        onward.append(
            send(sides_ref.at[origin], sides_ref.at[origin], sems, d + 1, {"lev": partner})
        )
    for copy in copies + onward[:1]:
        copy.start()
    rows_of(half, inner - size)

    @pl.when(me > 0)
    def _():
        up.wait_send()

    return copies, onward


def relay(copies, onward):
    for copy, later in zip(copies, onward[1:]):
        copy.wait_recv()
        later.start()
    for copy in copies:
        copy.wait_send()
    for copy in onward:
        copy.wait()


def finish(part_ref, sides_ref, high_ref, low_ref, out_ref):
    levels, size, columns = out_ref.shape
    count = sides_ref.shape[0]
    b_high, b_low = split(sides_ref[...].reshape(count * size, columns))
    mul = functools.partial(jnp.dot, preferred_element_type=jnp.float32)
    for k in range(levels):
        rows = slice(k * size, (k + 1) * size)
        a, b = high_ref[rows], low_ref[rows]
        row = mul(a, b_high) + (mul(b, b_high) + mul(a, b_low))
        out_ref[k] = row + part_ref[rows] if k < levels - 1 else row


def open_kernel(
    links_ref, mix_ref, prev_ref, pair_ref, force_ref, top_ref, edges, halo, link_out, sems
):
    levels = prev_ref.shape[0]
    count, me = lax.axis_size("lev"), lax.axis_index("lev")
    pack_edges(prev_ref, edges)
    link_out[...] = jnp.full(link_out.shape, links_ref[levels - 1], jnp.float32)
    greet(False, False)
    copies = halo_copies(edges, halo, sems)
    down = send(link_out, top_ref, sems, 2, {"lev": lax.rem(me + 1, count)})
    for copy in copies:
        copy.start()

    @pl.when(me < count - 1)
    def _():
        down.start()

    @pl.when(me == 0)
    def _():
        top_ref[...] = jnp.zeros(top_ref.shape, jnp.float32)

    local_forcing(mix_ref, prev_ref, prev_ref, pair_ref, force_ref)
    for copy in copies:
        copy.wait()
    add_halo(mix_ref, halo, force_ref)

    @pl.when(me < count - 1)
    def _():
        down.wait_send()

    @pl.when(me > 0)
    def _():
        down.wait_recv()


def newton_kernel(
    links_ref, mix_ref, top_ref, sent_ref, ends_ref, first_force, g_high, g_low, prev_ref, pair_ref,
    out_ref, var_ref, all_ref, rows_ref, h_high, h_low, cur_ref, edges, halo, force_ref, part_ref,
    first_sides, sides_ref, f_high, f_low, first_out, first_in, top_out, top_in, sums_ref,
    block_sems, first_sems, halo_sems, sems, sum_sems,
):
    levels, size, columns = prev_ref.shape
    count, me = lax.axis_size("lev"), lax.axis_index("lev")
    around, place = lax.axis_size("lon"), lax.axis_index("lon")
    greet(True, True)
    blocks = [
        send(sent_ref, all_ref.at[me], block_sems, d, {"lev": lax.rem(me + d, count)})
        for d in range(1, count)
    ]
    for copy in blocks:
        copy.start()
    all_ref[me] = sent_ref[...]
    copies = couple(
        links_ref, top_ref[0:1, 0:1], g_high, g_low, first_force, part_ref, f_high, f_low,
        first_out, first_in, first_sides, first_sems, True,
    )
    for copy in blocks:
        copy.wait()
    interface(all_ref, ends_ref, h_high, h_low, rows_ref)
    for copy in copies[0]:
        copy.wait()
    finish(part_ref, first_sides, h_high, h_low, cur_ref)
    pack_edges(cur_ref, edges)
    copies = halo_copies(edges, halo, halo_sems)
    for copy in copies:
        copy.start()
    local_forcing(mix_ref, cur_ref, prev_ref, pair_ref, force_ref)
    for copy in copies:
        copy.wait()
    add_halo(mix_ref, halo, force_ref)
    copies = couple(
        links_ref, top_ref[0:1, 0:1], g_high, g_low, force_ref, part_ref, f_high, f_low,
        top_out, top_in, sides_ref, sems, False,
    )
    relay(*copies)
    finish(part_ref, sides_ref, h_high, h_low, out_ref)
    lane = lax.broadcasted_iota(jnp.int32, (size, 128), 1)
    total = jnp.zeros((size, 128), jnp.float32)
    for k in range(levels):
        row = out_ref[k]
        total = jnp.where(lane == k, jnp.sum(row * row, axis=1, keepdims=True), total)
    sums_ref[0] = total.T[: sums_ref.shape[1]]
    copies = [
        send(sums_ref.at[0], sums_ref.at[d], sum_sems, d, {"lon": lax.rem(place + d, around)})
        for d in range(1, around)
    ]
    for copy in copies:
        copy.start()
    for copy in copies:
        copy.wait()
    total = sums_ref[place]
    for j in range(1, around):
        total = total + sums_ref[lax.rem(place - j + around, around)]
    var_ref[...] = (total / (columns * around))[:levels]


def call(kernel, outs, places, scratch=(), group=None):
    extra = {} if group is None else {"collective_id": group, "has_side_effects": True}
    return pl.pallas_call(
        kernel,
        out_shape=[jax.ShapeDtypeStruct(shape, dtype) for shape, dtype in outs],
        in_specs=places,
        out_specs=[VMEM] * len(outs),
        scratch_shapes=list(scratch),
        compiler_params=pltpu.CompilerParams(vmem_limit_bytes=60 * 2**20, **extra),
    )


def local(previous, loss_matrix, pair_matrix, diffusivity, mixing):
    levels, size, columns = previous.shape
    count = lax.axis_size("lev")
    around = lax.axis_size("lon")
    inner = (levels - 1) * size
    f32, bf16 = jnp.float32, jnp.bfloat16
    buf, sem = pltpu.VMEM, lambda n: pltpu.SemaphoreType.DMA((2, n))
    force, top = call(
        open_kernel,
        [((levels * size, columns), f32), ((8, 128), f32)],
        [SMEM, SMEM, VMEM, VMEM],
        [buf((2, size, 128), f32), buf((2, size, 128), f32), buf((8, 128), f32), sem(3)],
        0,
    )(diffusivity, mixing, previous, pair_matrix)
    g_high, g_low, ends, sent = call(
        factor_kernel,
        [((inner, inner), bf16), ((inner, inner), bf16), ((2, inner, size), f32), ((3, size + 8, size), f32)],
        [SMEM, VMEM, VMEM],
    )(diffusivity, top, loss_matrix)
    return call(
        newton_kernel,
        [((levels, size, columns), f32), ((levels, size), f32)],
        [SMEM, SMEM] + [VMEM] * 8,
        [
            buf((count, 3, size + 8, size), f32),
            buf((count, count * size, size), f32),
            buf((levels * size, count * size), bf16),
            buf((levels * size, count * size), bf16),
            buf((levels, size, columns), f32),
            buf((2, size, 128), f32),
            buf((2, size, 128), f32),
            buf((levels * size, columns), f32),
            buf((inner, columns), f32),
            buf((count, size, columns), f32),
            buf((count, size, columns), f32),
            buf((inner, columns), bf16),
            buf((inner, columns), bf16),
            buf((size, columns), f32),
            buf((size, columns), f32),
            buf((size, columns), f32),
            buf((size, columns), f32),
            buf((around, -(-levels // 8) * 8, size), f32),
            sem(count),
            sem(count),
            sem(2),
            sem(count),
            sem(around),
        ],
        1,
    )(diffusivity, mixing, top, sent, ends, force, g_high, g_low, previous, pair_matrix)


def cat3(a_high, a_low, b_high, b_low):
    return jnp.dot(
        jnp.concatenate([a_high, a_low, a_high], axis=1),
        jnp.concatenate([b_high, b_high, b_low], axis=0),
        preferred_element_type=jnp.float32,
    )


def wide(a):
    high, low = split(a)
    return jnp.concatenate([high, low, high, jnp.zeros_like(high)], axis=1)


def tall(b):
    high, low = split(b)
    return jnp.concatenate([high, high, low, jnp.zeros_like(high)], axis=0)


def wide_dot(a, b):
    return jnp.dot(a, b, preferred_element_type=jnp.float32)


def near_dot(a, b):
    return lax.dot_general(
        a, b, (((1,), (0,)), ((), ())), precision=lax.Precision.HIGH, preferred_element_type=jnp.float32
    )


def pull(links, loss):
    stiff = links[0]
    for a in links[1:]:
        own = 1.0 + loss + stiff
        stiff = a * own / (a + own)
    return stiff


def worst_ratio(above, below):
    sides = []
    for count in (above, below):
        draws = itertools.product((200.0, 2000.0), repeat=min(count, 8) + 1)
        sides.append([(pull(d, 640.0), pull(d, 0.05)) for d in draws])
    return 1.15 * max((641.0 + a + c) / (1.05 + b + d) for a, b in sides[0] for c, d in sides[1])


def gains_for(ratio):
    rho, gains = (ratio - 1.0) / (ratio + 1.0), []
    while rho > 1.2e-3:
        gains.append(2.0 / (2.0 - rho * rho))
        rho = rho * rho / (2.0 - rho * rho)
    return gains


def invert_fixed(blocks, floors, ratio):
    size = blocks[0].shape[0]
    unit = jnp.where(eye_of(size), 1.0, 0.0).astype(jnp.float32)
    gains = gains_for(ratio)
    xs, rests = [], []
    for a, low in zip(blocks, floors):
        scale = (2.0 / (1.0 + ratio)) / low
        rest = unit - scale * a
        xs.append((gains[0] * scale) * (unit + rest))
        rests.append(rest)
    rests = [gains[0] * dot(r, r) - (gains[0] - 1.0) * unit for r in rests]
    for step, g in enumerate(gains[1:]):
        left = len(gains) - step - 2
        mul = dot if left > 2 else near_dot
        if left == 0:
            xs = [g * (x + mul(x, r)) for x, r in zip(xs, rests)]
            break
        both = [mul(jnp.concatenate([x, r], axis=0), r) for x, r in zip(xs, rests)]
        xs = [g * (x + b[:size]) for x, b in zip(xs, both)]
        rests = [g * b[size:] - (g - 1.0) * unit for b in both]
    rests = [unit - dot(a, x) for a, x in zip(blocks, xs)]
    return [x + near_dot(x, r) for x, r in zip(xs, rests)]


def chain_factor(diag, links, floors, panel_ref, hook):
    count, size = len(diag), diag[0].shape[0]
    unit = jnp.where(eye_of(size), 1.0, 0.0).astype(jnp.float32)
    by_depth, thin, corners = {}, {}, {}
    plan(0, count, by_depth)

    def rows(lo, hi):
        return slice(lo * size, hi * size)

    for depth in sorted(by_depth):
        nodes = by_depth[depth]
        ratio = max(worst_ratio(mid - lo, hi - 1 - mid) for lo, mid, hi in nodes)
        schur, arms, lows, thin_arms = [], [], [], []
        for lo, mid, hi in nodes:
            s, parts = diag[mid], []
            t, thin_parts = floors[mid], []
            if lo < mid:
                arm = links[mid] * panel_ref[mid - 1, rows(lo, mid)]
                s = s - (links[mid] * links[mid]) * corners[lo, mid][1]
                parts.append(arm)
                thin_parts += [links[mid] * x for x in thin[lo, mid][-1]]
                t = t - links[mid] * thin_parts[-1]
            parts.append(unit)
            thin_parts.append(1.0)
            if mid + 1 < hi:
                arm = links[mid + 1] * panel_ref[mid + 1, rows(mid + 1, hi)]
                s = s - (links[mid + 1] * links[mid + 1]) * corners[mid + 1, hi][0]
                parts.append(arm)
                thin_arm = [links[mid + 1] * x for x in thin[mid + 1, hi][0]]
                t = t - links[mid + 1] * thin_arm[0]
                thin_parts += thin_arm
            schur.append(s)
            lows.append(t)
            arms.append(jnp.concatenate(parts, axis=0) if len(parts) > 1 else parts[0])
            thin_arms.append(thin_parts)
        inverses = invert_fixed(schur, [0.97 * t for t in lows], ratio)
        for (lo, mid, hi), v, z, thin_v, t in zip(nodes, arms, inverses, thin_arms, lows):
            thin[lo, hi] = [[a * b / t for b in thin_v] for a in thin_v]
            for a, b in ((lo, mid), (mid + 1, hi)):
                for i in range(a, b):
                    for j in range(a, b):
                        thin[lo, hi][i - lo][j - lo] += thin[a, b][i - a][j - a]
            if hi - lo == 1:
                panel_ref[mid, rows(mid, hi)] = z
                corners[lo, hi] = z, z
                continue
            ends = v[:size], v[-size:]
            arms_out = [dot(x, z) for x in ends]
            corners[lo, hi] = tuple(
                z if at == mid else corners[part][side] + dot_t(y, x)
                for side, (at, part, x, y) in enumerate(
                    ((lo, (lo, mid), ends[0], arms_out[0]), (hi - 1, (mid + 1, hi), ends[1], arms_out[1]))
                )
            )
            if hi - lo == count:
                far = dot_t(arms_out[1], ends[0])
            w = dot(v, z)
            if hi - lo == count:
                continue
            new = dot_t(w, v)
            for k in range(lo, hi):
                own = new[:, (k - lo) * size : (k - lo + 1) * size]
                panel_ref[k, rows(mid, mid + 1)] = own[rows(mid - lo, mid - lo + 1)]
                for a, b in ((lo, mid), (mid + 1, hi)):
                    if a >= b:
                        continue
                    piece = own[rows(a - lo, b - lo)]
                    if a <= k < b:
                        piece = piece + panel_ref[k, rows(a, b)]
                    panel_ref[k, rows(a, b)] = piece
        if depth < max(by_depth):
            hook(depth)
    return v, w, by_depth[max(by_depth)][0][1], thin[0, count], (*corners[0, count], far)


def fold(x):
    half = x.shape[0] // 2
    return jnp.concatenate([x[:half], x[half:]], axis=1)


def unfold(x):
    half = x.shape[1] // 2
    return jnp.concatenate([x[:, :half], x[:, half:]], axis=0)


def pack_pairs(field_ref, columns, edges_ref):
    levels, size = field_ref.shape[:2]
    lane = lax.broadcasted_iota(jnp.int32, (size, 128), 1)
    last = jnp.zeros((size, 128), jnp.float32)
    first = last
    for k in range(levels):
        tail = pltpu.roll(field_ref[k, :, columns - 128 : columns], (2 * k + 2) % 128, 1)
        head = field_ref[k, :, :128]
        head = pltpu.roll(head, 2 * k, 1) if k else head
        mine = (lane == 2 * k) | (lane == 2 * k + 1)
        last = jnp.where(mine, tail, last)
        first = jnp.where(mine, head, first)
    edges_ref[0] = last
    edges_ref[1] = first


def unpack_pairs(halo_ref, columns, field_ref):
    levels, size = field_ref.shape[:2]
    lane = lax.broadcasted_iota(jnp.int32, (size, 128), 1)
    before, after = halo_ref[0], halo_ref[1]
    for k in range(levels):
        at_head = pltpu.roll(after, (128 - 2 * k) % 128, 1) if k else after
        at_tail = pltpu.roll(before, (126 - 2 * k) % 128, 1)
        field_ref[k, :, columns:] = jnp.where(lane < 2, at_head, jnp.where(lane >= 126, at_tail, 0.0))


def forcing(mix_ref, cur_ref, prev_ref, pairs_ref, width, sep_ref, f_high, f_low):
    levels, size, full = cur_ref.shape
    for k in range(levels):
        c = cur_ref[k]
        ring = pltpu.roll(c, 1, 1) + pltpu.roll(c, full - 1, 1)
        own = c[:, :width]
        chem = wide_dot(pairs_ref[k], tall(own * own))
        force = prev_ref[k, :, :width] - chem + mix_ref[k] * (ring[:, :width] - 2.0 * own)
        if k == 0:
            sep_ref[:, :width] = force
        else:
            rows = slice((k - 1) * size, k * size)
            f_high[rows, :width], f_low[rows, :width] = split(force)


def start_all(copies):
    @pl.when(lax.axis_index("lev") < lax.axis_size("lev"))
    def _():
        for copy in copies:
            copy.start()


def step_kernel(
    links_hbm, mix_hbm, loss_hbm, prev_hbm, pair_hbm, out_ref, var_ref, links_ref, mix_ref,
    loss_ref, prev_ref, pair_ref, pairs_ref, edges, halo, z_high, z_low, send_ref, all_ref,
    ends_high, ends_low, table_ref, sep_ref, f_high, f_low, part_ref, own_ref, near_ref, mine_ref, far_ref,
    side_high, side_low, hq_high, hq_low, u_ref, top_ref, cur_ref, sums_ref, panel_ref, w_ref, v_ref,
    load_sems, halo_sems, block_sems, near_sems, far_sems, sum_sems,
):
    levels, size, columns = prev_hbm.shape
    inner = levels - 1
    full = cur_ref.shape[2]
    count, me = lax.axis_size("lev"), lax.axis_index("lev")
    around, place = lax.axis_size("lon"), lax.axis_index("lon")
    core, chip = lax.rem(me, 2), me // 2
    partner = me + 1 - 2 * core
    across = lax.rem(me + 2, count)

    loads = [
        pltpu.make_async_copy(loss_hbm, loss_ref, load_sems.at[0]),
        pltpu.make_async_copy(prev_hbm, prev_ref.at[:, :, pl.ds(0, columns)], load_sems.at[1]),
        pltpu.make_async_copy(pair_hbm, pair_ref, load_sems.at[2]),
        pltpu.make_async_copy(links_hbm, links_ref, load_sems.at[3]),
        pltpu.make_async_copy(mix_hbm, mix_ref, load_sems.at[4]),
    ]
    for k in (3, 0, 1, 2, 4):
        loads[k].start()
    barrier = pltpu.get_barrier_semaphore()
    partners = [{"lev": lax.rem(me + d, count)} for d in range(1, count)]
    partners += [{"lon": lax.rem(place + d, around)} for d in range(1, around)]
    for device in partners:
        pl.semaphore_signal(barrier, inc=1, device_id=device, device_id_type=pl.DeviceIdType.MESH)

    loads[3].wait()
    links = [jnp.full((1, 1), links_ref[k]) for k in range(levels)]
    on_diag = eye_of(size)
    halo_moves = halo_copies(edges, halo, halo_sems)

    def hook(depth):
        if depth != 2:
            return
        loads[1].wait()
        pack_pairs(prev_ref, columns, edges)
        pl.semaphore_wait(barrier, len(partners))
        start_all(halo_moves)

    loads[0].wait()
    diag = [
        loss_ref[k] + jnp.where(on_diag, 1.0 + links[k] + (links[k - 1] if k else 0.0), 0.0)
        for k in range(levels)
    ]
    floors = [LEAST + links[k] + (links[k - 1] if k else 0.0) for k in range(levels)]
    v, w, mid, thin, (z_first, z_last, z_far) = chain_factor(diag[1:], links[:inner], floors[1:], panel_ref, hook)
    a, b = links[0], links[inner]
    sub = lax.broadcasted_iota(jnp.int32, (8, 128), 0)
    send_ref[: size // 2] = fold(diag[0] - a * a * z_first)
    send_ref[size // 2 : size] = fold(jnp.where(on_diag, b, 0.0) - b * b * z_last)
    send_ref[size : 3 * size // 2] = fold(a * b * z_far)
    send_ref[3 * size // 2 :] = jnp.where(
        sub == 0, floors[0] - a * a * thin[0][0], jnp.where(sub == 1, b - b * b * thin[-1][-1], a * b * thin[0][-1])
    )
    blocks = [
        send(send_ref, all_ref.at[me], block_sems, d, {"lev": lax.rem(me + d, count)})
        for d in range(1, count)
    ]
    start_all(blocks)
    all_ref[me] = send_ref[...]

    old = [
        panel_ref[0, : mid * size],
        jnp.zeros((size, size), jnp.float32),
        panel_ref[inner - 1, (mid + 1) * size :],
    ]
    tips = dot_t(w, jnp.concatenate([v[:size], v[-size:]], axis=0))
    first = tips[:, :size] + jnp.concatenate([old[0], old[1], jnp.zeros_like(old[2])], axis=0)
    last = tips[:, size:] + jnp.concatenate([jnp.zeros_like(old[0]), old[1], old[2]], axis=0)
    ends_high[...], ends_low[...] = split(jnp.concatenate([a * first, b * last], axis=1))
    w_ref[...] = wide(w)
    v_high, v_low = split(v)
    v_ref[...] = jnp.concatenate([v_high, v_high, v_low, jnp.zeros_like(v_high)], axis=1)

    def form(lo, hi):
        spot = slice(lo * size, hi * size)
        new = lax.dot_general(
            w_ref[spot], v_ref[...], (((1,), (1,)), ((), ())), preferred_element_type=jnp.float32
        )
        start, stop = (0, mid) if lo < mid else (mid + 1, inner)
        if lo != mid:
            zeros = jnp.zeros((new.shape[0], size), jnp.float32)
            new = new + jnp.concatenate(
                [panel_ref[j, spot] if start <= j < stop else zeros for j in range(inner)], axis=1
            )
        z_high[spot], z_low[spot] = split(new)

    form(0, 1)
    form(inner - 1, inner)
    loads[2].wait()
    loads[4].wait()
    for k in range(levels):
        pairs_ref[k] = wide(pair_ref[k])
    for move in halo_moves:
        move.wait()
    unpack_pairs(halo, columns, prev_ref)

    def z_rows(start, stop, width):
        return cat3(z_high[start:stop], z_low[start:stop], f_high[:, :width], f_low[:, :width])

    def ends(turn, width):
        rows = cat3(
            jnp.concatenate([z_high[:size], z_high[-size:]], axis=0),
            jnp.concatenate([z_low[:size], z_low[-size:]], axis=0),
            f_high[:, :width],
            f_low[:, :width],
        )
        part_ref[:size, :width] = rows[:size]
        part_ref[-size:, :width] = rows[size:]
        own_ref[turn, 0, :, :width] = sep_ref[:, :width] + a * rows[:size]
        own_ref[turn, 1, :, :width] = b * rows[size:]
        copy = send(
            own_ref.at[turn, :, :, pl.ds(0, width)], near_ref.at[turn, :, :, pl.ds(0, width)], near_sems, turn,
            {"lev": partner},
        )
        start_all([copy])
        return copy

    def middle(width):
        part_ref[size:-size, :width] = z_rows(size, (inner - 1) * size, width)

    def merge(turn, width):
        upper = core == 0
        s_own, t_own = own_ref[turn, 0, :, :width], own_ref[turn, 1, :, :width]
        s_in, t_in = near_ref[turn, 0, :, :width], near_ref[turn, 1, :, :width]
        low_side = jnp.where(upper, s_own, s_in)
        high_side = jnp.where(upper, s_in + t_own, s_own + t_in)
        side_high[:size, :width], side_low[:size, :width] = split(low_side)
        side_high[size:, :width], side_low[size:, :width] = split(high_side)
        return jnp.where(chip == 0, jnp.where(upper, t_in, t_own), 0.0)

    def condense(turn, width, tail, k_high, k_low):
        mine_ref[turn, :, :width] = tail + cat3(k_high, k_low, side_high[:, :width], side_low[:, :width])
        half, quarter = columns // 2, columns // 4
        first = pl.ds(pl.multiple_of(core * half, 128), quarter)
        second = pl.ds(pl.multiple_of(core * half + quarter, 128), quarter)
        routes = [(mine_ref, first, across), (mine_ref, second, across), (mine_ref, second, lax.rem(partner + 2, count))]
        routes += [(mine_ref, pl.ds(columns, width - columns), across)] if width > columns else []
        routes += [(far_ref, first, partner)]
        copies = [
            send(src.at[turn, :, spot], far_ref.at[turn, :, spot], far_sems, 5 * turn + k, {"lev": device})
            for k, (src, spot, device) in enumerate(routes)
        ]
        start_all(copies[:-1])
        return copies

    def relay_far(copies):
        copies[0].wait_recv()
        start_all(copies[-1:])

    def wait_far(copies):
        copies[0].wait_send()
        for copy in copies[1:]:
            copy.wait()

    def gather_sides(width):
        rest = cat3(hq_high[...], hq_low[...], side_high[:, :width], side_low[:, :width])
        for k in range(levels):
            rows = rest[k * size : (k + 1) * size]
            cur_ref[k, :, :width] = rows if k == 0 else rows + part_ref[(k - 1) * size : k * size, :width]

    def finish(turn, width, to_ref):
        total = mine_ref[turn, :, :width] + far_ref[turn, :, :width]
        top = tall(wide_dot(top_ref[...], tall(total)))
        for k in range(levels):
            to_ref[k, :, :width] = cur_ref[k, :, :width] + wide_dot(u_ref[k * size : (k + 1) * size], top)

    forcing(mix_ref, prev_ref, prev_ref, pairs_ref, full, sep_ref, f_high, f_low)
    near = ends(0, full)
    for lo, hi in ((1, mid), (mid, mid + 1), (mid + 1, inner - 1)):
        form(lo, hi)
    middle(full)
    for copy in blocks:
        copy.wait()

    def block(k, which):
        return unfold(all_ref[k, which * size // 2 : (which + 1) * size // 2])

    def floor(k, which):
        row = 3 * size // 2 + which
        return all_ref[k, row : row + 1, 0:1]

    ratio = spread(size)
    s = [block(k, 0) + (block(k - 1, 1) if k else 0.0) for k in range(count)]
    t = [floor(k, 0) + (floor(k - 1, 1) if k else 0.0) for k in range(count)]
    c = [None] + [block(k, 2) for k in range(count - 1)]
    e = [None] + [floor(k, 2) for k in range(count - 1)]
    z0, z3 = invert_fixed([s[0], s[3]], [0.97 * t[0], 0.97 * t[3]], ratio)
    a1, a3 = dot(c[1], z0), dot(z3, c[3])
    s1 = s[1] - dot_t(a1, c[1])
    t1 = t[1] - e[1] * e[1] / t[0]
    (z1,) = invert_fixed([s1], [0.97 * t1], ratio)
    a2 = dot(c[2], z1)
    s2 = s[2] - dot_t(a2, c[2]) - dot(c[3], a3, ((0,), (0,)))
    t2 = t[2] - e[2] * e[2] / t1 - e[3] * e[3] / t[3]
    b1 = dot(z1, a1)
    p0 = dot(a2, a1)
    zero = jnp.zeros((size, size), jnp.float32)
    unit = jnp.where(on_diag, 1.0, 0.0).astype(jnp.float32)
    sides = [
        (z0 + dot(a1, b1, ((0,), (0,))), b1.T, p0.T),
        (b1, z1, a2.T),
        (zero, zero, unit),
        (zero, z3, a3),
        (zero, zero, zero),
    ]
    for k, (left, right, top) in enumerate(sides):
        table_ref[k, :size] = jnp.concatenate([left, right], axis=1)
        table_ref[k, size:, :size] = top
    for k, (left, right) in enumerate(((p0, a2), (unit, a3.T))):
        table_ref[len(sides) + k, :size] = jnp.concatenate([left, right], axis=1)
    near.wait()
    tail = merge(0, full)
    k_high, k_low = split(table_ref[len(sides) + chip, :size])
    far = condense(0, full, tail, k_high, k_low)
    (z2,) = invert_fixed([s2], [0.97 * t2], ratio)
    top_ref[...] = wide(z2)
    own_q, next_q = table_ref[me, :size], table_ref[me + 1, :size]
    own_p, next_p = table_ref[me, size:, :size], table_ref[me + 1, size:, :size]
    q_high, q_low = split(jnp.concatenate([own_q, next_q], axis=0))
    p_high, p_low = split(jnp.concatenate([own_p, next_p], axis=0))
    hq_high[size:], hq_low[size:] = split(cat3(ends_high[...], ends_low[...], q_high, q_low))
    hq_high[:size], hq_low[:size] = split(own_q)
    u_ref[size:] = wide(cat3(ends_high[...], ends_low[...], p_high, p_low))
    u_ref[:size] = wide(own_p)
    relay_far(far)
    gather_sides(full)
    wait_far(far)
    finish(0, full, cur_ref)

    forcing(mix_ref, cur_ref, prev_ref, pairs_ref, columns, sep_ref, f_high, f_low)
    near = ends(1, columns)
    near.wait()
    tail = merge(1, columns)
    far = condense(1, columns, tail, k_high, k_low)
    middle(columns)
    gather_sides(columns)
    relay_far(far)
    wait_far(far)
    finish(1, columns, out_ref)
    lane = lax.broadcasted_iota(jnp.int32, (size, 128), 1)
    total = jnp.zeros((size, 128), jnp.float32)
    for k in range(levels):
        row = out_ref[k]
        total = jnp.where(lane == k, jnp.sum(row * row, axis=1, keepdims=True), total)
    held = sums_ref.shape[1]
    total = total.T
    sums_ref[0] = jnp.concatenate([total[:held], total[held : 2 * held]], axis=1)
    copies = [
        send(sums_ref.at[0], sums_ref.at[d], sum_sems, d, {"lon": lax.rem(place + d, around)})
        for d in range(1, around)
    ]
    start_all(copies)
    for copy in copies:
        copy.wait()
    total = sums_ref[place]
    for j in range(1, around):
        total = total + sums_ref[lax.rem(place - j + around, around)]
    total = total / (columns * around)
    total = jnp.concatenate([total[:, :size], total[:, size:]], axis=0)
    var_ref[...] = total[:levels]


def hand_out(from_out, from_var, to_out, to_var, sems):
    copies = [
        pltpu.make_async_copy(from_out, to_out, sems.at[0]),
        pltpu.make_async_copy(from_var, to_var, sems.at[1]),
    ]
    for copy in copies:
        copy.start()
    for copy in copies:
        copy.wait()


def local_pairs(previous, loss_matrix, pair_matrix, diffusivity, mixing):
    levels, size, columns = previous.shape
    count, around = lax.axis_size("lev"), lax.axis_size("lon")
    inner, full = (levels - 1) * size, columns + 128
    f32, bf16 = jnp.float32, jnp.bfloat16
    buf, sem = pltpu.VMEM, lambda n: pltpu.SemaphoreType.DMA((2, n))
    hbm = pl.BlockSpec(memory_space=pltpu.MemorySpace.HBM)
    packed = 3 * size // 2 + 8
    results = pl.pallas_call(
        step_kernel,
        out_shape=[
            jax.ShapeDtypeStruct((levels, size, columns), f32),
            jax.ShapeDtypeStruct((levels, size), f32),
        ],
        in_specs=[hbm] * 5,
        out_specs=[VMEM, VMEM],
        scratch_shapes=[
            pltpu.SMEM((levels,), f32),
            pltpu.SMEM((levels,), f32),
            buf((levels, size, size), f32),
            buf((levels, size, full), f32),
            buf((levels, size, size), f32),
            buf((levels, size, 4 * size), bf16),
            buf((2, size, 128), f32),
            buf((2, size, 128), f32),
            buf((inner, inner), bf16),
            buf((inner, inner), bf16),
            buf((packed, 2 * size), f32),
            buf((count, packed, 2 * size), f32),
            buf((inner, 2 * size), bf16),
            buf((inner, 2 * size), bf16),
            buf((count + 3, 2 * size, 2 * size), f32),
            buf((size, full), f32),
            buf((inner, full), bf16),
            buf((inner, full), bf16),
            buf((inner, full), f32),
            buf((2, 2, size, full), f32),
            buf((2, 2, size, full), f32),
            buf((2, size, full), f32),
            buf((2, size, full), f32),
            buf((2 * size, full), bf16),
            buf((2 * size, full), bf16),
            buf((levels * size, 2 * size), bf16),
            buf((levels * size, 2 * size), bf16),
            buf((levels * size, 4 * size), bf16),
            buf((size, 4 * size), bf16),
            buf((levels, size, full), f32),
            buf((around, -(-levels // 16) * 8, 2 * size), f32),
            buf((levels - 1, inner, size), f32),
            buf((inner, 4 * size), bf16),
            buf((inner, 4 * size), bf16),
            pltpu.SemaphoreType.DMA((5,)),
            sem(2),
            sem(count),
            sem(2),
            sem(10),
            sem(around),
        ],
        compiler_params=pltpu.CompilerParams(
            vmem_limit_bytes=40 * 2**20, collective_id=2, has_side_effects=True
        ),
    )(*(pltpu.with_memory_space_constraint(x, pltpu.MemorySpace.HBM) for x in (diffusivity, mixing, loss_matrix, previous, pair_matrix)))
    return pl.pallas_call(
        hand_out,
        out_shape=[jax.ShapeDtypeStruct(x.shape, x.dtype) for x in results],
        in_specs=[VMEM, VMEM],
        out_specs=[hbm, hbm],
        scratch_shapes=[pltpu.SemaphoreType.DMA((2,))],
        compiler_params=pltpu.CompilerParams(vmem_limit_bytes=2**20),
    )(*results)


def chosen(previous, *rest):
    paired = lax.axis_size("lev") == 4 and previous.shape[2] % 512 == 0
    return (local_pairs if paired else local)(previous, *rest)


def solution(mesh):
    placed = (P("lev", None, "lon"), P("lev", None, None), P("lev", None, None), P("lev"), P("lev"))
    return jax.shard_map(
        chosen,
        mesh=mesh,
        in_specs=placed,
        out_specs=(P("lev", None, "lon"), P("lev", None)),
        check_vma=False,
    )
```

```python
import functools
import itertools

import jax
import jax.numpy as jnp
from jax import lax
from jax.experimental import pallas as pl
from jax.experimental.pallas import tpu as pltpu
from jax.sharding import PartitionSpec as P

LEAST = 1.05
MOST = 10.0
HIGHEST = lax.Precision.HIGHEST
SMEM = pl.BlockSpec(memory_space=pltpu.SMEM)
VMEM = pl.BlockSpec(memory_space=pltpu.VMEM)


def dot(a, b, dims=((1,), (0,))):
    return lax.dot_general(
        a, b, (dims, ((), ())), precision=HIGHEST, preferred_element_type=jnp.float32
    )


def dot_t(a, b):
    return dot(a, b, ((1,), (1,)))


def eye_of(size):
    rows = lax.broadcasted_iota(jnp.int32, (size, size), 0)
    cols = lax.broadcasted_iota(jnp.int32, (size, size), 1)
    return rows == cols


def invert_all(blocks, floors, steps):
    size = blocks[0].shape[0]
    unit = jnp.where(eye_of(size), 1.0, 0.0).astype(jnp.float32)
    start, worst = [], None
    for a, lo in zip(blocks, floors):
        hi = jnp.max(jnp.sum(jnp.abs(a), axis=0, keepdims=True), axis=1, keepdims=True)
        hi = jnp.clip(hi, lo, lo * spread(size))
        scale = 2.0 / (hi + lo)
        rho = (hi - lo) / (hi + lo)
        start.append((scale, a))
        worst = rho if worst is None else jnp.maximum(worst, rho)

    def grow(rho):
        square = rho * rho
        return square / (2.0 - square), 2.0 / (2.0 - square)

    rho, gain = grow(worst)
    start = [(gain * scale) * (2.0 * unit - scale * a) for scale, a in start]

    def step(carry):
        rho, *xs = carry
        rest = [unit - dot(a, x) for a, x in zip(blocks, xs)]
        rho, gain = grow(rho)
        return (rho, *[gain * (x + dot(x, r)) for x, r in zip(xs, rest)])

    if steps is None:
        return lax.while_loop(lambda carry: jnp.max(carry[0]) > 3e-8, step, (rho, *start))[1:]
    return lax.fori_loop(0, steps, lambda i, carry: step(carry), (rho, *start))[1:]


def spread(size):
    return (1.0 + MOST * size) / (0.96 * LEAST)


def enough_steps(condition):
    rho, steps = (condition - 1.0) / (condition + 1.0), -1
    while rho > 3e-8:
        rho, steps = rho * rho / (2.0 - rho * rho), steps + 1
    return steps


def plan(lo, hi, out):
    if lo >= hi:
        return 0
    mid = lo + (hi - lo) // 2
    depth = 1 + max(plan(lo, mid, out), plan(mid + 1, hi, out))
    out.setdefault(depth, []).append((lo, mid, hi))
    return depth


def dense_inverse(diag, low, floor_diag, floor_low, steps=None):
    count, size = len(diag), diag[0].shape[0]
    unit = jnp.where(eye_of(size), 1.0, 0.0).astype(jnp.float32)
    by_depth, done, thin = {}, {}, {}
    plan(0, count, by_depth)
    for depth in sorted(by_depth):
        nodes = by_depth[depth]
        schur, arms, floors, thin_arms = [], [], [], []
        for lo, mid, hi in nodes:
            s, parts = diag[mid], []
            t, thin_parts = floor_diag[mid], []
            if lo < mid:
                arm = low_right(done[lo, mid][-1], low, mid, False)
                s = s - low(mid, arm[-size:])
                parts.append(arm)
                thin_parts += [floor_low[mid] * x for x in thin[lo, mid][-1]]
                t = t - floor_low[mid] * thin_parts[-1]
            parts.append(unit)
            thin_parts.append(1.0)
            if mid + 1 < hi:
                arm = low_right(done[mid + 1, hi][0], low, mid + 1, True)
                s = s - low(mid + 1, arm[:size], True)
                parts.append(arm)
                thin_arm = [floor_low[mid + 1] * x for x in thin[mid + 1, hi][0]]
                t = t - floor_low[mid + 1] * thin_arm[0]
                thin_parts += thin_arm
            schur.append(s)
            floors.append(t)
            arms.append(jnp.concatenate(parts, axis=0) if len(parts) > 1 else parts[0])
            thin_arms.append(thin_parts)
        inverses = invert_all(schur, [0.97 * t for t in floors], steps)
        for (lo, mid, hi), v, z, thin_v, t in zip(nodes, arms, inverses, thin_arms, floors):
            thin[lo, hi] = [[a * b / t for b in thin_v] for a in thin_v]
            for a, b in ((lo, mid), (mid + 1, hi)):
                for i in range(a, b):
                    for j in range(a, b):
                        thin[lo, hi][i - lo][j - lo] += thin[a, b][i - a][j - a]
            if hi - lo == 1:
                done[lo, hi] = [z]
                continue
            w = dot(v, z)
            panels = []
            for k in range(lo, hi):
                vk = v[(k - lo) * size : (k - lo + 1) * size]
                new = w if k == mid else dot_t(w, vk)
                pieces = []
                for a, b in ((lo, mid), (mid, mid + 1), (mid + 1, hi)):
                    if a >= b:
                        continue
                    piece = new[(a - lo) * size : (b - lo) * size]
                    if a <= k < b and k != mid:
                        piece = piece + done[a, b][k - a]
                    pieces.append(piece)
                panels.append(jnp.concatenate(pieces, axis=0) if len(pieces) > 1 else pieces[0])
            done[lo, hi] = panels
    return done[0, count], thin[0, count]


def low_right(panel, low, k, plain):
    return low(k, panel, not plain, True)


def split(x):
    high = x.astype(jnp.bfloat16)
    return high, (x - high.astype(jnp.float32)).astype(jnp.bfloat16)


def dot3(a_high, a_low, b):
    b_high, b_low = split(b)
    mul = functools.partial(jnp.dot, preferred_element_type=jnp.float32)
    return mul(a_high, b_high) + (mul(a_low, b_high) + mul(a_high, b_low))


def factor_kernel(links_ref, top_ref, loss_ref, high_ref, low_ref, ends_ref, send_ref):
    levels, size = loss_ref.shape[0], loss_ref.shape[1]
    inner = levels - 1
    on_diag = eye_of(size)
    top_link, inner_link = top_ref[0:1, 0:1], jnp.full((1, 1), links_ref[inner - 1])
    links = [jnp.full((1, 1), links_ref[k]) for k in range(levels)]

    def diag_of(k):
        above = top_link if k == 0 else links[k - 1]
        return loss_ref[k] + jnp.where(on_diag, 1.0 + above + links[k], 0.0)

    def low(k, x, transposed=False, right=False):
        return links_ref[k - 1] * x

    floor_diag = [
        LEAST + links[k] + (top_link if k == 0 else links[k - 1]) for k in range(levels)
    ]
    panels, thin = dense_inverse(
        [diag_of(k) for k in range(inner)], low, floor_diag[:inner], [top_link] + links[: inner - 1]
    )
    for k, panel in enumerate(panels):
        high, rest = split(panel)
        high_ref[:, k * size : (k + 1) * size] = high
        low_ref[:, k * size : (k + 1) * size] = rest
    ends_ref[0] = top_link * panels[0]
    ends_ref[1] = inner_link * panels[-1]
    blocks = [
        (
            diag_of(inner) - inner_link * inner_link * panels[-1][-size:],
            floor_diag[inner] - inner_link * inner_link * thin[-1][-1],
        ),
        (top_link * top_link * panels[0][:size], top_link * top_link * thin[0][0]),
        (inner_link * top_link * panels[0][-size:], inner_link * top_link * thin[0][-1]),
    ]
    for k, (block, floor) in enumerate(blocks):
        send_ref[k, :size] = block
        send_ref[k, size:] = jnp.broadcast_to(floor, (8, size))


def interface(all_ref, ends_ref, high_ref, low_ref, rows_ref):
    count, size = all_ref.shape[0], all_ref.shape[3]

    def diag_of(rows, cols):
        own = [all_ref[k, 0, rows, cols] for k in range(count)]
        return [
            own[k] - all_ref[k + 1, 1, rows, cols] if k + 1 < count else own[k]
            for k in range(count)
        ]

    def low(k, x, transposed=False, right=False):
        block = all_ref[k, 2, :size]
        if right:
            return dot_t(x, block) if transposed else dot(x, block)
        return dot(block, x, ((0,), (0,))) if transposed else dot(block, x)

    thin = slice(size, size + 1), slice(0, 1)
    panels, _ = dense_inverse(
        diag_of(slice(0, size), slice(0, size)),
        low,
        diag_of(*thin),
        [all_ref[k, 2, thin[0], thin[1]] for k in range(count)],
        enough_steps(spread(size)),
    )
    for k, panel in enumerate(panels):
        rows_ref[k] = panel
    me = lax.axis_index("lev")
    own = rows_ref[me]
    above = rows_ref[jnp.maximum(me - 1, 0)]
    inner = dot_t(ends_ref[0], above) + dot_t(ends_ref[1], own)
    length = inner.shape[0]
    high_ref[:length], low_ref[:length] = split(inner)
    high_ref[length:], low_ref[length:] = split(own.T)


def send(src, dst, sems, slot, device):
    return pltpu.make_async_remote_copy(
        src_ref=src,
        dst_ref=dst,
        send_sem=sems.at[0, slot],
        recv_sem=sems.at[1, slot],
        device_id=device,
        device_id_type=pl.DeviceIdType.MESH,
    )


def greet(lev_all, lon_all):
    barrier = pltpu.get_barrier_semaphore()
    partners = []
    for axis, everyone in (("lev", lev_all), ("lon", lon_all)):
        count, me = lax.axis_size(axis), lax.axis_index(axis)
        if everyone is None:
            continue
        steps = range(1, count) if everyone else sorted({1, count - 1})
        partners += [{axis: lax.rem(me + d, count)} for d in steps if d % count]
    for device in partners:
        pl.semaphore_signal(
            barrier, inc=1, device_id=device, device_id_type=pl.DeviceIdType.MESH
        )
    pl.semaphore_wait(barrier, len(partners))


def pack_edges(cur_ref, edges_ref):
    levels, size, columns = cur_ref.shape
    lane = lax.broadcasted_iota(jnp.int32, (size, 128), 1)
    last = jnp.zeros((size, 128), jnp.float32)
    first = last
    for k in range(levels):
        tail = pltpu.roll(cur_ref[k, :, columns - 128 :], k + 1, 1)
        head = cur_ref[k, :, :128]
        head = pltpu.roll(head, k, 1) if k else head
        last = jnp.where(lane == k, tail, last)
        first = jnp.where(lane == k, head, first)
    edges_ref[0] = last
    edges_ref[1] = first


def halo_copies(edges_ref, halo_ref, sems):
    around, me = lax.axis_size("lon"), lax.axis_index("lon")
    return [
        send(edges_ref.at[0], halo_ref.at[0], sems, 0, {"lon": lax.rem(me + 1, around)}),
        send(edges_ref.at[1], halo_ref.at[1], sems, 1, {"lon": lax.rem(me + around - 1, around)}),
    ]


def local_forcing(mix_ref, cur_ref, prev_ref, pair_ref, force_ref):
    levels, size, columns = cur_ref.shape
    lane = lax.broadcasted_iota(jnp.int32, (size, columns), 1)
    for k in range(levels):
        c = cur_ref[k]
        back = jnp.where(lane == 0, 0.0, pltpu.roll(c, 1, 1))
        ahead = jnp.where(lane == columns - 1, 0.0, pltpu.roll(c, columns - 1, 1))
        p_high, p_low = split(pair_ref[k])
        chem = dot3(p_high, p_low, c * c)
        force_ref[k * size : (k + 1) * size] = (
            prev_ref[k] - chem + mix_ref[k] * (back + ahead - 2.0 * c)
        )


def add_halo(mix_ref, halo_ref, force_ref):
    levels = mix_ref.shape[0]
    size, columns = halo_ref.shape[1], force_ref.shape[1]
    lane = lax.broadcasted_iota(jnp.int32, (size, 128), 1)
    before, after = halo_ref[0], halo_ref[1]
    for k in range(levels):
        rows = slice(k * size, (k + 1) * size)
        at_head = pltpu.roll(before, 128 - k, 1) if k else before
        at_tail = pltpu.roll(after, 127 - k, 1)
        force_ref[rows, :128] += jnp.where(lane == 0, mix_ref[k] * at_head, 0.0)
        force_ref[rows, columns - 128 :] += jnp.where(lane == 127, mix_ref[k] * at_tail, 0.0)


def couple(
    links_ref, top_link, g_high, g_low, force_ref, part_ref, f_high, f_low, top_out, top_in, sides_ref,
    sems, direct,
):
    count, me = lax.axis_size("lev"), lax.axis_index("lev")
    inner, size = part_ref.shape[0], top_out.shape[0]
    f_high[...], f_low[...] = split(force_ref[:inner])
    mul = functools.partial(jnp.dot, preferred_element_type=jnp.float32)

    def rows_of(start, stop):
        a, b = g_high[start:stop], g_low[start:stop]
        part = mul(a, f_high[...]) + (mul(b, f_high[...]) + mul(a, f_low[...]))
        part_ref[start:stop] = part
        return part

    top_out[...] = top_link * rows_of(0, size)
    sides_ref[me] = force_ref[inner:] + links_ref[inner // size - 1] * rows_of(inner - size, inner)
    up = send(top_out, top_in, sems, 0, {"lev": lax.rem(me + count - 1, count)})
    half = size * ((inner // size) // 2)

    @pl.when(me > 0)
    def _():
        up.start()

    rows_of(size, half)

    @pl.when(me < count - 1)
    def _():
        up.wait_recv()
        sides_ref[me] += top_in[...]

    partner = me + 1 - 2 * lax.rem(me, 2)
    copies = [
        send(sides_ref.at[me], sides_ref.at[me], sems, d, {"lev": lax.rem(me + d, count)})
        for d in range(1 if direct else 2, count, 1 if direct else 2)
    ]
    onward = [] if direct else [send(sides_ref.at[me], sides_ref.at[me], sems, 1, {"lev": partner})]
    for d in range(count if direct else 2, count, 2):
        origin = lax.rem(me - d + count, count)
        onward.append(
            send(sides_ref.at[origin], sides_ref.at[origin], sems, d + 1, {"lev": partner})
        )
    for copy in copies + onward[:1]:
        copy.start()
    rows_of(half, inner - size)

    @pl.when(me > 0)
    def _():
        up.wait_send()

    return copies, onward


def relay(copies, onward):
    for copy, later in zip(copies, onward[1:]):
        copy.wait_recv()
        later.start()
    for copy in copies:
        copy.wait_send()
    for copy in onward:
        copy.wait()


def finish(part_ref, sides_ref, high_ref, low_ref, out_ref):
    levels, size, columns = out_ref.shape
    count = sides_ref.shape[0]
    b_high, b_low = split(sides_ref[...].reshape(count * size, columns))
    mul = functools.partial(jnp.dot, preferred_element_type=jnp.float32)
    for k in range(levels):
        rows = slice(k * size, (k + 1) * size)
        a, b = high_ref[rows], low_ref[rows]
        row = mul(a, b_high) + (mul(b, b_high) + mul(a, b_low))
        out_ref[k] = row + part_ref[rows] if k < levels - 1 else row


def open_kernel(
    links_ref, mix_ref, prev_ref, pair_ref, force_ref, top_ref, edges, halo, link_out, sems
):
    levels = prev_ref.shape[0]
    count, me = lax.axis_size("lev"), lax.axis_index("lev")
    pack_edges(prev_ref, edges)
    link_out[...] = jnp.full(link_out.shape, links_ref[levels - 1], jnp.float32)
    greet(False, False)
    copies = halo_copies(edges, halo, sems)
    down = send(link_out, top_ref, sems, 2, {"lev": lax.rem(me + 1, count)})
    for copy in copies:
        copy.start()

    @pl.when(me < count - 1)
    def _():
        down.start()

    @pl.when(me == 0)
    def _():
        top_ref[...] = jnp.zeros(top_ref.shape, jnp.float32)

    local_forcing(mix_ref, prev_ref, prev_ref, pair_ref, force_ref)
    for copy in copies:
        copy.wait()
    add_halo(mix_ref, halo, force_ref)

    @pl.when(me < count - 1)
    def _():
        down.wait_send()

    @pl.when(me > 0)
    def _():
        down.wait_recv()


def newton_kernel(
    links_ref, mix_ref, top_ref, sent_ref, ends_ref, first_force, g_high, g_low, prev_ref, pair_ref,
    out_ref, var_ref, all_ref, rows_ref, h_high, h_low, cur_ref, edges, halo, force_ref, part_ref,
    first_sides, sides_ref, f_high, f_low, first_out, first_in, top_out, top_in, sums_ref,
    block_sems, first_sems, halo_sems, sems, sum_sems,
):
    levels, size, columns = prev_ref.shape
    count, me = lax.axis_size("lev"), lax.axis_index("lev")
    around, place = lax.axis_size("lon"), lax.axis_index("lon")
    greet(True, True)
    blocks = [
        send(sent_ref, all_ref.at[me], block_sems, d, {"lev": lax.rem(me + d, count)})
        for d in range(1, count)
    ]
    for copy in blocks:
        copy.start()
    all_ref[me] = sent_ref[...]
    copies = couple(
        links_ref, top_ref[0:1, 0:1], g_high, g_low, first_force, part_ref, f_high, f_low,
        first_out, first_in, first_sides, first_sems, True,
    )
    for copy in blocks:
        copy.wait()
    interface(all_ref, ends_ref, h_high, h_low, rows_ref)
    for copy in copies[0]:
        copy.wait()
    finish(part_ref, first_sides, h_high, h_low, cur_ref)
    pack_edges(cur_ref, edges)
    copies = halo_copies(edges, halo, halo_sems)
    for copy in copies:
        copy.start()
    local_forcing(mix_ref, cur_ref, prev_ref, pair_ref, force_ref)
    for copy in copies:
        copy.wait()
    add_halo(mix_ref, halo, force_ref)
    copies = couple(
        links_ref, top_ref[0:1, 0:1], g_high, g_low, force_ref, part_ref, f_high, f_low,
        top_out, top_in, sides_ref, sems, False,
    )
    relay(*copies)
    finish(part_ref, sides_ref, h_high, h_low, out_ref)
    lane = lax.broadcasted_iota(jnp.int32, (size, 128), 1)
    total = jnp.zeros((size, 128), jnp.float32)
    for k in range(levels):
        row = out_ref[k]
        total = jnp.where(lane == k, jnp.sum(row * row, axis=1, keepdims=True), total)
    sums_ref[0] = total.T[: sums_ref.shape[1]]
    copies = [
        send(sums_ref.at[0], sums_ref.at[d], sum_sems, d, {"lon": lax.rem(place + d, around)})
        for d in range(1, around)
    ]
    for copy in copies:
        copy.start()
    for copy in copies:
        copy.wait()
    total = sums_ref[place]
    for j in range(1, around):
        total = total + sums_ref[lax.rem(place - j + around, around)]
    var_ref[...] = (total / (columns * around))[:levels]


def call(kernel, outs, places, scratch=(), group=None):
    extra = {} if group is None else {"collective_id": group, "has_side_effects": True}
    return pl.pallas_call(
        kernel,
        out_shape=[jax.ShapeDtypeStruct(shape, dtype) for shape, dtype in outs],
        in_specs=places,
        out_specs=[VMEM] * len(outs),
        scratch_shapes=list(scratch),
        compiler_params=pltpu.CompilerParams(vmem_limit_bytes=60 * 2**20, **extra),
    )


def local(previous, loss_matrix, pair_matrix, diffusivity, mixing):
    levels, size, columns = previous.shape
    count = lax.axis_size("lev")
    around = lax.axis_size("lon")
    inner = (levels - 1) * size
    f32, bf16 = jnp.float32, jnp.bfloat16
    buf, sem = pltpu.VMEM, lambda n: pltpu.SemaphoreType.DMA((2, n))
    force, top = call(
        open_kernel,
        [((levels * size, columns), f32), ((8, 128), f32)],
        [SMEM, SMEM, VMEM, VMEM],
        [buf((2, size, 128), f32), buf((2, size, 128), f32), buf((8, 128), f32), sem(3)],
        0,
    )(diffusivity, mixing, previous, pair_matrix)
    g_high, g_low, ends, sent = call(
        factor_kernel,
        [((inner, inner), bf16), ((inner, inner), bf16), ((2, inner, size), f32), ((3, size + 8, size), f32)],
        [SMEM, VMEM, VMEM],
    )(diffusivity, top, loss_matrix)
    return call(
        newton_kernel,
        [((levels, size, columns), f32), ((levels, size), f32)],
        [SMEM, SMEM] + [VMEM] * 8,
        [
            buf((count, 3, size + 8, size), f32),
            buf((count, count * size, size), f32),
            buf((levels * size, count * size), bf16),
            buf((levels * size, count * size), bf16),
            buf((levels, size, columns), f32),
            buf((2, size, 128), f32),
            buf((2, size, 128), f32),
            buf((levels * size, columns), f32),
            buf((inner, columns), f32),
            buf((count, size, columns), f32),
            buf((count, size, columns), f32),
            buf((inner, columns), bf16),
            buf((inner, columns), bf16),
            buf((size, columns), f32),
            buf((size, columns), f32),
            buf((size, columns), f32),
            buf((size, columns), f32),
            buf((around, -(-levels // 8) * 8, size), f32),
            sem(count),
            sem(count),
            sem(2),
            sem(count),
            sem(around),
        ],
        1,
    )(diffusivity, mixing, top, sent, ends, force, g_high, g_low, previous, pair_matrix)


def cat3(a_high, a_low, b_high, b_low):
    return jnp.dot(
        jnp.concatenate([a_high, a_low, a_high], axis=1),
        jnp.concatenate([b_high, b_high, b_low], axis=0),
        preferred_element_type=jnp.float32,
    )


def wide(a):
    high, low = split(a)
    return jnp.concatenate([high, low, high, jnp.zeros_like(high)], axis=1)


def tall(b):
    high, low = split(b)
    return jnp.concatenate([high, high, low, jnp.zeros_like(high)], axis=0)


def wide_dot(a, b):
    return jnp.dot(a, b, preferred_element_type=jnp.float32)


def near_dot(a, b):
    return lax.dot_general(
        a, b, (((1,), (0,)), ((), ())), precision=lax.Precision.HIGH, preferred_element_type=jnp.float32
    )


def pull(links, loss):
    stiff = links[0]
    for a in links[1:]:
        own = 1.0 + loss + stiff
        stiff = a * own / (a + own)
    return stiff


def worst_ratio(above, below):
    sides = []
    for count in (above, below):
        draws = itertools.product((200.0, 2000.0), repeat=min(count, 8) + 1)
        sides.append([(pull(d, 640.0), pull(d, 0.05)) for d in draws])
    return 1.15 * max((641.0 + a + c) / (1.05 + b + d) for a, b in sides[0] for c, d in sides[1])


def edge_ratios(inner):
    inner = min(inner, 8)
    held = [(pull(d, 640.0), pull(d, 0.05)) for d in itertools.product((200.0, 2000.0), repeat=inner + 1)]
    draws = [(0.0, *d) for d in itertools.product((200.0, 2000.0), repeat=inner + 1)]
    free = [(pull(d, 640.0), pull(d, 0.05)) for d in draws]
    outer = max((641.0 + a) / (1.05 + b) for a, b in held)
    outer = max(outer, max((320.5 + a) / (0.525 + b) for a, b in held))
    second = max((641.0 + a + c) / (1.05 + b + d) for a, b in held for c, d in free)
    return 1.15 * outer, 1.15 * second


def gains_for(ratio):
    rho, gains = (ratio - 1.0) / (ratio + 1.0), []
    while rho > 1.2e-3:
        gains.append(2.0 / (2.0 - rho * rho))
        rho = rho * rho / (2.0 - rho * rho)
    return gains


def invert_fixed(blocks, floors, ratio):
    size = blocks[0].shape[0]
    unit = jnp.where(eye_of(size), 1.0, 0.0).astype(jnp.float32)
    gains = gains_for(ratio)
    xs, rests = [], []
    for a, low in zip(blocks, floors):
        scale = (2.0 / (1.0 + ratio)) / low
        rest = unit - scale * a
        xs.append((gains[0] * scale) * (unit + rest))
        rests.append(rest)
    rests = [gains[0] * dot(r, r) - (gains[0] - 1.0) * unit for r in rests]
    for step, g in enumerate(gains[1:]):
        left = len(gains) - step - 2
        mul = dot if left > 2 else near_dot
        if left == 0:
            xs = [g * (x + mul(x, r)) for x, r in zip(xs, rests)]
            break
        both = [mul(jnp.concatenate([x, r], axis=0), r) for x, r in zip(xs, rests)]
        xs = [g * (x + b[:size]) for x, b in zip(xs, both)]
        rests = [g * b[size:] - (g - 1.0) * unit for b in both]
    rests = [unit - dot(a, x) for a, x in zip(blocks, xs)]
    return [x + near_dot(x, r) for x, r in zip(xs, rests)]


def chain_factor(diag, links, floors, panel_ref, hook):
    count, size = len(diag), diag[0].shape[0]
    unit = jnp.where(eye_of(size), 1.0, 0.0).astype(jnp.float32)
    by_depth, thin, corners = {}, {}, {}
    plan(0, count, by_depth)

    def rows(lo, hi):
        return slice(lo * size, hi * size)

    for depth in sorted(by_depth):
        nodes = by_depth[depth]
        ratio = max(worst_ratio(mid - lo, hi - 1 - mid) for lo, mid, hi in nodes)
        schur, arms, lows, thin_arms = [], [], [], []
        for lo, mid, hi in nodes:
            s, parts = diag[mid], []
            t, thin_parts = floors[mid], []
            if lo < mid:
                arm = links[mid] * panel_ref[mid - 1, rows(lo, mid)]
                s = s - (links[mid] * links[mid]) * corners[lo, mid][1]
                parts.append(arm)
                thin_parts += [links[mid] * x for x in thin[lo, mid][-1]]
                t = t - links[mid] * thin_parts[-1]
            parts.append(unit)
            thin_parts.append(1.0)
            if mid + 1 < hi:
                arm = links[mid + 1] * panel_ref[mid + 1, rows(mid + 1, hi)]
                s = s - (links[mid + 1] * links[mid + 1]) * corners[mid + 1, hi][0]
                parts.append(arm)
                thin_arm = [links[mid + 1] * x for x in thin[mid + 1, hi][0]]
                t = t - links[mid + 1] * thin_arm[0]
                thin_parts += thin_arm
            schur.append(s)
            lows.append(t)
            arms.append(jnp.concatenate(parts, axis=0) if len(parts) > 1 else parts[0])
            thin_arms.append(thin_parts)
        inverses = invert_fixed(schur, [0.97 * t for t in lows], ratio)
        for (lo, mid, hi), v, z, thin_v, t in zip(nodes, arms, inverses, thin_arms, lows):
            thin[lo, hi] = [[a * b / t for b in thin_v] for a in thin_v]
            for a, b in ((lo, mid), (mid + 1, hi)):
                for i in range(a, b):
                    for j in range(a, b):
                        thin[lo, hi][i - lo][j - lo] += thin[a, b][i - a][j - a]
            if hi - lo == 1:
                panel_ref[mid, rows(mid, hi)] = z
                corners[lo, hi] = z, z
                continue
            ends = v[:size], v[-size:]
            arms_out = [dot(x, z) for x in ends]
            corners[lo, hi] = tuple(
                z if at == mid else corners[part][side] + dot_t(y, x)
                for side, (at, part, x, y) in enumerate(
                    ((lo, (lo, mid), ends[0], arms_out[0]), (hi - 1, (mid + 1, hi), ends[1], arms_out[1]))
                )
            )
            if hi - lo == count:
                far = dot_t(arms_out[1], ends[0])
            w = dot(v, z)
            if hi - lo == count:
                continue
            new = dot_t(w, v)
            for k in range(lo, hi):
                own = new[:, (k - lo) * size : (k - lo + 1) * size]
                panel_ref[k, rows(mid, mid + 1)] = own[rows(mid - lo, mid - lo + 1)]
                for a, b in ((lo, mid), (mid + 1, hi)):
                    if a >= b:
                        continue
                    piece = own[rows(a - lo, b - lo)]
                    if a <= k < b:
                        piece = piece + panel_ref[k, rows(a, b)]
                    panel_ref[k, rows(a, b)] = piece
        if depth < max(by_depth):
            hook(depth)
    return v, w, by_depth[max(by_depth)][0][1], thin[0, count], (*corners[0, count], far)


def fold(x):
    half = x.shape[0] // 2
    return jnp.concatenate([x[:half], x[half:]], axis=1)


def unfold(x):
    half = x.shape[1] // 2
    return jnp.concatenate([x[:, :half], x[:, half:]], axis=0)


def pack_pairs(field_ref, columns, edges_ref):
    levels, size = field_ref.shape[:2]
    lane = lax.broadcasted_iota(jnp.int32, (size, 128), 1)
    last = jnp.zeros((size, 128), jnp.float32)
    first = last
    for k in range(levels):
        tail = pltpu.roll(field_ref[k, :, columns - 128 : columns], (2 * k + 2) % 128, 1)
        head = field_ref[k, :, :128]
        head = pltpu.roll(head, 2 * k, 1) if k else head
        mine = (lane == 2 * k) | (lane == 2 * k + 1)
        last = jnp.where(mine, tail, last)
        first = jnp.where(mine, head, first)
    edges_ref[0] = last
    edges_ref[1] = first


def unpack_pairs(halo_ref, columns, field_ref):
    levels, size = field_ref.shape[:2]
    lane = lax.broadcasted_iota(jnp.int32, (size, 128), 1)
    before, after = halo_ref[0], halo_ref[1]
    for k in range(levels):
        at_head = pltpu.roll(after, (128 - 2 * k) % 128, 1) if k else after
        at_tail = pltpu.roll(before, (126 - 2 * k) % 128, 1)
        field_ref[k, :, columns:] = jnp.where(lane < 2, at_head, jnp.where(lane >= 126, at_tail, 0.0))


def forcing(mix_ref, cur_ref, prev_ref, pairs_ref, width, sep_ref, f_high, f_low):
    levels, size, full = cur_ref.shape
    for k in range(levels):
        c = cur_ref[k]
        ring = pltpu.roll(c, 1, 1) + pltpu.roll(c, full - 1, 1)
        own = c[:, :width]
        chem = wide_dot(pairs_ref[k], tall(own * own))
        force = prev_ref[k, :, :width] - chem + mix_ref[k] * (ring[:, :width] - 2.0 * own)
        if k == 0:
            sep_ref[:, :width] = force
        else:
            rows = slice((k - 1) * size, k * size)
            f_high[rows, :width], f_low[rows, :width] = split(force)


def start_all(copies):
    @pl.when(lax.axis_index("lev") < lax.axis_size("lev"))
    def _():
        for copy in copies:
            copy.start()


def step_kernel(
    links_hbm, mix_hbm, loss_hbm, prev_hbm, pair_hbm, out_ref, var_ref, links_ref, mix_ref,
    loss_ref, prev_ref, pair_ref, pairs_ref, edges, halo, z_high, z_low, send_ref, all_ref,
    ends_high, ends_low, table_ref, sep_ref, f_high, f_low, part_ref, own_ref, near_ref, mine_ref, far_ref,
    side_high, side_low, hq_high, hq_low, u_ref, top_ref, cur_ref, sums_ref, panel_ref, w_ref, v_ref,
    load_sems, halo_sems, block_sems, near_sems, far_sems, sum_sems,
):
    levels, size, columns = prev_hbm.shape
    inner = levels - 1
    full = cur_ref.shape[2]
    count, me = lax.axis_size("lev"), lax.axis_index("lev")
    around, place = lax.axis_size("lon"), lax.axis_index("lon")
    core, chip = lax.rem(me, 2), me // 2
    partner = me + 1 - 2 * core
    across = lax.rem(me + 2, count)

    loads = [
        pltpu.make_async_copy(loss_hbm, loss_ref, load_sems.at[0]),
        pltpu.make_async_copy(prev_hbm, prev_ref.at[:, :, pl.ds(0, columns)], load_sems.at[1]),
        pltpu.make_async_copy(pair_hbm, pair_ref, load_sems.at[2]),
        pltpu.make_async_copy(links_hbm, links_ref, load_sems.at[3]),
        pltpu.make_async_copy(mix_hbm, mix_ref, load_sems.at[4]),
    ]
    for k in (3, 0, 1, 2, 4):
        loads[k].start()
    barrier = pltpu.get_barrier_semaphore()
    partners = [{"lev": lax.rem(me + d, count)} for d in range(1, count)]
    partners += [{"lon": lax.rem(place + d, around)} for d in range(1, around)]
    for device in partners:
        pl.semaphore_signal(barrier, inc=1, device_id=device, device_id_type=pl.DeviceIdType.MESH)

    loads[3].wait()
    links = [jnp.full((1, 1), links_ref[k]) for k in range(levels)]
    on_diag = eye_of(size)
    halo_moves = halo_copies(edges, halo, halo_sems)

    def hook(depth):
        if depth != 2:
            return
        loads[1].wait()
        pack_pairs(prev_ref, columns, edges)
        pl.semaphore_wait(barrier, len(partners))
        start_all(halo_moves)

    loads[0].wait()
    diag = [
        loss_ref[k] + jnp.where(on_diag, 1.0 + links[k] + (links[k - 1] if k else 0.0), 0.0)
        for k in range(levels)
    ]
    floors = [LEAST + links[k] + (links[k - 1] if k else 0.0) for k in range(levels)]
    v, w, mid, thin, (z_first, z_last, z_far) = chain_factor(diag[1:], links[:inner], floors[1:], panel_ref, hook)
    a, b = links[0], links[inner]
    sub = lax.broadcasted_iota(jnp.int32, (8, 128), 0)
    send_ref[: size // 2] = fold(diag[0] - a * a * z_first)
    send_ref[size // 2 : size] = fold(jnp.where(on_diag, b, 0.0) - b * b * z_last)
    send_ref[size : 3 * size // 2] = fold(a * b * z_far)
    send_ref[3 * size // 2 :] = jnp.where(
        sub == 0, floors[0] - a * a * thin[0][0], jnp.where(sub == 1, b - b * b * thin[-1][-1], a * b * thin[0][-1])
    )
    blocks = [
        send(send_ref, all_ref.at[me], block_sems, d, {"lev": lax.rem(me + d, count)})
        for d in range(1, count)
    ]
    start_all(blocks)
    all_ref[me] = send_ref[...]

    old = [
        panel_ref[0, : mid * size],
        jnp.zeros((size, size), jnp.float32),
        panel_ref[inner - 1, (mid + 1) * size :],
    ]
    tips = dot_t(w, jnp.concatenate([v[:size], v[-size:]], axis=0))
    first = tips[:, :size] + jnp.concatenate([old[0], old[1], jnp.zeros_like(old[2])], axis=0)
    last = tips[:, size:] + jnp.concatenate([jnp.zeros_like(old[0]), old[1], old[2]], axis=0)
    ends_high[...], ends_low[...] = split(jnp.concatenate([a * first, b * last], axis=1))
    w_ref[...] = wide(w)
    v_high, v_low = split(v)
    v_ref[...] = jnp.concatenate([v_high, v_high, v_low, jnp.zeros_like(v_high)], axis=1)

    def form(lo, hi):
        spot = slice(lo * size, hi * size)
        new = lax.dot_general(
            w_ref[spot], v_ref[...], (((1,), (1,)), ((), ())), preferred_element_type=jnp.float32
        )
        start, stop = (0, mid) if lo < mid else (mid + 1, inner)
        if lo != mid:
            zeros = jnp.zeros((new.shape[0], size), jnp.float32)
            new = new + jnp.concatenate(
                [panel_ref[j, spot] if start <= j < stop else zeros for j in range(inner)], axis=1
            )
        z_high[spot], z_low[spot] = split(new)

    form(0, 1)
    form(inner - 1, inner)
    loads[2].wait()
    loads[4].wait()
    for k in range(levels):
        pairs_ref[k] = wide(pair_ref[k])
    for move in halo_moves:
        move.wait()
    unpack_pairs(halo, columns, prev_ref)

    def z_rows(start, stop, width):
        return cat3(z_high[start:stop], z_low[start:stop], f_high[:, :width], f_low[:, :width])

    def ends(turn, width):
        rows = cat3(
            jnp.concatenate([z_high[:size], z_high[-size:]], axis=0),
            jnp.concatenate([z_low[:size], z_low[-size:]], axis=0),
            f_high[:, :width],
            f_low[:, :width],
        )
        part_ref[:size, :width] = rows[:size]
        part_ref[-size:, :width] = rows[size:]
        own_ref[turn, 0, :, :width] = sep_ref[:, :width] + a * rows[:size]
        own_ref[turn, 1, :, :width] = b * rows[size:]
        copy = send(
            own_ref.at[turn, :, :, pl.ds(0, width)], near_ref.at[turn, :, :, pl.ds(0, width)], near_sems, turn,
            {"lev": partner},
        )
        start_all([copy])
        return copy

    def middle(width):
        part_ref[size:-size, :width] = z_rows(size, (inner - 1) * size, width)

    def merge(turn, width):
        upper = core == 0
        s_own, t_own = own_ref[turn, 0, :, :width], own_ref[turn, 1, :, :width]
        s_in, t_in = near_ref[turn, 0, :, :width], near_ref[turn, 1, :, :width]
        low_side = jnp.where(upper, s_own, s_in)
        high_side = jnp.where(upper, s_in + t_own, s_own + t_in)
        side_high[:size, :width], side_low[:size, :width] = split(low_side)
        side_high[size:, :width], side_low[size:, :width] = split(high_side)
        return jnp.where(chip == 0, jnp.where(upper, t_in, t_own), 0.0)

    def condense(turn, width, tail, k_high, k_low):
        mine_ref[turn, :, :width] = tail + cat3(k_high, k_low, side_high[:, :width], side_low[:, :width])
        half, quarter = columns // 2, columns // 4
        first = pl.ds(pl.multiple_of(core * half, 128), quarter)
        second = pl.ds(pl.multiple_of(core * half + quarter, 128), quarter)
        routes = [(mine_ref, first, across), (mine_ref, second, across), (mine_ref, second, lax.rem(partner + 2, count))]
        routes += [(mine_ref, pl.ds(columns, width - columns), across)] if width > columns else []
        routes += [(far_ref, first, partner)]
        copies = [
            send(src.at[turn, :, spot], far_ref.at[turn, :, spot], far_sems, 5 * turn + k, {"lev": device})
            for k, (src, spot, device) in enumerate(routes)
        ]
        start_all(copies[:-1])
        return copies

    def relay_far(copies):
        copies[0].wait_recv()
        start_all(copies[-1:])

    def wait_far(copies):
        copies[0].wait_send()
        for copy in copies[1:]:
            copy.wait()

    def gather_sides(width):
        rest = cat3(hq_high[...], hq_low[...], side_high[:, :width], side_low[:, :width])
        for k in range(levels):
            rows = rest[k * size : (k + 1) * size]
            cur_ref[k, :, :width] = rows if k == 0 else rows + part_ref[(k - 1) * size : k * size, :width]

    def finish(turn, width, to_ref):
        total = mine_ref[turn, :, :width] + far_ref[turn, :, :width]
        top = tall(wide_dot(top_ref[...], tall(total)))
        for k in range(levels):
            to_ref[k, :, :width] = cur_ref[k, :, :width] + wide_dot(u_ref[k * size : (k + 1) * size], top)

    forcing(mix_ref, prev_ref, prev_ref, pairs_ref, full, sep_ref, f_high, f_low)
    near = ends(0, full)
    for lo, hi in ((1, mid), (mid, mid + 1), (mid + 1, inner - 1)):
        form(lo, hi)
    middle(full)
    for copy in blocks:
        copy.wait()

    def block(k, which):
        return unfold(all_ref[k, which * size // 2 : (which + 1) * size // 2])

    def floor(k, which):
        row = 3 * size // 2 + which
        return all_ref[k, row : row + 1, 0:1]

    ratio = spread(size)
    s = [block(k, 0) + (block(k - 1, 1) if k else 0.0) for k in range(count)]
    t = [floor(k, 0) + (floor(k - 1, 1) if k else 0.0) for k in range(count)]
    c = [None] + [block(k, 2) for k in range(count - 1)]
    e = [None] + [floor(k, 2) for k in range(count - 1)]
    outer, second = edge_ratios(inner)
    z0, z3 = invert_fixed([s[0], s[3]], [0.97 * t[0], 0.97 * t[3]], outer)
    a1, a3 = dot(c[1], z0), dot(z3, c[3])
    s1 = s[1] - dot_t(a1, c[1])
    t1 = t[1] - e[1] * e[1] / t[0]
    (z1,) = invert_fixed([s1], [0.97 * t1], second)
    a2 = dot(c[2], z1)
    s2 = s[2] - dot_t(a2, c[2]) - dot(c[3], a3, ((0,), (0,)))
    t2 = t[2] - e[2] * e[2] / t1 - e[3] * e[3] / t[3]
    b1 = dot(z1, a1)
    p0 = dot(a2, a1)
    zero = jnp.zeros((size, size), jnp.float32)
    unit = jnp.where(on_diag, 1.0, 0.0).astype(jnp.float32)
    sides = [
        (z0 + dot(a1, b1, ((0,), (0,))), b1.T, p0.T),
        (b1, z1, a2.T),
        (zero, zero, unit),
        (zero, z3, a3),
        (zero, zero, zero),
    ]
    for k, (left, right, top) in enumerate(sides):
        table_ref[k, :size] = jnp.concatenate([left, right], axis=1)
        table_ref[k, size:, :size] = top
    for k, (left, right) in enumerate(((p0, a2), (unit, a3.T))):
        table_ref[len(sides) + k, :size] = jnp.concatenate([left, right], axis=1)
    near.wait()
    tail = merge(0, full)
    k_high, k_low = split(table_ref[len(sides) + chip, :size])
    far = condense(0, full, tail, k_high, k_low)
    (z2,) = invert_fixed([s2], [0.97 * t2], ratio)
    top_ref[...] = wide(z2)
    own_q, next_q = table_ref[me, :size], table_ref[me + 1, :size]
    own_p, next_p = table_ref[me, size:, :size], table_ref[me + 1, size:, :size]
    q_high, q_low = split(jnp.concatenate([own_q, next_q], axis=0))
    p_high, p_low = split(jnp.concatenate([own_p, next_p], axis=0))
    hq_high[size:], hq_low[size:] = split(cat3(ends_high[...], ends_low[...], q_high, q_low))
    hq_high[:size], hq_low[:size] = split(own_q)
    u_ref[size:] = wide(cat3(ends_high[...], ends_low[...], p_high, p_low))
    u_ref[:size] = wide(own_p)
    relay_far(far)
    gather_sides(full)
    wait_far(far)
    finish(0, full, cur_ref)

    forcing(mix_ref, cur_ref, prev_ref, pairs_ref, columns, sep_ref, f_high, f_low)
    near = ends(1, columns)
    near.wait()
    tail = merge(1, columns)
    far = condense(1, columns, tail, k_high, k_low)
    middle(columns)
    gather_sides(columns)
    relay_far(far)
    wait_far(far)
    finish(1, columns, out_ref)
    lane = lax.broadcasted_iota(jnp.int32, (size, 128), 1)
    total = jnp.zeros((size, 128), jnp.float32)
    for k in range(levels):
        row = out_ref[k]
        total = jnp.where(lane == k, jnp.sum(row * row, axis=1, keepdims=True), total)
    held = sums_ref.shape[1]
    total = total.T
    sums_ref[0] = jnp.concatenate([total[:held], total[held : 2 * held]], axis=1)
    copies = [
        send(sums_ref.at[0], sums_ref.at[d], sum_sems, d, {"lon": lax.rem(place + d, around)})
        for d in range(1, around)
    ]
    start_all(copies)
    for copy in copies:
        copy.wait()
    total = sums_ref[place]
    for j in range(1, around):
        total = total + sums_ref[lax.rem(place - j + around, around)]
    total = total / (columns * around)
    total = jnp.concatenate([total[:, :size], total[:, size:]], axis=0)
    var_ref[...] = total[:levels]


def hand_out(from_out, from_var, to_out, to_var, sems):
    copies = [
        pltpu.make_async_copy(from_out, to_out, sems.at[0]),
        pltpu.make_async_copy(from_var, to_var, sems.at[1]),
    ]
    for copy in copies:
        copy.start()
    for copy in copies:
        copy.wait()


def local_pairs(previous, loss_matrix, pair_matrix, diffusivity, mixing):
    levels, size, columns = previous.shape
    count, around = lax.axis_size("lev"), lax.axis_size("lon")
    inner, full = (levels - 1) * size, columns + 128
    f32, bf16 = jnp.float32, jnp.bfloat16
    buf, sem = pltpu.VMEM, lambda n: pltpu.SemaphoreType.DMA((2, n))
    hbm = pl.BlockSpec(memory_space=pltpu.MemorySpace.HBM)
    packed = 3 * size // 2 + 8
    results = pl.pallas_call(
        step_kernel,
        out_shape=[
            jax.ShapeDtypeStruct((levels, size, columns), f32),
            jax.ShapeDtypeStruct((levels, size), f32),
        ],
        in_specs=[hbm] * 5,
        out_specs=[VMEM, VMEM],
        scratch_shapes=[
            pltpu.SMEM((levels,), f32),
            pltpu.SMEM((levels,), f32),
            buf((levels, size, size), f32),
            buf((levels, size, full), f32),
            buf((levels, size, size), f32),
            buf((levels, size, 4 * size), bf16),
            buf((2, size, 128), f32),
            buf((2, size, 128), f32),
            buf((inner, inner), bf16),
            buf((inner, inner), bf16),
            buf((packed, 2 * size), f32),
            buf((count, packed, 2 * size), f32),
            buf((inner, 2 * size), bf16),
            buf((inner, 2 * size), bf16),
            buf((count + 3, 2 * size, 2 * size), f32),
            buf((size, full), f32),
            buf((inner, full), bf16),
            buf((inner, full), bf16),
            buf((inner, full), f32),
            buf((2, 2, size, full), f32),
            buf((2, 2, size, full), f32),
            buf((2, size, full), f32),
            buf((2, size, full), f32),
            buf((2 * size, full), bf16),
            buf((2 * size, full), bf16),
            buf((levels * size, 2 * size), bf16),
            buf((levels * size, 2 * size), bf16),
            buf((levels * size, 4 * size), bf16),
            buf((size, 4 * size), bf16),
            buf((levels, size, full), f32),
            buf((around, -(-levels // 16) * 8, 2 * size), f32),
            buf((levels - 1, inner, size), f32),
            buf((inner, 4 * size), bf16),
            buf((inner, 4 * size), bf16),
            pltpu.SemaphoreType.DMA((5,)),
            sem(2),
            sem(count),
            sem(2),
            sem(10),
            sem(around),
        ],
        compiler_params=pltpu.CompilerParams(
            vmem_limit_bytes=40 * 2**20, collective_id=2, has_side_effects=True
        ),
    )(*(pltpu.with_memory_space_constraint(x, pltpu.MemorySpace.HBM) for x in (diffusivity, mixing, loss_matrix, previous, pair_matrix)))
    return pl.pallas_call(
        hand_out,
        out_shape=[jax.ShapeDtypeStruct(x.shape, x.dtype) for x in results],
        in_specs=[VMEM, VMEM],
        out_specs=[hbm, hbm],
        scratch_shapes=[pltpu.SemaphoreType.DMA((2,))],
        compiler_params=pltpu.CompilerParams(vmem_limit_bytes=2**20),
    )(*results)


def chosen(previous, *rest):
    paired = lax.axis_size("lev") == 4 and previous.shape[2] % 512 == 0
    return (local_pairs if paired else local)(previous, *rest)


def solution(mesh):
    placed = (P("lev", None, "lon"), P("lev", None, None), P("lev", None, None), P("lev"), P("lev"))
    return jax.shard_map(
        chosen,
        mesh=mesh,
        in_specs=placed,
        out_specs=(P("lev", None, "lon"), P("lev", None)),
        check_vma=False,
    )
```

```python
import functools
import itertools

import jax
import jax.numpy as jnp
from jax import lax
from jax.experimental import pallas as pl
from jax.experimental.pallas import tpu as pltpu
from jax.sharding import PartitionSpec as P

LEAST = 1.05
MOST = 10.0
HIGHEST = lax.Precision.HIGHEST
SMEM = pl.BlockSpec(memory_space=pltpu.SMEM)
VMEM = pl.BlockSpec(memory_space=pltpu.VMEM)


def dot(a, b, dims=((1,), (0,))):
    return lax.dot_general(
        a, b, (dims, ((), ())), precision=HIGHEST, preferred_element_type=jnp.float32
    )


def dot_t(a, b):
    return dot(a, b, ((1,), (1,)))


def eye_of(size):
    rows = lax.broadcasted_iota(jnp.int32, (size, size), 0)
    cols = lax.broadcasted_iota(jnp.int32, (size, size), 1)
    return rows == cols


def invert_all(blocks, floors, steps):
    size = blocks[0].shape[0]
    unit = jnp.where(eye_of(size), 1.0, 0.0).astype(jnp.float32)
    start, worst = [], None
    for a, lo in zip(blocks, floors):
        hi = jnp.max(jnp.sum(jnp.abs(a), axis=0, keepdims=True), axis=1, keepdims=True)
        hi = jnp.clip(hi, lo, lo * spread(size))
        scale = 2.0 / (hi + lo)
        rho = (hi - lo) / (hi + lo)
        start.append((scale, a))
        worst = rho if worst is None else jnp.maximum(worst, rho)

    def grow(rho):
        square = rho * rho
        return square / (2.0 - square), 2.0 / (2.0 - square)

    rho, gain = grow(worst)
    start = [(gain * scale) * (2.0 * unit - scale * a) for scale, a in start]

    def step(carry):
        rho, *xs = carry
        rest = [unit - dot(a, x) for a, x in zip(blocks, xs)]
        rho, gain = grow(rho)
        return (rho, *[gain * (x + dot(x, r)) for x, r in zip(xs, rest)])

    if steps is None:
        return lax.while_loop(lambda carry: jnp.max(carry[0]) > 3e-8, step, (rho, *start))[1:]
    return lax.fori_loop(0, steps, lambda i, carry: step(carry), (rho, *start))[1:]


def spread(size):
    return (1.0 + MOST * size) / (0.96 * LEAST)


def enough_steps(condition):
    rho, steps = (condition - 1.0) / (condition + 1.0), -1
    while rho > 3e-8:
        rho, steps = rho * rho / (2.0 - rho * rho), steps + 1
    return steps


def plan(lo, hi, out):
    if lo >= hi:
        return 0
    mid = lo + (hi - lo) // 2
    depth = 1 + max(plan(lo, mid, out), plan(mid + 1, hi, out))
    out.setdefault(depth, []).append((lo, mid, hi))
    return depth


def dense_inverse(diag, low, floor_diag, floor_low, steps=None):
    count, size = len(diag), diag[0].shape[0]
    unit = jnp.where(eye_of(size), 1.0, 0.0).astype(jnp.float32)
    by_depth, done, thin = {}, {}, {}
    plan(0, count, by_depth)
    for depth in sorted(by_depth):
        nodes = by_depth[depth]
        schur, arms, floors, thin_arms = [], [], [], []
        for lo, mid, hi in nodes:
            s, parts = diag[mid], []
            t, thin_parts = floor_diag[mid], []
            if lo < mid:
                arm = low_right(done[lo, mid][-1], low, mid, False)
                s = s - low(mid, arm[-size:])
                parts.append(arm)
                thin_parts += [floor_low[mid] * x for x in thin[lo, mid][-1]]
                t = t - floor_low[mid] * thin_parts[-1]
            parts.append(unit)
            thin_parts.append(1.0)
            if mid + 1 < hi:
                arm = low_right(done[mid + 1, hi][0], low, mid + 1, True)
                s = s - low(mid + 1, arm[:size], True)
                parts.append(arm)
                thin_arm = [floor_low[mid + 1] * x for x in thin[mid + 1, hi][0]]
                t = t - floor_low[mid + 1] * thin_arm[0]
                thin_parts += thin_arm
            schur.append(s)
            floors.append(t)
            arms.append(jnp.concatenate(parts, axis=0) if len(parts) > 1 else parts[0])
            thin_arms.append(thin_parts)
        inverses = invert_all(schur, [0.97 * t for t in floors], steps)
        for (lo, mid, hi), v, z, thin_v, t in zip(nodes, arms, inverses, thin_arms, floors):
            thin[lo, hi] = [[a * b / t for b in thin_v] for a in thin_v]
            for a, b in ((lo, mid), (mid + 1, hi)):
                for i in range(a, b):
                    for j in range(a, b):
                        thin[lo, hi][i - lo][j - lo] += thin[a, b][i - a][j - a]
            if hi - lo == 1:
                done[lo, hi] = [z]
                continue
            w = dot(v, z)
            panels = []
            for k in range(lo, hi):
                vk = v[(k - lo) * size : (k - lo + 1) * size]
                new = w if k == mid else dot_t(w, vk)
                pieces = []
                for a, b in ((lo, mid), (mid, mid + 1), (mid + 1, hi)):
                    if a >= b:
                        continue
                    piece = new[(a - lo) * size : (b - lo) * size]
                    if a <= k < b and k != mid:
                        piece = piece + done[a, b][k - a]
                    pieces.append(piece)
                panels.append(jnp.concatenate(pieces, axis=0) if len(pieces) > 1 else pieces[0])
            done[lo, hi] = panels
    return done[0, count], thin[0, count]


def low_right(panel, low, k, plain):
    return low(k, panel, not plain, True)


def split(x):
    high = x.astype(jnp.bfloat16)
    return high, (x - high.astype(jnp.float32)).astype(jnp.bfloat16)


def dot3(a_high, a_low, b):
    b_high, b_low = split(b)
    mul = functools.partial(jnp.dot, preferred_element_type=jnp.float32)
    return mul(a_high, b_high) + (mul(a_low, b_high) + mul(a_high, b_low))


def factor_kernel(links_ref, top_ref, loss_ref, high_ref, low_ref, ends_ref, send_ref):
    levels, size = loss_ref.shape[0], loss_ref.shape[1]
    inner = levels - 1
    on_diag = eye_of(size)
    top_link, inner_link = top_ref[0:1, 0:1], jnp.full((1, 1), links_ref[inner - 1])
    links = [jnp.full((1, 1), links_ref[k]) for k in range(levels)]

    def diag_of(k):
        above = top_link if k == 0 else links[k - 1]
        return loss_ref[k] + jnp.where(on_diag, 1.0 + above + links[k], 0.0)

    def low(k, x, transposed=False, right=False):
        return links_ref[k - 1] * x

    floor_diag = [
        LEAST + links[k] + (top_link if k == 0 else links[k - 1]) for k in range(levels)
    ]
    panels, thin = dense_inverse(
        [diag_of(k) for k in range(inner)], low, floor_diag[:inner], [top_link] + links[: inner - 1]
    )
    for k, panel in enumerate(panels):
        high, rest = split(panel)
        high_ref[:, k * size : (k + 1) * size] = high
        low_ref[:, k * size : (k + 1) * size] = rest
    ends_ref[0] = top_link * panels[0]
    ends_ref[1] = inner_link * panels[-1]
    blocks = [
        (
            diag_of(inner) - inner_link * inner_link * panels[-1][-size:],
            floor_diag[inner] - inner_link * inner_link * thin[-1][-1],
        ),
        (top_link * top_link * panels[0][:size], top_link * top_link * thin[0][0]),
        (inner_link * top_link * panels[0][-size:], inner_link * top_link * thin[0][-1]),
    ]
    for k, (block, floor) in enumerate(blocks):
        send_ref[k, :size] = block
        send_ref[k, size:] = jnp.broadcast_to(floor, (8, size))


def interface(all_ref, ends_ref, high_ref, low_ref, rows_ref):
    count, size = all_ref.shape[0], all_ref.shape[3]

    def diag_of(rows, cols):
        own = [all_ref[k, 0, rows, cols] for k in range(count)]
        return [
            own[k] - all_ref[k + 1, 1, rows, cols] if k + 1 < count else own[k]
            for k in range(count)
        ]

    def low(k, x, transposed=False, right=False):
        block = all_ref[k, 2, :size]
        if right:
            return dot_t(x, block) if transposed else dot(x, block)
        return dot(block, x, ((0,), (0,))) if transposed else dot(block, x)

    thin = slice(size, size + 1), slice(0, 1)
    panels, _ = dense_inverse(
        diag_of(slice(0, size), slice(0, size)),
        low,
        diag_of(*thin),
        [all_ref[k, 2, thin[0], thin[1]] for k in range(count)],
        enough_steps(spread(size)),
    )
    for k, panel in enumerate(panels):
        rows_ref[k] = panel
    me = lax.axis_index("lev")
    own = rows_ref[me]
    above = rows_ref[jnp.maximum(me - 1, 0)]
    inner = dot_t(ends_ref[0], above) + dot_t(ends_ref[1], own)
    length = inner.shape[0]
    high_ref[:length], low_ref[:length] = split(inner)
    high_ref[length:], low_ref[length:] = split(own.T)


def send(src, dst, sems, slot, device):
    return pltpu.make_async_remote_copy(
        src_ref=src,
        dst_ref=dst,
        send_sem=sems.at[0, slot],
        recv_sem=sems.at[1, slot],
        device_id=device,
        device_id_type=pl.DeviceIdType.MESH,
    )


def greet(lev_all, lon_all):
    barrier = pltpu.get_barrier_semaphore()
    partners = []
    for axis, everyone in (("lev", lev_all), ("lon", lon_all)):
        count, me = lax.axis_size(axis), lax.axis_index(axis)
        if everyone is None:
            continue
        steps = range(1, count) if everyone else sorted({1, count - 1})
        partners += [{axis: lax.rem(me + d, count)} for d in steps if d % count]
    for device in partners:
        pl.semaphore_signal(
            barrier, inc=1, device_id=device, device_id_type=pl.DeviceIdType.MESH
        )
    pl.semaphore_wait(barrier, len(partners))


def pack_edges(cur_ref, edges_ref):
    levels, size, columns = cur_ref.shape
    lane = lax.broadcasted_iota(jnp.int32, (size, 128), 1)
    last = jnp.zeros((size, 128), jnp.float32)
    first = last
    for k in range(levels):
        tail = pltpu.roll(cur_ref[k, :, columns - 128 :], k + 1, 1)
        head = cur_ref[k, :, :128]
        head = pltpu.roll(head, k, 1) if k else head
        last = jnp.where(lane == k, tail, last)
        first = jnp.where(lane == k, head, first)
    edges_ref[0] = last
    edges_ref[1] = first


def halo_copies(edges_ref, halo_ref, sems):
    around, me = lax.axis_size("lon"), lax.axis_index("lon")
    return [
        send(edges_ref.at[0], halo_ref.at[0], sems, 0, {"lon": lax.rem(me + 1, around)}),
        send(edges_ref.at[1], halo_ref.at[1], sems, 1, {"lon": lax.rem(me + around - 1, around)}),
    ]


def local_forcing(mix_ref, cur_ref, prev_ref, pair_ref, force_ref):
    levels, size, columns = cur_ref.shape
    lane = lax.broadcasted_iota(jnp.int32, (size, columns), 1)
    for k in range(levels):
        c = cur_ref[k]
        back = jnp.where(lane == 0, 0.0, pltpu.roll(c, 1, 1))
        ahead = jnp.where(lane == columns - 1, 0.0, pltpu.roll(c, columns - 1, 1))
        p_high, p_low = split(pair_ref[k])
        chem = dot3(p_high, p_low, c * c)
        force_ref[k * size : (k + 1) * size] = (
            prev_ref[k] - chem + mix_ref[k] * (back + ahead - 2.0 * c)
        )


def add_halo(mix_ref, halo_ref, force_ref):
    levels = mix_ref.shape[0]
    size, columns = halo_ref.shape[1], force_ref.shape[1]
    lane = lax.broadcasted_iota(jnp.int32, (size, 128), 1)
    before, after = halo_ref[0], halo_ref[1]
    for k in range(levels):
        rows = slice(k * size, (k + 1) * size)
        at_head = pltpu.roll(before, 128 - k, 1) if k else before
        at_tail = pltpu.roll(after, 127 - k, 1)
        force_ref[rows, :128] += jnp.where(lane == 0, mix_ref[k] * at_head, 0.0)
        force_ref[rows, columns - 128 :] += jnp.where(lane == 127, mix_ref[k] * at_tail, 0.0)


def couple(
    links_ref, top_link, g_high, g_low, force_ref, part_ref, f_high, f_low, top_out, top_in, sides_ref,
    sems, direct,
):
    count, me = lax.axis_size("lev"), lax.axis_index("lev")
    inner, size = part_ref.shape[0], top_out.shape[0]
    f_high[...], f_low[...] = split(force_ref[:inner])
    mul = functools.partial(jnp.dot, preferred_element_type=jnp.float32)

    def rows_of(start, stop):
        a, b = g_high[start:stop], g_low[start:stop]
        part = mul(a, f_high[...]) + (mul(b, f_high[...]) + mul(a, f_low[...]))
        part_ref[start:stop] = part
        return part

    top_out[...] = top_link * rows_of(0, size)
    sides_ref[me] = force_ref[inner:] + links_ref[inner // size - 1] * rows_of(inner - size, inner)
    up = send(top_out, top_in, sems, 0, {"lev": lax.rem(me + count - 1, count)})
    half = size * ((inner // size) // 2)

    @pl.when(me > 0)
    def _():
        up.start()

    rows_of(size, half)

    @pl.when(me < count - 1)
    def _():
        up.wait_recv()
        sides_ref[me] += top_in[...]

    partner = me + 1 - 2 * lax.rem(me, 2)
    copies = [
        send(sides_ref.at[me], sides_ref.at[me], sems, d, {"lev": lax.rem(me + d, count)})
        for d in range(1 if direct else 2, count, 1 if direct else 2)
    ]
    onward = [] if direct else [send(sides_ref.at[me], sides_ref.at[me], sems, 1, {"lev": partner})]
    for d in range(count if direct else 2, count, 2):
        origin = lax.rem(me - d + count, count)
        onward.append(
            send(sides_ref.at[origin], sides_ref.at[origin], sems, d + 1, {"lev": partner})
        )
    for copy in copies + onward[:1]:
        copy.start()
    rows_of(half, inner - size)

    @pl.when(me > 0)
    def _():
        up.wait_send()

    return copies, onward


def relay(copies, onward):
    for copy, later in zip(copies, onward[1:]):
        copy.wait_recv()
        later.start()
    for copy in copies:
        copy.wait_send()
    for copy in onward:
        copy.wait()


def finish(part_ref, sides_ref, high_ref, low_ref, out_ref):
    levels, size, columns = out_ref.shape
    count = sides_ref.shape[0]
    b_high, b_low = split(sides_ref[...].reshape(count * size, columns))
    mul = functools.partial(jnp.dot, preferred_element_type=jnp.float32)
    for k in range(levels):
        rows = slice(k * size, (k + 1) * size)
        a, b = high_ref[rows], low_ref[rows]
        row = mul(a, b_high) + (mul(b, b_high) + mul(a, b_low))
        out_ref[k] = row + part_ref[rows] if k < levels - 1 else row


def open_kernel(
    links_ref, mix_ref, prev_ref, pair_ref, force_ref, top_ref, edges, halo, link_out, sems
):
    levels = prev_ref.shape[0]
    count, me = lax.axis_size("lev"), lax.axis_index("lev")
    pack_edges(prev_ref, edges)
    link_out[...] = jnp.full(link_out.shape, links_ref[levels - 1], jnp.float32)
    greet(False, False)
    copies = halo_copies(edges, halo, sems)
    down = send(link_out, top_ref, sems, 2, {"lev": lax.rem(me + 1, count)})
    for copy in copies:
        copy.start()

    @pl.when(me < count - 1)
    def _():
        down.start()

    @pl.when(me == 0)
    def _():
        top_ref[...] = jnp.zeros(top_ref.shape, jnp.float32)

    local_forcing(mix_ref, prev_ref, prev_ref, pair_ref, force_ref)
    for copy in copies:
        copy.wait()
    add_halo(mix_ref, halo, force_ref)

    @pl.when(me < count - 1)
    def _():
        down.wait_send()

    @pl.when(me > 0)
    def _():
        down.wait_recv()


def newton_kernel(
    links_ref, mix_ref, top_ref, sent_ref, ends_ref, first_force, g_high, g_low, prev_ref, pair_ref,
    out_ref, var_ref, all_ref, rows_ref, h_high, h_low, cur_ref, edges, halo, force_ref, part_ref,
    first_sides, sides_ref, f_high, f_low, first_out, first_in, top_out, top_in, sums_ref,
    block_sems, first_sems, halo_sems, sems, sum_sems,
):
    levels, size, columns = prev_ref.shape
    count, me = lax.axis_size("lev"), lax.axis_index("lev")
    around, place = lax.axis_size("lon"), lax.axis_index("lon")
    greet(True, True)
    blocks = [
        send(sent_ref, all_ref.at[me], block_sems, d, {"lev": lax.rem(me + d, count)})
        for d in range(1, count)
    ]
    for copy in blocks:
        copy.start()
    all_ref[me] = sent_ref[...]
    copies = couple(
        links_ref, top_ref[0:1, 0:1], g_high, g_low, first_force, part_ref, f_high, f_low,
        first_out, first_in, first_sides, first_sems, True,
    )
    for copy in blocks:
        copy.wait()
    interface(all_ref, ends_ref, h_high, h_low, rows_ref)
    for copy in copies[0]:
        copy.wait()
    finish(part_ref, first_sides, h_high, h_low, cur_ref)
    pack_edges(cur_ref, edges)
    copies = halo_copies(edges, halo, halo_sems)
    for copy in copies:
        copy.start()
    local_forcing(mix_ref, cur_ref, prev_ref, pair_ref, force_ref)
    for copy in copies:
        copy.wait()
    add_halo(mix_ref, halo, force_ref)
    copies = couple(
        links_ref, top_ref[0:1, 0:1], g_high, g_low, force_ref, part_ref, f_high, f_low,
        top_out, top_in, sides_ref, sems, False,
    )
    relay(*copies)
    finish(part_ref, sides_ref, h_high, h_low, out_ref)
    lane = lax.broadcasted_iota(jnp.int32, (size, 128), 1)
    total = jnp.zeros((size, 128), jnp.float32)
    for k in range(levels):
        row = out_ref[k]
        total = jnp.where(lane == k, jnp.sum(row * row, axis=1, keepdims=True), total)
    sums_ref[0] = total.T[: sums_ref.shape[1]]
    copies = [
        send(sums_ref.at[0], sums_ref.at[d], sum_sems, d, {"lon": lax.rem(place + d, around)})
        for d in range(1, around)
    ]
    for copy in copies:
        copy.start()
    for copy in copies:
        copy.wait()
    total = sums_ref[place]
    for j in range(1, around):
        total = total + sums_ref[lax.rem(place - j + around, around)]
    var_ref[...] = (total / (columns * around))[:levels]


def call(kernel, outs, places, scratch=(), group=None):
    extra = {} if group is None else {"collective_id": group, "has_side_effects": True}
    return pl.pallas_call(
        kernel,
        out_shape=[jax.ShapeDtypeStruct(shape, dtype) for shape, dtype in outs],
        in_specs=places,
        out_specs=[VMEM] * len(outs),
        scratch_shapes=list(scratch),
        compiler_params=pltpu.CompilerParams(vmem_limit_bytes=60 * 2**20, **extra),
    )


def local(previous, loss_matrix, pair_matrix, diffusivity, mixing):
    levels, size, columns = previous.shape
    count = lax.axis_size("lev")
    around = lax.axis_size("lon")
    inner = (levels - 1) * size
    f32, bf16 = jnp.float32, jnp.bfloat16
    buf, sem = pltpu.VMEM, lambda n: pltpu.SemaphoreType.DMA((2, n))
    force, top = call(
        open_kernel,
        [((levels * size, columns), f32), ((8, 128), f32)],
        [SMEM, SMEM, VMEM, VMEM],
        [buf((2, size, 128), f32), buf((2, size, 128), f32), buf((8, 128), f32), sem(3)],
        0,
    )(diffusivity, mixing, previous, pair_matrix)
    g_high, g_low, ends, sent = call(
        factor_kernel,
        [((inner, inner), bf16), ((inner, inner), bf16), ((2, inner, size), f32), ((3, size + 8, size), f32)],
        [SMEM, VMEM, VMEM],
    )(diffusivity, top, loss_matrix)
    return call(
        newton_kernel,
        [((levels, size, columns), f32), ((levels, size), f32)],
        [SMEM, SMEM] + [VMEM] * 8,
        [
            buf((count, 3, size + 8, size), f32),
            buf((count, count * size, size), f32),
            buf((levels * size, count * size), bf16),
            buf((levels * size, count * size), bf16),
            buf((levels, size, columns), f32),
            buf((2, size, 128), f32),
            buf((2, size, 128), f32),
            buf((levels * size, columns), f32),
            buf((inner, columns), f32),
            buf((count, size, columns), f32),
            buf((count, size, columns), f32),
            buf((inner, columns), bf16),
            buf((inner, columns), bf16),
            buf((size, columns), f32),
            buf((size, columns), f32),
            buf((size, columns), f32),
            buf((size, columns), f32),
            buf((around, -(-levels // 8) * 8, size), f32),
            sem(count),
            sem(count),
            sem(2),
            sem(count),
            sem(around),
        ],
        1,
    )(diffusivity, mixing, top, sent, ends, force, g_high, g_low, previous, pair_matrix)


def cat3(a_high, a_low, b_high, b_low):
    return jnp.dot(
        jnp.concatenate([a_high, a_low, a_high], axis=1),
        jnp.concatenate([b_high, b_high, b_low], axis=0),
        preferred_element_type=jnp.float32,
    )


def wide(a):
    high, low = split(a)
    return jnp.concatenate([high, low, high, jnp.zeros_like(high)], axis=1)


def tall(b):
    high, low = split(b)
    return jnp.concatenate([high, high, low, jnp.zeros_like(high)], axis=0)


def wide_dot(a, b):
    return jnp.dot(a, b, preferred_element_type=jnp.float32)


def near_dot(a, b):
    return lax.dot_general(
        a, b, (((1,), (0,)), ((), ())), precision=lax.Precision.HIGH, preferred_element_type=jnp.float32
    )


def pull(links, loss):
    stiff = links[0]
    for a in links[1:]:
        own = 1.0 + loss + stiff
        stiff = a * own / (a + own)
    return stiff


def worst_ratio(above, below):
    sides = []
    for count in (above, below):
        draws = itertools.product((200.0, 2000.0), repeat=min(count, 8) + 1)
        sides.append([(pull(d, 640.0), pull(d, 0.05)) for d in draws])
    return 1.15 * max((641.0 + a + c) / (1.05 + b + d) for a, b in sides[0] for c, d in sides[1])


def edge_ratios(inner):
    inner = min(inner, 8)
    held = [(pull(d, 640.0), pull(d, 0.05)) for d in itertools.product((200.0, 2000.0), repeat=inner + 1)]
    draws = [(0.0, *d) for d in itertools.product((200.0, 2000.0), repeat=inner + 1)]
    free = [(pull(d, 640.0), pull(d, 0.05)) for d in draws]
    outer = max((641.0 + a) / (1.05 + b) for a, b in held)
    outer = max(outer, max((320.5 + a) / (0.525 + b) for a, b in held))
    second = max((641.0 + a + c) / (1.05 + b + d) for a, b in held for c, d in free)
    return 1.15 * outer, 1.15 * second


def gains_for(ratio):
    rho, gains = (ratio - 1.0) / (ratio + 1.0), []
    while rho > 1.2e-3:
        gains.append(2.0 / (2.0 - rho * rho))
        rho = rho * rho / (2.0 - rho * rho)
    return gains


def invert_fixed(blocks, floors, ratio):
    size = blocks[0].shape[0]
    unit = jnp.where(eye_of(size), 1.0, 0.0).astype(jnp.float32)
    gains = gains_for(ratio)
    xs, rests = [], []
    for a, low in zip(blocks, floors):
        scale = (2.0 / (1.0 + ratio)) / low
        rest = unit - scale * a
        xs.append((gains[0] * scale) * (unit + rest))
        rests.append(rest)
    rests = [gains[0] * dot(r, r) - (gains[0] - 1.0) * unit for r in rests]
    for step, g in enumerate(gains[1:]):
        left = len(gains) - step - 2
        mul = dot if left > 2 else near_dot
        if left == 0:
            xs = [g * (x + mul(x, r)) for x, r in zip(xs, rests)]
            break
        both = [mul(jnp.concatenate([x, r], axis=0), r) for x, r in zip(xs, rests)]
        xs = [g * (x + b[:size]) for x, b in zip(xs, both)]
        rests = [g * b[size:] - (g - 1.0) * unit for b in both]
    rests = [unit - dot(a, x) for a, x in zip(blocks, xs)]
    return [x + near_dot(x, r) for x, r in zip(xs, rests)]


def chain_factor(diag, links, floors, panel_ref, hook):
    count, size = len(diag), diag[0].shape[0]
    unit = jnp.where(eye_of(size), 1.0, 0.0).astype(jnp.float32)
    by_depth, thin, corners = {}, {}, {}
    plan(0, count, by_depth)

    def rows(lo, hi):
        return slice(lo * size, hi * size)

    for depth in sorted(by_depth):
        nodes = by_depth[depth]
        ratio = max(worst_ratio(mid - lo, hi - 1 - mid) for lo, mid, hi in nodes)
        schur, arms, lows, thin_arms = [], [], [], []
        for lo, mid, hi in nodes:
            s, parts = diag[mid], []
            t, thin_parts = floors[mid], []
            if lo < mid:
                arm = links[mid] * panel_ref[mid - 1, rows(lo, mid)]
                s = s - (links[mid] * links[mid]) * corners[lo, mid][1]
                parts.append(arm)
                thin_parts += [links[mid] * x for x in thin[lo, mid][-1]]
                t = t - links[mid] * thin_parts[-1]
            parts.append(unit)
            thin_parts.append(1.0)
            if mid + 1 < hi:
                arm = links[mid + 1] * panel_ref[mid + 1, rows(mid + 1, hi)]
                s = s - (links[mid + 1] * links[mid + 1]) * corners[mid + 1, hi][0]
                parts.append(arm)
                thin_arm = [links[mid + 1] * x for x in thin[mid + 1, hi][0]]
                t = t - links[mid + 1] * thin_arm[0]
                thin_parts += thin_arm
            schur.append(s)
            lows.append(t)
            arms.append(jnp.concatenate(parts, axis=0) if len(parts) > 1 else parts[0])
            thin_arms.append(thin_parts)
        inverses = invert_fixed(schur, [0.97 * t for t in lows], ratio)
        for (lo, mid, hi), v, z, thin_v, t in zip(nodes, arms, inverses, thin_arms, lows):
            thin[lo, hi] = [[a * b / t for b in thin_v] for a in thin_v]
            for a, b in ((lo, mid), (mid + 1, hi)):
                for i in range(a, b):
                    for j in range(a, b):
                        thin[lo, hi][i - lo][j - lo] += thin[a, b][i - a][j - a]
            if hi - lo == 1:
                panel_ref[mid, rows(mid, hi)] = z
                corners[lo, hi] = z, z
                continue
            ends = v[:size], v[-size:]
            arms_out = [dot(x, z) for x in ends]
            corners[lo, hi] = tuple(
                z if at == mid else corners[part][side] + dot_t(y, x)
                for side, (at, part, x, y) in enumerate(
                    ((lo, (lo, mid), ends[0], arms_out[0]), (hi - 1, (mid + 1, hi), ends[1], arms_out[1]))
                )
            )
            if hi - lo == count:
                far = dot_t(arms_out[1], ends[0])
            w = near_dot(v, z) if hi - lo == count else dot(v, z)
            if hi - lo == count:
                continue
            new = dot_t(w, v)
            for k in range(lo, hi):
                own = new[:, (k - lo) * size : (k - lo + 1) * size]
                panel_ref[k, rows(mid, mid + 1)] = own[rows(mid - lo, mid - lo + 1)]
                for a, b in ((lo, mid), (mid + 1, hi)):
                    if a >= b:
                        continue
                    piece = own[rows(a - lo, b - lo)]
                    if a <= k < b:
                        piece = piece + panel_ref[k, rows(a, b)]
                    panel_ref[k, rows(a, b)] = piece
        if depth < max(by_depth):
            hook(depth)
    return v, w, by_depth[max(by_depth)][0][1], thin[0, count], (*corners[0, count], far)


def fold(x):
    half = x.shape[0] // 2
    return jnp.concatenate([x[:half], x[half:]], axis=1)


def unfold(x):
    half = x.shape[1] // 2
    return jnp.concatenate([x[:, :half], x[:, half:]], axis=0)


def pack_pairs(field_ref, columns, edges_ref):
    levels, size = field_ref.shape[:2]
    lane = lax.broadcasted_iota(jnp.int32, (size, 128), 1)
    last = jnp.zeros((size, 128), jnp.float32)
    first = last
    for k in range(levels):
        tail = pltpu.roll(field_ref[k, :, columns - 128 : columns], (2 * k + 2) % 128, 1)
        head = field_ref[k, :, :128]
        head = pltpu.roll(head, 2 * k, 1) if k else head
        mine = (lane == 2 * k) | (lane == 2 * k + 1)
        last = jnp.where(mine, tail, last)
        first = jnp.where(mine, head, first)
    edges_ref[0] = last
    edges_ref[1] = first


def unpack_pairs(halo_ref, columns, field_ref):
    levels, size = field_ref.shape[:2]
    lane = lax.broadcasted_iota(jnp.int32, (size, 128), 1)
    before, after = halo_ref[0], halo_ref[1]
    for k in range(levels):
        at_head = pltpu.roll(after, (128 - 2 * k) % 128, 1) if k else after
        at_tail = pltpu.roll(before, (126 - 2 * k) % 128, 1)
        field_ref[k, :, columns:] = jnp.where(lane < 2, at_head, jnp.where(lane >= 126, at_tail, 0.0))


def forcing(mix_ref, cur_ref, prev_ref, pairs_ref, width, sep_ref, f_high, f_low):
    levels, size, full = cur_ref.shape
    for k in range(levels):
        c = cur_ref[k]
        ring = pltpu.roll(c, 1, 1) + pltpu.roll(c, full - 1, 1)
        own = c[:, :width]
        chem = wide_dot(pairs_ref[k], tall(own * own))
        force = prev_ref[k, :, :width] - chem + mix_ref[k] * (ring[:, :width] - 2.0 * own)
        if k == 0:
            sep_ref[:, :width] = force
        else:
            rows = slice((k - 1) * size, k * size)
            f_high[rows, :width], f_low[rows, :width] = split(force)


def start_all(copies):
    @pl.when(lax.axis_index("lev") < lax.axis_size("lev"))
    def _():
        for copy in copies:
            copy.start()


def step_kernel(
    links_hbm, mix_hbm, loss_hbm, prev_hbm, pair_hbm, out_ref, var_ref, links_ref, mix_ref,
    loss_ref, prev_ref, pair_ref, pairs_ref, edges, halo, z_high, z_low, send_ref, all_ref,
    ends_high, ends_low, table_ref, sep_ref, f_high, f_low, part_ref, own_ref, near_ref, mine_ref, far_ref,
    side_high, side_low, hq_high, hq_low, u_ref, top_ref, cur_ref, sums_ref, panel_ref, w_ref, v_ref,
    load_sems, halo_sems, block_sems, near_sems, far_sems, sum_sems,
):
    levels, size, columns = prev_hbm.shape
    inner = levels - 1
    full = cur_ref.shape[2]
    count, me = lax.axis_size("lev"), lax.axis_index("lev")
    around, place = lax.axis_size("lon"), lax.axis_index("lon")
    core, chip = lax.rem(me, 2), me // 2
    partner = me + 1 - 2 * core
    across = lax.rem(me + 2, count)

    loads = [
        pltpu.make_async_copy(loss_hbm, loss_ref, load_sems.at[0]),
        pltpu.make_async_copy(prev_hbm, prev_ref.at[:, :, pl.ds(0, columns)], load_sems.at[1]),
        pltpu.make_async_copy(pair_hbm, pair_ref, load_sems.at[2]),
        pltpu.make_async_copy(links_hbm, links_ref, load_sems.at[3]),
        pltpu.make_async_copy(mix_hbm, mix_ref, load_sems.at[4]),
    ]
    for k in (3, 0, 1, 2, 4):
        loads[k].start()
    barrier = pltpu.get_barrier_semaphore()
    partners = [{"lev": lax.rem(me + d, count)} for d in range(1, count)]
    partners += [{"lon": lax.rem(place + d, around)} for d in range(1, around)]
    for device in partners:
        pl.semaphore_signal(barrier, inc=1, device_id=device, device_id_type=pl.DeviceIdType.MESH)

    loads[3].wait()
    links = [jnp.full((1, 1), links_ref[k]) for k in range(levels)]
    on_diag = eye_of(size)
    halo_moves = halo_copies(edges, halo, halo_sems)

    def hook(depth):
        if depth != 2:
            return
        loads[1].wait()
        pack_pairs(prev_ref, columns, edges)
        pl.semaphore_wait(barrier, len(partners))
        start_all(halo_moves)

    loads[0].wait()
    diag = [
        loss_ref[k] + jnp.where(on_diag, 1.0 + links[k] + (links[k - 1] if k else 0.0), 0.0)
        for k in range(levels)
    ]
    floors = [LEAST + links[k] + (links[k - 1] if k else 0.0) for k in range(levels)]
    v, w, mid, thin, (z_first, z_last, z_far) = chain_factor(diag[1:], links[:inner], floors[1:], panel_ref, hook)
    a, b = links[0], links[inner]
    sub = lax.broadcasted_iota(jnp.int32, (8, 128), 0)
    send_ref[: size // 2] = fold(diag[0] - a * a * z_first)
    send_ref[size // 2 : size] = fold(jnp.where(on_diag, b, 0.0) - b * b * z_last)
    send_ref[size : 3 * size // 2] = fold(a * b * z_far)
    send_ref[3 * size // 2 :] = jnp.where(
        sub == 0, floors[0] - a * a * thin[0][0], jnp.where(sub == 1, b - b * b * thin[-1][-1], a * b * thin[0][-1])
    )
    blocks = [
        send(send_ref, all_ref.at[me], block_sems, d, {"lev": lax.rem(me + d, count)})
        for d in range(1, count)
    ]
    start_all(blocks)
    all_ref[me] = send_ref[...]

    old = [
        panel_ref[0, : mid * size],
        jnp.zeros((size, size), jnp.float32),
        panel_ref[inner - 1, (mid + 1) * size :],
    ]
    tips = dot_t(w, jnp.concatenate([v[:size], v[-size:]], axis=0))
    first = tips[:, :size] + jnp.concatenate([old[0], old[1], jnp.zeros_like(old[2])], axis=0)
    last = tips[:, size:] + jnp.concatenate([jnp.zeros_like(old[0]), old[1], old[2]], axis=0)
    ends_high[...], ends_low[...] = split(jnp.concatenate([a * first, b * last], axis=1))
    w_ref[...] = wide(w)
    v_high, v_low = split(v)
    v_ref[...] = jnp.concatenate([v_high, v_high, v_low, jnp.zeros_like(v_high)], axis=1)

    def form(lo, hi):
        spot = slice(lo * size, hi * size)
        new = lax.dot_general(
            w_ref[spot], v_ref[...], (((1,), (1,)), ((), ())), preferred_element_type=jnp.float32
        )
        start, stop = (0, mid) if lo < mid else (mid + 1, inner)
        if lo != mid:
            zeros = jnp.zeros((new.shape[0], size), jnp.float32)
            new = new + jnp.concatenate(
                [panel_ref[j, spot] if start <= j < stop else zeros for j in range(inner)], axis=1
            )
        z_high[spot], z_low[spot] = split(new)

    form(0, 1)
    form(inner - 1, inner)
    loads[2].wait()
    loads[4].wait()
    for k in range(levels):
        pairs_ref[k] = wide(pair_ref[k])
    for move in halo_moves:
        move.wait()
    unpack_pairs(halo, columns, prev_ref)

    def z_rows(start, stop, width):
        return cat3(z_high[start:stop], z_low[start:stop], f_high[:, :width], f_low[:, :width])

    def ends(turn, width):
        rows = cat3(
            jnp.concatenate([z_high[:size], z_high[-size:]], axis=0),
            jnp.concatenate([z_low[:size], z_low[-size:]], axis=0),
            f_high[:, :width],
            f_low[:, :width],
        )
        part_ref[:size, :width] = rows[:size]
        part_ref[-size:, :width] = rows[size:]
        own_ref[turn, 0, :, :width] = sep_ref[:, :width] + a * rows[:size]
        own_ref[turn, 1, :, :width] = b * rows[size:]
        copy = send(
            own_ref.at[turn, :, :, pl.ds(0, width)], near_ref.at[turn, :, :, pl.ds(0, width)], near_sems, turn,
            {"lev": partner},
        )
        start_all([copy])
        return copy

    def middle(width):
        part_ref[size:-size, :width] = z_rows(size, (inner - 1) * size, width)

    def merge(turn, width):
        upper = core == 0
        s_own, t_own = own_ref[turn, 0, :, :width], own_ref[turn, 1, :, :width]
        s_in, t_in = near_ref[turn, 0, :, :width], near_ref[turn, 1, :, :width]
        low_side = jnp.where(upper, s_own, s_in)
        high_side = jnp.where(upper, s_in + t_own, s_own + t_in)
        side_high[:size, :width], side_low[:size, :width] = split(low_side)
        side_high[size:, :width], side_low[size:, :width] = split(high_side)
        return jnp.where(chip == 0, jnp.where(upper, t_in, t_own), 0.0)

    def condense(turn, width, tail, k_high, k_low):
        mine_ref[turn, :, :width] = tail + cat3(k_high, k_low, side_high[:, :width], side_low[:, :width])
        half, quarter = columns // 2, columns // 4
        first = pl.ds(pl.multiple_of(core * half, 128), quarter)
        second = pl.ds(pl.multiple_of(core * half + quarter, 128), quarter)
        routes = [(mine_ref, first, across), (mine_ref, second, across), (mine_ref, second, lax.rem(partner + 2, count))]
        routes += [(mine_ref, pl.ds(columns, width - columns), across)] if width > columns else []
        routes += [(far_ref, first, partner)]
        copies = [
            send(src.at[turn, :, spot], far_ref.at[turn, :, spot], far_sems, 5 * turn + k, {"lev": device})
            for k, (src, spot, device) in enumerate(routes)
        ]
        start_all(copies[:-1])
        return copies

    def relay_far(copies):
        copies[0].wait_recv()
        start_all(copies[-1:])

    def wait_far(copies):
        copies[0].wait_send()
        for copy in copies[1:]:
            copy.wait()

    def gather_sides(width):
        rest = cat3(hq_high[...], hq_low[...], side_high[:, :width], side_low[:, :width])
        for k in range(levels):
            rows = rest[k * size : (k + 1) * size]
            cur_ref[k, :, :width] = rows if k == 0 else rows + part_ref[(k - 1) * size : k * size, :width]

    def finish(turn, width, to_ref):
        total = mine_ref[turn, :, :width] + far_ref[turn, :, :width]
        top = tall(wide_dot(top_ref[...], tall(total)))
        for k in range(levels):
            to_ref[k, :, :width] = cur_ref[k, :, :width] + wide_dot(u_ref[k * size : (k + 1) * size], top)

    forcing(mix_ref, prev_ref, prev_ref, pairs_ref, full, sep_ref, f_high, f_low)
    near = ends(0, full)
    for lo, hi in ((1, mid), (mid, mid + 1), (mid + 1, inner - 1)):
        form(lo, hi)
    middle(full)
    for copy in blocks:
        copy.wait()

    def block(k, which):
        return unfold(all_ref[k, which * size // 2 : (which + 1) * size // 2])

    def floor(k, which):
        row = 3 * size // 2 + which
        return all_ref[k, row : row + 1, 0:1]

    ratio = spread(size)
    s = [block(k, 0) + (block(k - 1, 1) if k else 0.0) for k in range(count)]
    t = [floor(k, 0) + (floor(k - 1, 1) if k else 0.0) for k in range(count)]
    c = [None] + [block(k, 2) for k in range(count - 1)]
    e = [None] + [floor(k, 2) for k in range(count - 1)]
    outer, second = edge_ratios(inner)
    z0, z3 = invert_fixed([s[0], s[3]], [0.97 * t[0], 0.97 * t[3]], outer)
    a1, a3 = dot(c[1], z0), dot(z3, c[3])
    s1 = s[1] - dot_t(a1, c[1])
    t1 = t[1] - e[1] * e[1] / t[0]
    (z1,) = invert_fixed([s1], [0.97 * t1], second)
    a2 = dot(c[2], z1)
    s2 = s[2] - dot_t(a2, c[2]) - dot(c[3], a3, ((0,), (0,)))
    t2 = t[2] - e[2] * e[2] / t1 - e[3] * e[3] / t[3]
    b1 = near_dot(z1, a1)
    p0 = near_dot(a2, a1)
    zero = jnp.zeros((size, size), jnp.float32)
    unit = jnp.where(on_diag, 1.0, 0.0).astype(jnp.float32)
    sides = [
        (z0 + dot(a1, b1, ((0,), (0,))), b1.T, p0.T),
        (b1, z1, a2.T),
        (zero, zero, unit),
        (zero, z3, a3),
        (zero, zero, zero),
    ]
    for k, (left, right, top) in enumerate(sides):
        table_ref[k, :size] = jnp.concatenate([left, right], axis=1)
        table_ref[k, size:, :size] = top
    for k, (left, right) in enumerate(((p0, a2), (unit, a3.T))):
        table_ref[len(sides) + k, :size] = jnp.concatenate([left, right], axis=1)
    near.wait()
    tail = merge(0, full)
    k_high, k_low = split(table_ref[len(sides) + chip, :size])
    far = condense(0, full, tail, k_high, k_low)
    (z2,) = invert_fixed([s2], [0.97 * t2], ratio)
    top_ref[...] = wide(z2)
    own_q, next_q = table_ref[me, :size], table_ref[me + 1, :size]
    own_p, next_p = table_ref[me, size:, :size], table_ref[me + 1, size:, :size]
    q_high, q_low = split(jnp.concatenate([own_q, next_q], axis=0))
    p_high, p_low = split(jnp.concatenate([own_p, next_p], axis=0))
    hq_high[size:], hq_low[size:] = split(cat3(ends_high[...], ends_low[...], q_high, q_low))
    hq_high[:size], hq_low[:size] = split(own_q)
    u_ref[size:] = wide(cat3(ends_high[...], ends_low[...], p_high, p_low))
    u_ref[:size] = wide(own_p)
    relay_far(far)
    gather_sides(full)
    wait_far(far)
    finish(0, full, cur_ref)

    forcing(mix_ref, cur_ref, prev_ref, pairs_ref, columns, sep_ref, f_high, f_low)
    near = ends(1, columns)
    near.wait()
    tail = merge(1, columns)
    far = condense(1, columns, tail, k_high, k_low)
    middle(columns)
    gather_sides(columns)
    relay_far(far)
    wait_far(far)
    finish(1, columns, out_ref)
    lane = lax.broadcasted_iota(jnp.int32, (size, 128), 1)
    total = jnp.zeros((size, 128), jnp.float32)
    for k in range(levels):
        row = out_ref[k]
        total = jnp.where(lane == k, jnp.sum(row * row, axis=1, keepdims=True), total)
    held = sums_ref.shape[1]
    total = total.T
    sums_ref[0] = jnp.concatenate([total[:held], total[held : 2 * held]], axis=1)
    copies = [
        send(sums_ref.at[0], sums_ref.at[d], sum_sems, d, {"lon": lax.rem(place + d, around)})
        for d in range(1, around)
    ]
    start_all(copies)
    for copy in copies:
        copy.wait()
    total = sums_ref[place]
    for j in range(1, around):
        total = total + sums_ref[lax.rem(place - j + around, around)]
    total = total / (columns * around)
    total = jnp.concatenate([total[:, :size], total[:, size:]], axis=0)
    var_ref[...] = total[:levels]


def hand_out(from_out, from_var, to_out, to_var, sems):
    copies = [
        pltpu.make_async_copy(from_out, to_out, sems.at[0]),
        pltpu.make_async_copy(from_var, to_var, sems.at[1]),
    ]
    for copy in copies:
        copy.start()
    for copy in copies:
        copy.wait()


def local_pairs(previous, loss_matrix, pair_matrix, diffusivity, mixing):
    levels, size, columns = previous.shape
    count, around = lax.axis_size("lev"), lax.axis_size("lon")
    inner, full = (levels - 1) * size, columns + 128
    f32, bf16 = jnp.float32, jnp.bfloat16
    buf, sem = pltpu.VMEM, lambda n: pltpu.SemaphoreType.DMA((2, n))
    hbm = pl.BlockSpec(memory_space=pltpu.MemorySpace.HBM)
    packed = 3 * size // 2 + 8
    results = pl.pallas_call(
        step_kernel,
        out_shape=[
            jax.ShapeDtypeStruct((levels, size, columns), f32),
            jax.ShapeDtypeStruct((levels, size), f32),
        ],
        in_specs=[hbm] * 5,
        out_specs=[VMEM, VMEM],
        scratch_shapes=[
            pltpu.SMEM((levels,), f32),
            pltpu.SMEM((levels,), f32),
            buf((levels, size, size), f32),
            buf((levels, size, full), f32),
            buf((levels, size, size), f32),
            buf((levels, size, 4 * size), bf16),
            buf((2, size, 128), f32),
            buf((2, size, 128), f32),
            buf((inner, inner), bf16),
            buf((inner, inner), bf16),
            buf((packed, 2 * size), f32),
            buf((count, packed, 2 * size), f32),
            buf((inner, 2 * size), bf16),
            buf((inner, 2 * size), bf16),
            buf((count + 3, 2 * size, 2 * size), f32),
            buf((size, full), f32),
            buf((inner, full), bf16),
            buf((inner, full), bf16),
            buf((inner, full), f32),
            buf((2, 2, size, full), f32),
            buf((2, 2, size, full), f32),
            buf((2, size, full), f32),
            buf((2, size, full), f32),
            buf((2 * size, full), bf16),
            buf((2 * size, full), bf16),
            buf((levels * size, 2 * size), bf16),
            buf((levels * size, 2 * size), bf16),
            buf((levels * size, 4 * size), bf16),
            buf((size, 4 * size), bf16),
            buf((levels, size, full), f32),
            buf((around, -(-levels // 16) * 8, 2 * size), f32),
            buf((levels - 1, inner, size), f32),
            buf((inner, 4 * size), bf16),
            buf((inner, 4 * size), bf16),
            pltpu.SemaphoreType.DMA((5,)),
            sem(2),
            sem(count),
            sem(2),
            sem(10),
            sem(around),
        ],
        compiler_params=pltpu.CompilerParams(
            vmem_limit_bytes=40 * 2**20, collective_id=2, has_side_effects=True
        ),
    )(*(pltpu.with_memory_space_constraint(x, pltpu.MemorySpace.HBM) for x in (diffusivity, mixing, loss_matrix, previous, pair_matrix)))
    return pl.pallas_call(
        hand_out,
        out_shape=[jax.ShapeDtypeStruct(x.shape, x.dtype) for x in results],
        in_specs=[VMEM, VMEM],
        out_specs=[hbm, hbm],
        scratch_shapes=[pltpu.SemaphoreType.DMA((2,))],
        compiler_params=pltpu.CompilerParams(vmem_limit_bytes=2**20),
    )(*results)


def chosen(previous, *rest):
    paired = lax.axis_size("lev") == 4 and previous.shape[2] % 512 == 0
    return (local_pairs if paired else local)(previous, *rest)


def solution(mesh):
    placed = (P("lev", None, "lon"), P("lev", None, None), P("lev", None, None), P("lev"), P("lev"))
    return jax.shard_map(
        chosen,
        mesh=mesh,
        in_specs=placed,
        out_specs=(P("lev", None, "lon"), P("lev", None)),
        check_vma=False,
    )
```
